128 devices in a mesh: ctx: 8 (over z_hi, x), tp: 8 (over y, core), ep: 2 (over z_lo).
Axes of the slice: x: 4, y: 4, z: 4 (z_hi: 2, z_lo: 2; z = z_hi * 2 + z_lo), core: 2. Of those that a mesh axis runs over, the one named last changes fastest.
Arguments:
- resid: bfloat16 [2048, 6144], P('ctx', ('tp', 'ep')), may hold values from -60 to 60
- queries: bfloat16 [2048, 6144], P('ctx', 'tp'), may hold values from -6 to 6
- keys: bfloat16 [2048, 1024], P('ctx', 'tp'), may hold values from -4 to 4
- values: bfloat16 [2048, 1024], P('ctx', 'tp'), may hold values from -5 to 5
- w_out: bfloat16 [6144, 6144], P('tp', ('ctx', 'ep')), may hold values from -0.078125 to 0.078125
- norm_gain: bfloat16 [6144], P(('tp', 'ep')), may hold values from 0.5 to 1.5
- w_gate: bfloat16 [8, 6144, 8192], P('tp', None, ('ctx', 'ep')), may hold values from -0.078125 to 0.078125
- w_up: bfloat16 [8, 6144, 8192], P('tp', None, ('ctx', 'ep')), may hold values from -0.078125 to 0.078125
- w_down: bfloat16 [8, 8192, 6144], P('tp', ('ctx', 'ep')), may hold values from -0.0625 to 0.0625
- expert_ids: int32 [2048, 2], P('ctx'), may hold values from 0 to 7, all different within a row; in each aligned block of 256 rows (0 to 255, 256 to 511, ...) at most 96 rows name the same one
- route_units: int32 [2048, 2], P('ctx'), may hold values from 1 to 65535
Outputs:
- mixed: bfloat16 [2048, 6144], P('ctx', ('tp', 'ep'))
The draws below stay inside these ranges and needn't reach their ends.
Inputs may be any that keep to these rules, and one draw needn't show every extreme that they name: `expert_ids`: each row names two different experts; in every aligned block of 256 rows no expert is named by more than 96 rows, a bound that some block reaches.
All inputs are finite; a program needn't handle non-finite values.
Results may differ from the reference program's by a relative error of at most 0.01.
Values may be sent and summed in bfloat16 or wider, within the bound.
A program may use at most 128 MiB of HBM per device.

```python
import math
import jax
import jax.numpy as jnp
import numpy as np
from jax import lax

D = 6144
H = 48
KVH = 8
HD = 128
FF = 8192
TOK_DEV = 256
TOKENS = 2048
EXPERTS = 8
CAP = 96
N_CTX = 8


def draw_resid(key, part):
    base = jax.random.fold_in(key, 5)
    key_z, key_rows, key_cols = jax.random.split(base, 3)
    column = jnp.arange(D, dtype=jnp.float32) / D
    values_z = jnp.clip(jax.random.normal(key_z, (TOKENS, D), jnp.float32), -4.0, 4.0)
    row_scale = jnp.power(10.0, jax.random.uniform(key_rows, (TOKENS, 1), jnp.float32, -0.5, 0.5))
    col_scale = jnp.power(10.0, jax.random.uniform(key_cols, (1, D), jnp.float32, -0.5, 0.5)) * jnp.power(3.0, 0.5 * (column - 0.5))[None, :]
    return (values_z * row_scale * col_scale).astype(jnp.bfloat16)


def query_key_pair(key):
    base = jax.random.fold_in(key, 17)
    key_q, key_k = jax.random.split(base, 2)
    query_vals = jnp.clip(jax.random.normal(key_q, (TOKENS, H, HD), jnp.float32), -4.0, 4.0)
    key_vals = jnp.clip(jax.random.normal(key_k, (TOKENS, KVH, HD), jnp.float32), -4.0, 4.0)
    return (query_vals.reshape(TOKENS, H * HD), key_vals.reshape(TOKENS, KVH * HD))


def draw_queries(key, part):
    return query_key_pair(key)[0].astype(jnp.bfloat16)


def draw_keys(key, part):
    return query_key_pair(key)[1].astype(jnp.bfloat16)


def touch_ends(drawn, stream_key, low, high):
    longest = drawn.shape.index(max(drawn.shape))
    spots = []
    for shift in (0, 1):
        where = [jax.random.randint(jax.random.fold_in(stream_key, axis), (), 0, length) for axis, length in enumerate(drawn.shape)]
        where[longest] = (where[longest] + shift) % drawn.shape[longest]
        spots.append(tuple(where))
    return drawn.at[spots[0]].set(low).at[spots[1]].set(high)


def levels(key, extent, cuts, least, high):
    gain = 1.0
    for position, shards_of in cuts:
        heights = jax.random.uniform(jax.random.fold_in(jax.random.fold_in(key, 6), position), (shards_of,), jnp.float32, least / len(cuts), high / len(cuts))
        gain = gain * jnp.repeat(jnp.exp(heights), extent[position] // shards_of).reshape((-1,) + (1,) * (len(extent) - 1 - position))
    return gain


def deal_out(rng, own, number, rows, count, top, limit, skew):
    ranking = jax.random.permutation(rng, count)
    crowded, common = portions_of(count, rows * top, limit, skew, True), portions_of(count, rows * top, limit, skew, False)
    places = jnp.arange(count)

    def named(sizes, offset_by):
        used = int((sizes > 0).sum())
        fixed = max(1, used // 4)
        passed = fixed + (places - fixed + offset_by * (used - fixed)) % max(1, count - fixed)
        return jnp.zeros((count,), jnp.int32).at[ranking[jnp.where(places < fixed, places, passed)]].set(jnp.asarray(sizes, jnp.int32))

    sizes = jnp.where(number % 4 == 0, named(crowded, number // 4), named(common, number - number // 4 - 1))
    mixed = jax.random.permutation(jax.random.fold_in(own, 3), count)
    giver, receiver = mixed[0:count // 2 * 2:2], mixed[1:count // 2 * 2:2]
    slack = jnp.minimum(sizes[giver] - 1, limit - sizes[receiver]) // 2
    slack = jnp.where((giver == ranking[0]) | (receiver == ranking[0]) | (sizes[receiver] == 0), 0, jnp.maximum(slack, 0))
    passed = jax.random.randint(jax.random.fold_in(own, 4), (count // 2,), 0, 1 << 20) % (slack + 1)
    sizes = sizes.at[giver].add(-passed).at[receiver].add(passed)
    labels = jnp.searchsorted(jnp.cumsum(sizes), jnp.arange(rows * top), side="right").astype(jnp.int32)
    grid = labels.reshape(top, rows).T
    grid = grid[jax.random.permutation(jax.random.fold_in(own, 1), rows)]
    offset_by = jax.random.randint(jax.random.fold_in(own, 2), (rows, 1), 0, top)
    return jnp.take_along_axis(grid, (jnp.arange(top)[None, :] + offset_by) % top, axis=1)


def portions_of(amount, total, limit, lean, full):
    weights = [(1 << 20) // math.isqrt(grade ** lean) + 1 for grade in range(1, amount + 1)]
    largest = limit if full else min(limit, max(-(-total // amount), total * weights[0] // sum(weights)))
    least = 1 if total - largest >= amount - 1 else 0
    counts, rest = [largest] + [least] * (amount - 1), total - largest - least * (amount - 1)
    while rest > 0:
        free = [i for i in range(1, amount) if counts[i] < largest] or [i for i in range(1, amount) if counts[i] < limit]
        whole, left = sum([weights[i] for i in free]), rest
        for i in free:
            more = min(limit - counts[i], max(1, left * weights[i] // whole), rest)
            counts[i] = counts[i] + more
            rest = rest - more
    return np.array(counts)


def gaussian(own_key, extent, spread, limit, shards=(), kind=jnp.bfloat16):
    loudness = levels(own_key, extent, shards, -0.22, 0.18) if shards else 1.0
    values = jax.random.normal(own_key, extent, jnp.float32) * spread * loudness
    return jnp.minimum(jnp.maximum(values, -limit), limit).astype(kind)


def setup_inputs(seed: int = 0) -> dict:
    splits = jax.random.split(jax.random.key(seed), 12)
    resid = draw_resid(jax.random.fold_in(splits[11], 71), 0)
    queries = draw_queries(jax.random.fold_in(splits[11], 71), 0)
    keys = draw_keys(jax.random.fold_in(splits[11], 71), 0)
    values = gaussian(splits[3], (TOKENS, KVH * HD), 1.0, 5.0, ((0, 8), (1, 8)))
    w_out = gaussian(splits[4], (H * HD, D), (H * HD) ** -0.5, 0.078125, ((0, 8), (1, 16)))
    norm_gain = jnp.clip(1.0 + 0.1 * jax.random.normal(splits[5], (D,), jnp.float32), 0.5, 1.5).astype(jnp.bfloat16)
    w_gate = gaussian(splits[6], (EXPERTS, D, FF), D ** -0.5, 0.078125, ((0, 8), (2, 16)))
    w_up = gaussian(splits[7], (EXPERTS, D, FF), D ** -0.5, 0.078125, ((0, 8), (2, 16)))
    w_down = gaussian(splits[8], (EXPERTS, FF, D), FF ** -0.5, 0.0625, ((0, 8), (1, 16)))
    expert_ids_keys = jax.random.split(jax.random.fold_in(splits[9], 1), TOKENS // TOK_DEV)
    expert_ids_turns = jax.random.permutation(jax.random.fold_in(splits[9], 3), TOKENS // TOK_DEV)
    expert_ids = jax.vmap(lambda own, number: deal_out(jax.random.fold_in(splits[9], 2), own, number, TOK_DEV, EXPERTS, 2, CAP, 2))(expert_ids_keys, expert_ids_turns).reshape((TOKENS, 2))
    route_units = touch_ends(jax.random.randint(splits[10], (TOKENS, 2), 1, 65536), jax.random.fold_in(splits[10], 1), 1, 65535).astype(jnp.int32)
    return dict(resid=resid, queries=queries, keys=keys, values=values, w_out=w_out, norm_gain=norm_gain, w_gate=w_gate, w_up=w_up, w_down=w_down, expert_ids=expert_ids, route_units=route_units)


def attend(query_group, key_group, value_group):
    positions = jnp.arange(TOKENS, dtype=jnp.int32)
    causal = positions[None, :] <= positions[:, None]
    scores = jnp.einsum('tgd,nd->gtn', query_group.astype(jnp.float32), key_group.astype(jnp.float32)) * HD ** (-0.5)
    scores = jnp.where(causal[None], scores, -jnp.inf)
    row_max = lax.optimization_barrier(jnp.max(scores, axis=-1, keepdims=True))
    probs = jnp.where(causal[None], jnp.exp(scores - row_max), 0.0)
    denom = lax.optimization_barrier(jnp.sum(probs, axis=-1))
    probs_b = probs.astype(jnp.bfloat16)
    weighted = jnp.einsum('gtn,nd->gtd', probs_b.astype(jnp.float32), value_group.astype(jnp.float32))
    return weighted / denom[..., None]

def run_expert(operands):
    expert_in, gate_w, up_w, down_w = operands
    flat = expert_in.reshape(N_CTX * CAP, D)
    gate = jnp.dot(flat, gate_w, preferred_element_type=jnp.float32)
    upper = jnp.dot(flat, up_w, preferred_element_type=jnp.float32)
    hidden = (jax.nn.silu(gate) * upper).astype(jnp.bfloat16)
    result = jnp.dot(hidden, down_w, preferred_element_type=jnp.float32).astype(jnp.bfloat16)
    return result.reshape(N_CTX, CAP, D)

def reference(resid, queries, keys, values, w_out, norm_gain, w_gate, w_up, w_down, expert_ids, route_units):
    group = H // KVH
    query_heads = queries.reshape(TOKENS, KVH, group, HD).transpose(1, 0, 2, 3)
    key_heads = keys.reshape(TOKENS, KVH, HD).transpose(1, 0, 2)
    value_heads = values.reshape(TOKENS, KVH, HD).transpose(1, 0, 2)
    heads_out = lax.map(lambda ops: attend(ops[0], ops[1], ops[2]), (query_heads, key_heads, value_heads))
    attn = heads_out.transpose(2, 0, 1, 3).reshape(TOKENS, H * HD).astype(jnp.bfloat16)
    proj = jnp.dot(attn, w_out, preferred_element_type=jnp.float32)
    hres = (resid.astype(jnp.float32) + proj).astype(jnp.bfloat16)
    hfloat = hres.astype(jnp.float32)
    mean_sq = lax.optimization_barrier(jnp.mean(hfloat * hfloat, axis=1, keepdims=True))
    normed = (hfloat * lax.rsqrt(mean_sq + 1e-05) * norm_gain.astype(jnp.float32)).astype(jnp.bfloat16)
    ids = expert_ids.reshape(N_CTX, TOK_DEV, 2)
    onehot = (ids[..., None] == jnp.arange(EXPERTS, dtype=jnp.int32)).astype(jnp.int32)
    per_token = lax.optimization_barrier(jnp.sum(onehot, axis=2))
    earlier = jnp.cumsum(per_token, axis=1) - per_token
    slot = lax.optimization_barrier(jnp.sum(onehot * earlier[:, :, None, :], axis=-1)).astype(jnp.int32)
    block = jnp.broadcast_to(jnp.arange(N_CTX, dtype=jnp.int32)[:, None, None], ids.shape)
    rows = jnp.broadcast_to(normed.reshape(N_CTX, TOK_DEV, 1, D), (N_CTX, TOK_DEV, 2, D))
    expert_in = jnp.zeros((EXPERTS, N_CTX, CAP, D), jnp.bfloat16).at[ids, block, slot].set(rows)
    expert_out = lax.map(run_expert, (expert_in, w_gate, w_up, w_down))
    picked = expert_out[ids, block, slot]
    units = route_units.astype(jnp.float32).reshape(N_CTX, TOK_DEV, 2)
    weights = (units / lax.optimization_barrier(jnp.sum(units, axis=-1, keepdims=True))).astype(jnp.bfloat16)
    moe = lax.optimization_barrier(jnp.sum(weights.astype(jnp.float32)[..., None] * picked.astype(jnp.float32), axis=2))
    return (hfloat + moe.reshape(TOKENS, D)).astype(jnp.bfloat16)
```

```python
import jax
import jax.numpy as jnp
from jax import lax
from jax.experimental import pallas as pl
from jax.experimental.pallas import tpu as pltpu
from jax.sharding import Mesh
from jax.sharding import PartitionSpec as P

D = 6144
HD = 128
CTX = ("zh", "x")
TP = ("y", "core")
TP_EP = ("y", "core", "zl")
MESH_ID = pl.DeviceIdType.MESH
F32 = jnp.float32
BF16 = jnp.bfloat16
FAR_FIRST = (2, 1, -1, 0)


def wrapped(index, size=4):
    return lax.rem(index + size, size)


class Place:
    def __init__(self):
        self.x = lax.axis_index("x")
        self.z = lax.axis_index("zh") * 2 + lax.axis_index("zl")
        self.y = lax.axis_index("y")
        self.core = lax.axis_index("core")
        self.tp = self.y * 2 + self.core

    def beside(self, axis, step):
        if axis == "x":
            return {"x": wrapped(self.x + step)}
        z = wrapped(self.z + step)
        return {"zh": z // 2, "zl": lax.rem(z, 2)}

    def tp_peer(self, step):
        other = lax.rem(self.tp + step, 8)
        return {"y": other // 2, "core": lax.rem(other, 2)}

    def greet(self, tp_peers):
        barrier = pltpu.get_barrier_semaphore()
        peers = [self.beside(axis, step) for axis in ("x", "z") for step in (1, -1)]
        if tp_peers:
            peers += [self.tp_peer(step) for step in range(1, 8)]
        for peer in peers:
            pl.semaphore_signal(barrier, inc=1, device_id=peer, device_id_type=MESH_ID)
        pl.semaphore_wait(barrier, len(peers))


class Link:
    def __init__(self, send_sem, recv_sem):
        self.send_sem, self.recv_sem, self.open = send_sem, recv_sem, []

    def copy(self, number, src, dst, device):
        return pltpu.make_async_remote_copy(
            src_ref=src,
            dst_ref=dst,
            send_sem=self.send_sem.at[number],
            recv_sem=self.recv_sem.at[number],
            device_id=device,
            device_id_type=MESH_ID,
        )

    def send(self, number, src, dst, device):
        copy = self.copy(number, src, dst, device)
        copy.start()
        self.open.append(copy)

    def arrived(self, number, dst, device):
        self.copy(number, dst, dst, device).wait_recv()

    def finish(self):
        for copy in self.open:
            copy.wait_send()
        self.open = []


GATHER_COPIES = 40


def plane_gather(place, link, piece, first=0):
    here = (place.x, place.z)

    def block(part, along_f, along_s, half=None):
        f, s = (here[0], here[1]) if part == 0 else (here[1], here[0])
        f, s = wrapped(f + along_f), wrapped(s + along_s)
        return piece(f, s, part, half) if part == 0 else piece(s, f, part, half)

    def f_axis(part):
        return "xz"[part]

    def s_axis(part):
        return "zx"[part]

    def number(part, kind, g, direction):
        base = {"near": 0, "far": 2, "near2": 4, "far2": 12}[kind]
        return first + part * 20 + base + (FAR_FIRST.index(g) * 2 if kind in ("near2", "far2") else 0) + direction

    def pass_on(part, g):
        ref = block(part, g, 0)
        for direction, step in ((0, 1), (1, -1)):
            link.send(number(part, "near2", g, direction), ref, ref, place.beside(s_axis(part), step))

    for part in (0, 1):
        ref = block(part, 0, 0)
        for direction, step in ((0, 1), (1, -1)):
            link.send(number(part, "near", 0, direction), ref, ref, place.beside(f_axis(part), step))
    for part in (0, 1):
        pass_on(part, 0)
    for part in (0, 1):
        for direction, step in ((0, 1), (1, -1)):
            back = place.beside(f_axis(part), -step)
            link.arrived(number(part, "near", 0, direction), block(part, -step, 0), back)
            ref = block(part, -step, 0, direction)
            link.send(number(part, "far", 0, direction), ref, ref, place.beside(f_axis(part), step))
    for part in (0, 1):
        pass_on(part, -1)
        pass_on(part, 1)

    def relay(part, g):
        for direction, step in ((0, 1), (1, -1)):
            back = place.beside(s_axis(part), -step)
            link.arrived(number(part, "near2", g, direction), block(part, g, -step), back)
            ref = block(part, g, -step, direction)
            link.send(number(part, "far2", g, direction), ref, ref, place.beside(s_axis(part), step))

    for part in (0, 1):
        relay(part, 0)
    for part in (0, 1):
        for direction, step in ((0, 1), (1, -1)):
            back = place.beside(f_axis(part), -step)
            link.arrived(number(part, "far", 0, direction), block(part, 2, 0, direction), back)
        pass_on(part, 2)
    for g in (-1, 1, 2):
        for part in (0, 1):
            relay(part, g)
    for g in (0, -1, 1, 2):
        for part in (0, 1):
            for direction, step in ((0, 1), (1, -1)):
                back = place.beside(s_axis(part), -step)
                link.arrived(number(part, "far2", g, direction), block(part, g, 2, direction), back)


def experts_kernel(
    slots,
    w_gate,
    w_up,
    w_down,
    out,
    rows,
    gate_w,
    up_w,
    down_w,
    gate_acc,
    up_acc,
    hidden,
    partial,
    got_half,
    got_part,
    result,
    returned,
    load_sem,
    send_sem,
    recv_sem,
):
    place = Place()
    link = Link(send_sem, recv_sem)
    loads = [
        pltpu.make_async_copy(src, dst, load_sem.at[i])
        for i, (src, dst) in enumerate(((w_gate, gate_w), (w_up, up_w), (w_down, down_w)))
    ]
    for load in loads:
        load.start()
    place.greet(True)

    base = 80
    for step in range(1, 8):
        target = lax.rem(place.tp + step, 8)
        link.send(base + step, slots.at[target], rows.at[place.x, place.z, place.tp], place.tp_peer(step))
    rows[place.x, place.z, place.tp] = slots[place.tp]
    for step in range(1, 8):
        source = lax.rem(place.tp + 8 - step, 8)
        link.arrived(base + step, rows.at[place.x, place.z, source], place.tp_peer(8 - step))

    def block_of_rows(x, z, part, half):
        if half is None:
            return rows.at[x, z, pl.ds(part * 4, 4)]
        return rows.at[x, z, pl.ds(part * 4 + half * 2, 2)]

    plane_gather(place, link, block_of_rows)

    loads[0].wait()
    loads[1].wait()
    for zh in range(2):
        gate_acc[...] = jnp.zeros_like(gate_acc)
        up_acc[...] = jnp.zeros_like(up_acc)

        @pl.loop(0, 8)
        def _(t):
            even = rows[:, 2 * zh, t].reshape(384, 384)
            odd = rows[:, 2 * zh + 1, t].reshape(384, 384)
            left = jnp.concatenate([even, odd], axis=1)
            span = pl.ds(pl.multiple_of(t * 768, 768), 768)
            gate_acc[...] += jnp.dot(left, gate_w[span, :], preferred_element_type=F32)
            up_acc[...] += jnp.dot(left, up_w[span, :], preferred_element_type=F32)

        gate = gate_acc[...]
        value = gate / (1.0 + jnp.exp(-gate)) * up_acc[...]
        hidden[pl.ds(zh * 4, 4)] = value.astype(BF16).reshape(4, 96, 512)
    loads[2].wait()

    def compute(part, g):
        if part == 0:
            x = wrapped(place.x + g)
            left = jnp.concatenate([hidden[x], hidden[4 + x]], axis=0)

            @pl.loop(0, 4)
            def _(t):
                right = down_w[:, pl.ds(pl.multiple_of(t * 768, 768), 768)]
                both = jnp.dot(left, right, preferred_element_type=F32).astype(BF16)
                for zh in range(2):
                    for e in range(2):
                        partial[x, zh * 2 + e, t] = both[zh * 96 : zh * 96 + 96, e * 384 : e * 384 + 384]
        else:
            z = wrapped(place.z + g)
            left = hidden[pl.ds((z // 2) * 4, 4)].reshape(384, 512)

            @pl.loop(4, 8)
            def _(t):
                start = (2 * t + lax.rem(z, 2)) * 384
                right = down_w[:, pl.ds(pl.multiple_of(start, 384), 384)]
                both = jnp.dot(left, right, preferred_element_type=F32).astype(BF16)
                partial[:, z, t] = both.reshape(4, 96, 384)

    def block(part, along_f, along_s):
        x, z = (along_f, along_s) if part == 0 else (along_s, along_f)
        return wrapped(place.x + x), wrapped(place.z + z)

    def half_of(where, part, half):
        return partial.at[where[0], where[1], pl.ds(part * 4 + half * 2, 2)]

    def part_of(where, part):
        return partial.at[where[0], where[1], pl.ds(part * 4, 4)]

    def add(target, *sources):
        total = target[...].astype(F32)
        for source in sources:
            total = total + source[...].astype(F32)
        target[...] = total.astype(BF16)

    class Ring:
        def __init__(self, part, stage, axis, at):
            self.part, self.stage, self.axis, self.at = part, stage, axis, at
            self.number = 100 + (part * 5 + stage) * 4

        def far(self):
            for direction, step in ((0, 1), (1, -1)):
                link.send(
                    self.number + direction,
                    half_of(self.at(2), self.part, direction),
                    got_half.at[self.part, self.stage, direction],
                    place.beside(self.axis, step),
                )

        def near(self):
            for direction, step in ((0, 1), (1, -1)):
                got = got_half.at[self.part, self.stage, direction]
                link.arrived(self.number + direction, got, place.beside(self.axis, -step))
                add(half_of(self.at(step), self.part, direction), got)
                link.send(
                    self.number + 2 + direction,
                    part_of(self.at(step), self.part),
                    got_part.at[self.part, self.stage, direction],
                    place.beside(self.axis, step),
                )

        def receive(self):
            gots = []
            for direction, step in ((0, 1), (1, -1)):
                got = got_part.at[self.part, self.stage, direction]
                link.arrived(self.number + 2 + direction, got, place.beside(self.axis, -step))
                gots.append(got)
            return gots

        def end(self):
            add(part_of(self.at(0), self.part), *self.receive())

    outer = [
        {
            g: Ring(part, FAR_FIRST.index(g), "zx"[part], lambda step, part=part, g=g: block(part, g, step))
            for g in FAR_FIRST
        }
        for part in (0, 1)
    ]
    inner = [Ring(part, 4, "xz"[part], lambda step, part=part: block(part, step, 0)) for part in (0, 1)]
    for g in FAR_FIRST:
        for part in (0, 1):
            compute(part, g)
            outer[part][g].far()
    for g in FAR_FIRST:
        for part in (0, 1):
            outer[part][g].near()
    for part in (0, 1):
        outer[part][2].end()
        inner[part].far()
    for part in (0, 1):
        outer[part][1].end()
        outer[part][-1].end()
        inner[part].near()
    base = 88
    for part in (0, 1):
        outer[part][0].end()
        gots = inner[part].receive()
        total = part_of(inner[part].at(0), part)[...].astype(F32)
        for got in gots:
            total = total + got[...].astype(F32)
        result[pl.ds(part * 4, 4)] = total.astype(BF16)
    for step in range(1, 8):
        target = lax.rem(place.tp + step, 8)
        link.send(base + step, result.at[target], returned.at[place.tp], place.tp_peer(step))
    returned[place.tp] = result[place.tp]
    for step in range(1, 8):
        source = lax.rem(place.tp + 8 - step, 8)
        link.arrived(base + step, returned.at[source], place.tp_peer(8 - step))
    link.finish()
    out[...] = returned[...]


def experts(slots, w_gate, w_up, w_down):
    copies = 140
    return pl.pallas_call(
        experts_kernel,
        out_shape=jax.ShapeDtypeStruct((8, 96, 384), BF16),
        in_specs=[pl.BlockSpec(memory_space=pltpu.VMEM)] + [pl.BlockSpec(memory_space=pl.ANY)] * 3,
        out_specs=pl.BlockSpec(memory_space=pltpu.VMEM),
        scratch_shapes=[
            pltpu.VMEM((4, 4, 8, 96, 384), BF16),
            pltpu.VMEM((6144, 512), BF16),
            pltpu.VMEM((6144, 512), BF16),
            pltpu.VMEM((512, 6144), BF16),
            pltpu.VMEM((384, 512), F32),
            pltpu.VMEM((384, 512), F32),
            pltpu.VMEM((8, 96, 512), BF16),
            pltpu.VMEM((4, 4, 8, 96, 384), BF16),
            pltpu.VMEM((2, 5, 2, 2, 96, 384), BF16),
            pltpu.VMEM((2, 5, 2, 4, 96, 384), BF16),
            pltpu.VMEM((8, 96, 384), BF16),
            pltpu.VMEM((8, 96, 384), BF16),
            pltpu.SemaphoreType.DMA((3,)),
            pltpu.SemaphoreType.DMA((copies,)),
            pltpu.SemaphoreType.DMA((copies,)),
        ],
        compiler_params=pltpu.CompilerParams(
            collective_id=1, has_side_effects=True, vmem_limit_bytes=64 * 1024 * 1024 - 128 * 1024
        ),
        name="experts",
    )(slots, w_gate, w_up, w_down)


def split_up(x, dim, size):
    dims = x.shape
    tiles = x.reshape(*dims[:dim], size, dims[dim] // size, *dims[dim + 1 :])
    return jnp.moveaxis(tiles, dim, 0)


def sent_and_summed(x, axis, dim):
    tiles = split_up(x, dim, lax.axis_size(axis))
    arrived = lax.all_to_all(tiles, axis, split_axis=0, concat_axis=0, tiled=True)
    return arrived.astype(jnp.float32).sum(axis=0)


def from_everyone(x, axis):
    size = lax.axis_size(axis)
    return lax.all_to_all(jnp.broadcast_to(x[None], (size, *x.shape)), axis, 0, 0, tiled=True)


def taken_together(x, axis):
    everything = from_everyone(x, axis)
    return jnp.sum(everything, axis=0)


def on_device(
    resid, queries, keys, values, w_out, norm_gain, w_gate, w_up, w_down, expert_ids, route_units
):
    tp_size = lax.axis_size(TP)
    tok_rows = queries.shape[0]
    heads_dev = queries.shape[1] // HD
    kv_dev = keys.shape[1] // HD
    group = heads_dev // kv_dev
    feat_dev = resid.shape[1]
    capacity = 3 * tok_rows // tp_size
    first_pos = lax.axis_index(CTX) * tok_rows
    query_heads = queries.reshape(tok_rows, kv_dev, group, HD)
    query_pos = first_pos + jnp.arange(tok_rows, dtype=jnp.int32)
    running_max = jnp.full((kv_dev, group, tok_rows), -1e30, jnp.float32)
    key_piece = lax.all_gather(keys, CTX, axis=0, tiled=True)
    value_piece = lax.all_gather(values, CTX, axis=0, tiled=True)
    count = key_piece.shape[0]
    key_rows = key_piece.reshape(count, kv_dev, HD)
    value_rows = value_piece.reshape(count, kv_dev, HD)
    scores = jnp.einsum(
        "tkgd,nkd->kgtn", query_heads, key_rows, preferred_element_type=jnp.float32
    ) * HD ** (-0.5)
    key_pos = jnp.arange(count, dtype=jnp.int32)
    allowed = (key_pos[None, :] <= query_pos[:, None])[None, None]
    block_max = jnp.max(jnp.where(allowed, scores, -1e30), axis=-1)
    new_max = jnp.maximum(running_max, block_max)
    probs = jnp.where(allowed, jnp.exp(scores - new_max[..., None]), 0.0)
    new_sum = jnp.sum(probs, axis=-1)
    probs_b = probs.astype(jnp.bfloat16)
    update = jnp.einsum("kgtn,nkd->kgtd", probs_b, value_rows, preferred_element_type=jnp.float32)
    attn = (
        (update / new_sum[..., None])
        .transpose(2, 0, 1, 3)
        .reshape(tok_rows, heads_dev * HD)
        .astype(jnp.bfloat16)
    )
    partial_proj = jnp.dot(
        attn, lax.all_gather(w_out, CTX, axis=1, tiled=True), preferred_element_type=jnp.float32
    )
    proj = sent_and_summed(partial_proj.astype(jnp.bfloat16), TP, 1)
    hres = (resid.astype(jnp.float32) + proj).astype(jnp.bfloat16)
    hfloat = hres.astype(jnp.float32)
    square_total = taken_together(jnp.sum(hfloat * hfloat, axis=1, keepdims=True), TP_EP)
    normed = (hfloat * lax.rsqrt(square_total / D + 1e-05) * norm_gain.astype(jnp.float32)).astype(
        jnp.bfloat16
    )
    onehot = (expert_ids[..., None] == jnp.arange(tp_size, dtype=jnp.int32)).astype(jnp.int32)
    per_token = jnp.sum(onehot, axis=1)
    earlier = jnp.cumsum(per_token, axis=0) - per_token
    slot = jnp.sum(onehot * earlier[:, None, :], axis=-1)
    codes = expert_ids * capacity + slot
    slot_ids = jnp.arange(tp_size * capacity, dtype=jnp.int32)
    picks = (
        (slot_ids[:, None] == codes[None, :, 0]) | (slot_ids[:, None] == codes[None, :, 1])
    ).astype(jnp.bfloat16)
    dispatched = jnp.dot(picks, normed, preferred_element_type=jnp.float32).astype(jnp.bfloat16)
    returned = experts(dispatched.reshape(tp_size, capacity, feat_dev), w_gate[0], w_up[0], w_down[0])
    units = route_units.astype(jnp.float32)
    weights = (units / jnp.sum(units, axis=-1, keepdims=True)).astype(jnp.bfloat16)
    combine = jnp.where(slot_ids[None, :] == codes[:, 0:1], weights[:, 0:1], 0.0) + jnp.where(
        slot_ids[None, :] == codes[:, 1:2], weights[:, 1:2], 0.0
    )
    moe = jnp.dot(
        combine, returned.reshape(tp_size * capacity, feat_dev), preferred_element_type=jnp.float32
    )
    return (hfloat + moe).astype(jnp.bfloat16)


def solution(mesh):
    torus = Mesh(mesh.devices.reshape(2, 4, 4, 2, 2), ("zh", "x", "y", "core", "zl"))
    in_specs = (
        P(CTX, TP_EP),
        P(CTX, TP),
        P(CTX, TP),
        P(CTX, TP),
        P(TP, ("zh", "x", "zl")),
        P(TP_EP),
        P(TP, None, ("zh", "x", "zl")),
        P(TP, None, ("zh", "x", "zl")),
        P(TP, ("zh", "x", "zl"), None),
        P(CTX, None),
        P(CTX, None),
    )
    return jax.shard_map(
        on_device, mesh=torus, in_specs=in_specs, out_specs=P(CTX, TP_EP), check_vma=False
    )
```

```python
import jax
import jax.numpy as jnp
from jax import lax
from jax.experimental import pallas as pl
from jax.experimental.pallas import tpu as pltpu
from jax.sharding import Mesh
from jax.sharding import PartitionSpec as P

D = 6144
HD = 128
CTX = ("zh", "x")
TP = ("y", "core")
TP_EP = ("y", "core", "zl")
MESH_ID = pl.DeviceIdType.MESH
F32 = jnp.float32
BF16 = jnp.bfloat16
FAR_FIRST = (2, 1, -1, 0)


def wrapped(index, size=4):
    return lax.rem(index + size, size)


class Place:
    def __init__(self):
        self.x = lax.axis_index("x")
        self.z = lax.axis_index("zh") * 2 + lax.axis_index("zl")
        self.y = lax.axis_index("y")
        self.core = lax.axis_index("core")
        self.zl = lax.axis_index("zl")
        self.tp = self.y * 2 + self.core
        self.ctx = lax.axis_index("zh") * 4 + self.x
        self.member = self.tp * 2 + self.zl

    def beside(self, axis, step):
        if axis == "x":
            return {"x": wrapped(self.x + step)}
        z = wrapped(self.z + step)
        return {"zh": z // 2, "zl": lax.rem(z, 2)}

    def tp_peer(self, step):
        other = lax.rem(self.tp + step, 8)
        return {"y": other // 2, "core": lax.rem(other, 2)}

    def member_peer(self, step):
        other = lax.rem(self.member + step, 16)
        return {"y": other // 4, "core": lax.rem(other // 2, 2), "zl": lax.rem(other, 2)}

    def owner(self, j):
        ctx = 2 * j + self.core
        return {"zh": ctx // 4, "x": lax.rem(ctx, 4), "y": self.ctx // 2, "core": lax.rem(self.ctx, 2)}

    def giver(self, y):
        return {"zh": self.tp // 4, "x": lax.rem(self.tp, 4), "y": y, "core": lax.rem(self.ctx, 2)}

    def greet(self, peers):
        barrier = pltpu.get_barrier_semaphore()
        peers = [self.beside(axis, step) for axis in ("x", "z") for step in (1, -1)] + peers
        for peer in peers:
            pl.semaphore_signal(barrier, inc=1, device_id=peer, device_id_type=MESH_ID)
        return len(peers)


class Link:
    def __init__(self, send_sem, recv_sem):
        self.send_sem, self.recv_sem, self.open = send_sem, recv_sem, []

    def copy(self, number, src, dst, device, landing=None):
        return pltpu.make_async_remote_copy(
            src_ref=src,
            dst_ref=dst,
            send_sem=self.send_sem.at[number],
            recv_sem=self.recv_sem.at[number if landing is None else landing],
            device_id=device,
            device_id_type=MESH_ID,
        )

    def send(self, number, src, dst, device, landing=None):
        copy = self.copy(number, src, dst, device, landing)
        copy.start()
        self.open.append(copy)

    def arrived(self, number, dst, device):
        self.copy(number, dst, dst, device).wait_recv()

    def finish(self):
        for copy in self.open:
            copy.wait_send()
        self.open = []


GATHER_COPIES = 40


def plane_gather(place, link, piece, first=0, ready=None):
    here = (place.x, place.z)

    def block(part, along_f, along_s, half=None):
        f, s = (here[0], here[1]) if part == 0 else (here[1], here[0])
        f, s = wrapped(f + along_f), wrapped(s + along_s)
        return piece(f, s, part, half) if part == 0 else piece(s, f, part, half)

    def f_axis(part):
        return "xz"[part]

    def s_axis(part):
        return "zx"[part]

    def number(part, kind, g, direction):
        base = {"near": 0, "far": 2, "near2": 4, "far2": 12}[kind]
        return first + part * 20 + base + (FAR_FIRST.index(g) * 2 if kind in ("near2", "far2") else 0) + direction

    def pass_on(part, g):
        ref = block(part, g, 0)
        for direction, step in ((0, 1), (1, -1)):
            link.send(number(part, "near2", g, direction), ref, ref, place.beside(s_axis(part), step))

    for part in (0, 1):
        if ready is not None:
            ready(part)
        ref = block(part, 0, 0)
        for direction, step in ((0, 1), (1, -1)):
            link.send(number(part, "near", 0, direction), ref, ref, place.beside(f_axis(part), step))
        if ready is not None:
            pass_on(part, 0)
    if ready is None:
        for part in (0, 1):
            pass_on(part, 0)
    for part in (0, 1):
        for direction, step in ((0, 1), (1, -1)):
            back = place.beside(f_axis(part), -step)
            link.arrived(number(part, "near", 0, direction), block(part, -step, 0), back)
            ref = block(part, -step, 0, direction)
            link.send(number(part, "far", 0, direction), ref, ref, place.beside(f_axis(part), step))
    for part in (0, 1):
        pass_on(part, -1)
        pass_on(part, 1)

    def relay(part, g):
        for direction, step in ((0, 1), (1, -1)):
            back = place.beside(s_axis(part), -step)
            link.arrived(number(part, "near2", g, direction), block(part, g, -step), back)
            ref = block(part, g, -step, direction)
            link.send(number(part, "far2", g, direction), ref, ref, place.beside(s_axis(part), step))

    for part in (0, 1):
        relay(part, 0)
    for part in (0, 1):
        for direction, step in ((0, 1), (1, -1)):
            back = place.beside(f_axis(part), -step)
            link.arrived(number(part, "far", 0, direction), block(part, 2, 0, direction), back)
        pass_on(part, 2)
    for g in (-1, 1, 2):
        for part in (0, 1):
            relay(part, g)
    for g in (0, -1, 1, 2):
        for part in (0, 1):
            for direction, step in ((0, 1), (1, -1)):
                back = place.beside(s_axis(part), -step)
                link.arrived(number(part, "far2", g, direction), block(part, g, 2, direction), back)


def attention_kernel(
    queries,
    keys,
    values,
    w_out,
    resid,
    hres,
    squares,
    all_keys,
    all_values,
    attn,
    given,
    got_core,
    kept,
    got,
    stats,
    send_sem,
    recv_sem,
):
    place = Place()
    link = Link(send_sem, recv_sem)
    barrier = pltpu.get_barrier_semaphore()
    diagonal = place.ctx == place.tp
    own = [jnp.logical_and(diagonal, place.y == j) for j in range(4)]
    for j in range(4):

        @pl.when(jnp.logical_not(own[j]))
        def _():
            for peer in (place.owner(j), place.giver(j)):
                pl.semaphore_signal(barrier, inc=1, device_id=peer, device_id_type=MESH_ID)

    members = [place.member_peer(step) for step in range(1, 16)]
    greeted = place.greet(members)

    @pl.when(diagonal)
    def _():
        pl.semaphore_wait(barrier, greeted + 6)

    @pl.when(jnp.logical_not(diagonal))
    def _():
        pl.semaphore_wait(barrier, greeted + 8)

    def at(x, z):
        return ((z // 2) * 4 + x) * 2 + lax.rem(z, 2)

    here = place.ctx * 2 + place.zl
    mine = pl.ds(pl.multiple_of(place.zl * 128, 128), 128)
    all_keys[here] = keys[mine, :]
    all_values[here] = values[mine, :]

    def key_block(x, z, part, half):
        ref = (all_keys, all_values)[part]
        if half is None:
            return ref.at[at(x, z)]
        return ref.at[at(x, z), pl.ds(half * 64, 64)]

    plane_gather(place, link, key_block)

    def attend(part):
        @pl.loop(part * 3, part * 3 + 3)
        def _(head):
            columns = pl.ds(pl.multiple_of(head * HD, HD), HD)
            scores = lax.dot_general(
                queries[mine, columns],
                all_keys[...].reshape(2048, HD),
                (((1,), (1,)), ((), ())),
                preferred_element_type=F32,
            ) * HD ** (-0.5)
            query_pos = here * 128 + lax.broadcasted_iota(jnp.int32, (128, 2048), 0)
            key_pos = lax.broadcasted_iota(jnp.int32, (128, 2048), 1)
            scores = jnp.where(key_pos <= query_pos, scores, -1e30)
            probs = jnp.exp(scores - jnp.max(scores, axis=1, keepdims=True))
            denom = jnp.sum(probs, axis=1, keepdims=True)
            update = jnp.dot(
                probs.astype(BF16), all_values[...].reshape(2048, HD), preferred_element_type=F32
            )
            attn[here, :, columns] = (update / denom).astype(BF16)

    def attn_block(x, z, part, half):
        columns = pl.ds(part * 384, 384)
        if half is None:
            return attn.at[at(x, z), :, columns]
        return attn.at[at(x, z), pl.ds(half * 64, 64), columns]

    plane_gather(place, link, attn_block, first=40, ready=attend)

    def project(ctx):
        rows = attn[pl.ds(ctx * 2, 2)].reshape(256, 768)
        return jnp.dot(rows, w_out[...], preferred_element_type=F32)

    partner = {"core": 1 - place.core}
    for j in range(4):
        given[j] = project(2 * j + 1 - place.core).astype(BF16)
        link.send(80 + j, given.at[j], got_core.at[j], partner)
    for j in range(4):
        total = project(2 * j + place.core)
        link.arrived(80 + j, got_core.at[j], partner)
        kept[j] = (total + got_core[j].astype(F32)).astype(BF16)
        copy = link.copy(84 + j, kept.at[j], got.at[place.y], place.owner(j), 88 + place.y)

        @pl.when(own[j])
        def _():
            got[j] = kept[j]

        @pl.when(jnp.logical_not(own[j]))
        def _():
            copy.start()

    total = resid[...].astype(F32)
    for j in range(4):

        @pl.when(jnp.logical_not(own[j]))
        def _():
            link.arrived(88 + j, got.at[j], place.giver(j))

        total = total + got[j].astype(F32)
    value = total.astype(BF16)
    hres[...] = value
    value = value.astype(F32)
    sums = lax.dot_general(
        jnp.ones((8, 384), F32),
        value * value,
        (((1,), (1,)), ((), ())),
        precision=lax.Precision.HIGHEST,
        preferred_element_type=F32,
    )
    stats[place.member] = sums
    for step in range(1, 16):
        link.send(92 + step, stats.at[place.member], stats.at[place.member], members[step - 1])
    for step in range(1, 16):
        source = lax.rem(place.member + 16 - step, 16)
        link.arrived(92 + step, stats.at[source], members[15 - step])
    squares[...] = jnp.sum(stats[...], axis=0)
    link.finish()
    for j in range(4):

        @pl.when(jnp.logical_not(own[j]))
        def _():
            link.copy(84 + j, kept.at[j], got.at[place.y], place.owner(j), 88 + place.y).wait_send()


def attention(queries, keys, values, w_out, resid):
    vmem = pl.BlockSpec(memory_space=pltpu.VMEM)
    return pl.pallas_call(
        attention_kernel,
        out_shape=(jax.ShapeDtypeStruct((256, 384), BF16), jax.ShapeDtypeStruct((8, 256), F32)),
        in_specs=[vmem] * 5,
        out_specs=(vmem, vmem),
        scratch_shapes=[
            pltpu.VMEM((16, 128, HD), BF16),
            pltpu.VMEM((16, 128, HD), BF16),
            pltpu.VMEM((16, 128, 768), BF16),
            pltpu.VMEM((4, 256, 384), BF16),
            pltpu.VMEM((4, 256, 384), BF16),
            pltpu.VMEM((4, 256, 384), BF16),
            pltpu.VMEM((4, 256, 384), BF16),
            pltpu.VMEM((16, 8, 256), F32),
            pltpu.SemaphoreType.DMA((108,)),
            pltpu.SemaphoreType.DMA((108,)),
        ],
        compiler_params=pltpu.CompilerParams(
            collective_id=0, has_side_effects=True, vmem_limit_bytes=48 * 1024 * 1024
        ),
        name="attention",
    )(queries, keys, values, w_out, resid)


def experts_kernel(
    slots,
    w_gate,
    w_up,
    w_down,
    out,
    rows,
    gate_w,
    up_w,
    down_w,
    gate_acc,
    up_acc,
    hidden,
    partial,
    got_half,
    got_part,
    result,
    returned,
    load_sem,
    send_sem,
    recv_sem,
):
    place = Place()
    link = Link(send_sem, recv_sem)
    loads = [
        pltpu.make_async_copy(src, dst, load_sem.at[i])
        for i, (src, dst) in enumerate(((w_gate, gate_w), (w_up, up_w), (w_down, down_w)))
    ]
    for load in loads:
        load.start()
    greeted = place.greet([place.tp_peer(step) for step in range(1, 8)])
    pl.semaphore_wait(pltpu.get_barrier_semaphore(), greeted)

    base = 80
    for step in range(1, 8):
        target = lax.rem(place.tp + step, 8)
        link.send(base + step, slots.at[target], rows.at[place.x, place.z, place.tp], place.tp_peer(step))
    rows[place.x, place.z, place.tp] = slots[place.tp]
    for step in range(1, 8):
        source = lax.rem(place.tp + 8 - step, 8)
        link.arrived(base + step, rows.at[place.x, place.z, source], place.tp_peer(8 - step))

    def block_of_rows(x, z, part, half):
        if half is None:
            return rows.at[x, z, pl.ds(part * 4, 4)]
        return rows.at[x, z, pl.ds(part * 4 + half * 2, 2)]

    plane_gather(place, link, block_of_rows)

    loads[0].wait()
    loads[1].wait()
    for zh in range(2):
        gate_acc[...] = jnp.zeros_like(gate_acc)
        up_acc[...] = jnp.zeros_like(up_acc)

        @pl.loop(0, 8)
        def _(t):
            even = rows[:, 2 * zh, t].reshape(384, 384)
            odd = rows[:, 2 * zh + 1, t].reshape(384, 384)
            left = jnp.concatenate([even, odd], axis=1)
            span = pl.ds(pl.multiple_of(t * 768, 768), 768)
            gate_acc[...] += jnp.dot(left, gate_w[span, :], preferred_element_type=F32)
            up_acc[...] += jnp.dot(left, up_w[span, :], preferred_element_type=F32)

        gate = gate_acc[...]
        value = gate / (1.0 + jnp.exp(-gate)) * up_acc[...]
        hidden[pl.ds(zh * 4, 4)] = value.astype(BF16).reshape(4, 96, 512)
    loads[2].wait()

    def compute(part, g):
        if part == 0:
            x = wrapped(place.x + g)
            left = jnp.concatenate([hidden[x], hidden[4 + x]], axis=0)

            @pl.loop(0, 4)
            def _(t):
                right = down_w[:, pl.ds(pl.multiple_of(t * 768, 768), 768)]
                both = jnp.dot(left, right, preferred_element_type=F32).astype(BF16)
                for zh in range(2):
                    for e in range(2):
                        partial[x, zh * 2 + e, t] = both[zh * 96 : zh * 96 + 96, e * 384 : e * 384 + 384]
        else:
            z = wrapped(place.z + g)
            left = hidden[pl.ds((z // 2) * 4, 4)].reshape(384, 512)

            @pl.loop(4, 8)
            def _(t):
                start = (2 * t + lax.rem(z, 2)) * 384
                right = down_w[:, pl.ds(pl.multiple_of(start, 384), 384)]
                both = jnp.dot(left, right, preferred_element_type=F32).astype(BF16)
                partial[:, z, t] = both.reshape(4, 96, 384)

    def block(part, along_f, along_s):
        x, z = (along_f, along_s) if part == 0 else (along_s, along_f)
        return wrapped(place.x + x), wrapped(place.z + z)

    def half_of(where, part, half):
        return partial.at[where[0], where[1], pl.ds(part * 4 + half * 2, 2)]

    def part_of(where, part):
        return partial.at[where[0], where[1], pl.ds(part * 4, 4)]

    def add(target, *sources):
        total = target[...].astype(F32)
        for source in sources:
            total = total + source[...].astype(F32)
        target[...] = total.astype(BF16)

    class Ring:
        def __init__(self, part, stage, axis, at):
            self.part, self.stage, self.axis, self.at = part, stage, axis, at
            self.number = 100 + (part * 5 + stage) * 4

        def far(self):
            for direction, step in ((0, 1), (1, -1)):
                link.send(
                    self.number + direction,
                    half_of(self.at(2), self.part, direction),
                    got_half.at[self.part, self.stage, direction],
                    place.beside(self.axis, step),
                )

        def near(self):
            for direction, step in ((0, 1), (1, -1)):
                got = got_half.at[self.part, self.stage, direction]
                link.arrived(self.number + direction, got, place.beside(self.axis, -step))
                add(half_of(self.at(step), self.part, direction), got)
                link.send(
                    self.number + 2 + direction,
                    part_of(self.at(step), self.part),
                    got_part.at[self.part, self.stage, direction],
                    place.beside(self.axis, step),
                )

        def receive(self):
            gots = []
            for direction, step in ((0, 1), (1, -1)):
                got = got_part.at[self.part, self.stage, direction]
                link.arrived(self.number + 2 + direction, got, place.beside(self.axis, -step))
                gots.append(got)
            return gots

        def end(self):
            add(part_of(self.at(0), self.part), *self.receive())

    outer = [
        {
            g: Ring(part, FAR_FIRST.index(g), "zx"[part], lambda step, part=part, g=g: block(part, g, step))
            for g in FAR_FIRST
        }
        for part in (0, 1)
    ]
    inner = [Ring(part, 4, "xz"[part], lambda step, part=part: block(part, step, 0)) for part in (0, 1)]
    for g in FAR_FIRST:
        for part in (0, 1):
            compute(part, g)
            outer[part][g].far()
    for g in FAR_FIRST:
        for part in (0, 1):
            outer[part][g].near()
    for part in (0, 1):
        outer[part][2].end()
        inner[part].far()
    for part in (0, 1):
        outer[part][1].end()
        outer[part][-1].end()
        inner[part].near()
    base = 88
    for part in (0, 1):
        outer[part][0].end()
        gots = inner[part].receive()
        total = part_of(inner[part].at(0), part)[...].astype(F32)
        for got in gots:
            total = total + got[...].astype(F32)
        result[pl.ds(part * 4, 4)] = total.astype(BF16)
    for step in range(1, 8):
        target = lax.rem(place.tp + step, 8)
        link.send(base + step, result.at[target], returned.at[place.tp], place.tp_peer(step))
    returned[place.tp] = result[place.tp]
    for step in range(1, 8):
        source = lax.rem(place.tp + 8 - step, 8)
        link.arrived(base + step, returned.at[source], place.tp_peer(8 - step))
    link.finish()
    out[...] = returned[...]


def experts(slots, w_gate, w_up, w_down):
    copies = 140
    return pl.pallas_call(
        experts_kernel,
        out_shape=jax.ShapeDtypeStruct((8, 96, 384), BF16),
        in_specs=[pl.BlockSpec(memory_space=pltpu.VMEM)] + [pl.BlockSpec(memory_space=pl.ANY)] * 3,
        out_specs=pl.BlockSpec(memory_space=pltpu.VMEM),
        scratch_shapes=[
            pltpu.VMEM((4, 4, 8, 96, 384), BF16),
            pltpu.VMEM((6144, 512), BF16),
            pltpu.VMEM((6144, 512), BF16),
            pltpu.VMEM((512, 6144), BF16),
            pltpu.VMEM((384, 512), F32),
            pltpu.VMEM((384, 512), F32),
            pltpu.VMEM((8, 96, 512), BF16),
            pltpu.VMEM((4, 4, 8, 96, 384), BF16),
            pltpu.VMEM((2, 5, 2, 2, 96, 384), BF16),
            pltpu.VMEM((2, 5, 2, 4, 96, 384), BF16),
            pltpu.VMEM((8, 96, 384), BF16),
            pltpu.VMEM((8, 96, 384), BF16),
            pltpu.SemaphoreType.DMA((3,)),
            pltpu.SemaphoreType.DMA((copies,)),
            pltpu.SemaphoreType.DMA((copies,)),
        ],
        compiler_params=pltpu.CompilerParams(
            collective_id=1, has_side_effects=True, vmem_limit_bytes=64 * 1024 * 1024 - 128 * 1024
        ),
        name="experts",
    )(slots, w_gate, w_up, w_down)


def on_device(
    resid, queries, keys, values, w_out, norm_gain, w_gate, w_up, w_down, expert_ids, route_units
):
    tp_size = lax.axis_size(TP)
    tok_rows = queries.shape[0]
    feat_dev = resid.shape[1]
    capacity = 3 * tok_rows // tp_size
    hres, squares = attention(queries, keys, values, w_out, resid)
    hfloat = hres.astype(jnp.float32)
    square_total = squares[0][:, None]
    normed = (hfloat * lax.rsqrt(square_total / D + 1e-05) * norm_gain.astype(jnp.float32)).astype(
        jnp.bfloat16
    )
    onehot = (expert_ids[..., None] == jnp.arange(tp_size, dtype=jnp.int32)).astype(jnp.int32)
    per_token = jnp.sum(onehot, axis=1)
    earlier = jnp.cumsum(per_token, axis=0) - per_token
    slot = jnp.sum(onehot * earlier[:, None, :], axis=-1)
    codes = expert_ids * capacity + slot
    slot_ids = jnp.arange(tp_size * capacity, dtype=jnp.int32)
    picks = (
        (slot_ids[:, None] == codes[None, :, 0]) | (slot_ids[:, None] == codes[None, :, 1])
    ).astype(jnp.bfloat16)
    dispatched = jnp.dot(picks, normed, preferred_element_type=jnp.float32).astype(jnp.bfloat16)
    returned = experts(dispatched.reshape(tp_size, capacity, feat_dev), w_gate[0], w_up[0], w_down[0])
    units = route_units.astype(jnp.float32)
    weights = (units / jnp.sum(units, axis=-1, keepdims=True)).astype(jnp.bfloat16)
    combine = jnp.where(slot_ids[None, :] == codes[:, 0:1], weights[:, 0:1], 0.0) + jnp.where(
        slot_ids[None, :] == codes[:, 1:2], weights[:, 1:2], 0.0
    )
    moe = jnp.dot(
        combine, returned.reshape(tp_size * capacity, feat_dev), preferred_element_type=jnp.float32
    )
    return (hfloat + moe).astype(jnp.bfloat16)


def solution(mesh):
    torus = Mesh(mesh.devices.reshape(2, 4, 4, 2, 2), ("zh", "x", "y", "core", "zl"))
    in_specs = (
        P(CTX, TP_EP),
        P(CTX, TP),
        P(CTX, TP),
        P(CTX, TP),
        P(TP, ("zh", "x", "zl")),
        P(TP_EP),
        P(TP, None, ("zh", "x", "zl")),
        P(TP, None, ("zh", "x", "zl")),
        P(TP, ("zh", "x", "zl"), None),
        P(CTX, None),
        P(CTX, None),
    )
    return jax.shard_map(
        on_device, mesh=torus, in_specs=in_specs, out_specs=P(CTX, TP_EP), check_vma=False
    )
```

```python
import jax
import jax.numpy as jnp
from jax import lax
from jax.experimental import pallas as pl
from jax.experimental.pallas import tpu as pltpu
from jax.sharding import Mesh
from jax.sharding import PartitionSpec as P

D = 6144
HD = 128
CTX = ("zh", "x")
TP = ("y", "core")
TP_EP = ("y", "core", "zl")
MESH_ID = pl.DeviceIdType.MESH
F32 = jnp.float32
BF16 = jnp.bfloat16
FAR_FIRST = (2, 1, -1, 0)


def wrapped(index, size=4):
    return lax.rem(index + size, size)


class Place:
    def __init__(self):
        self.x = lax.axis_index("x")
        self.z = lax.axis_index("zh") * 2 + lax.axis_index("zl")
        self.y = lax.axis_index("y")
        self.core = lax.axis_index("core")
        self.zl = lax.axis_index("zl")
        self.tp = self.y * 2 + self.core
        self.ctx = lax.axis_index("zh") * 4 + self.x
        self.member = self.tp * 2 + self.zl

    def beside(self, axis, step):
        if axis == "x":
            return {"x": wrapped(self.x + step)}
        z = wrapped(self.z + step)
        return {"zh": z // 2, "zl": lax.rem(z, 2)}

    def tp_peer(self, step):
        other = lax.rem(self.tp + step, 8)
        return {"y": other // 2, "core": lax.rem(other, 2)}

    def member_peer(self, step):
        other = lax.rem(self.member + step, 16)
        return {"y": other // 4, "core": lax.rem(other // 2, 2), "zl": lax.rem(other, 2)}

    def mirror(self):
        return {"zh": self.tp // 4, "x": lax.rem(self.tp, 4), "y": self.ctx // 2, "core": lax.rem(self.ctx, 2)}

    def greet(self, peers):
        barrier = pltpu.get_barrier_semaphore()
        peers = [self.beside(axis, step) for axis in ("x", "z") for step in (1, -1)] + peers
        for peer in peers:
            pl.semaphore_signal(barrier, inc=1, device_id=peer, device_id_type=MESH_ID)
        return len(peers)


class Link:
    def __init__(self, send_sem, recv_sem):
        self.send_sem, self.recv_sem, self.open = send_sem, recv_sem, []

    def copy(self, number, src, dst, device, landing=None):
        return pltpu.make_async_remote_copy(
            src_ref=src,
            dst_ref=dst,
            send_sem=self.send_sem.at[number],
            recv_sem=self.recv_sem.at[number if landing is None else landing],
            device_id=device,
            device_id_type=MESH_ID,
        )

    def send(self, number, src, dst, device, landing=None):
        copy = self.copy(number, src, dst, device, landing)
        copy.start()
        self.open.append(copy)

    def arrived(self, number, dst, device):
        self.copy(number, dst, dst, device).wait_recv()

    def finish(self):
        for copy in self.open:
            copy.wait_send()
        self.open = []


GATHER_COPIES = 40


def plane_gather(place, link, piece, first=0, ready=None, seen=None):
    here = (place.x, place.z)

    def block(part, along_f, along_s, half=None):
        f, s = (here[0], here[1]) if part == 0 else (here[1], here[0])
        f, s = wrapped(f + along_f), wrapped(s + along_s)
        return piece(f, s, part, half) if part == 0 else piece(s, f, part, half)

    def f_axis(part):
        return "xz"[part]

    def s_axis(part):
        return "zx"[part]

    def number(part, kind, g, direction):
        base = {"near": 0, "far": 2, "near2": 4, "far2": 12}[kind]
        return first + part * 20 + base + (FAR_FIRST.index(g) * 2 if kind in ("near2", "far2") else 0) + direction

    def pass_on(part, g):
        ref = block(part, g, 0)
        for direction, step in ((0, 1), (1, -1)):
            link.send(number(part, "near2", g, direction), ref, ref, place.beside(s_axis(part), step))

    for part in (0, 1):
        if ready is not None:
            ready(part)
        ref = block(part, 0, 0)
        for direction, step in ((0, 1), (1, -1)):
            link.send(number(part, "near", 0, direction), ref, ref, place.beside(f_axis(part), step))
        if ready is not None:
            pass_on(part, 0)
    if ready is None:
        for part in (0, 1):
            pass_on(part, 0)
    for part in (0, 1):
        for direction, step in ((0, 1), (1, -1)):
            back = place.beside(f_axis(part), -step)
            link.arrived(number(part, "near", 0, direction), block(part, -step, 0), back)
            ref = block(part, -step, 0, direction)
            link.send(number(part, "far", 0, direction), ref, ref, place.beside(f_axis(part), step))
    for part in (0, 1):
        pass_on(part, -1)
        pass_on(part, 1)

    def relay(part, g):
        for direction, step in ((0, 1), (1, -1)):
            back = place.beside(s_axis(part), -step)
            link.arrived(number(part, "near2", g, direction), block(part, g, -step), back)
            ref = block(part, g, -step, direction)
            link.send(number(part, "far2", g, direction), ref, ref, place.beside(s_axis(part), step))

    def last(g):
        for part in (0, 1):
            for direction, step in ((0, 1), (1, -1)):
                back = place.beside(s_axis(part), -step)
                link.arrived(number(part, "far2", g, direction), block(part, g, 2, direction), back)

    def use(part, along_z):
        if seen is not None:
            seen(part, along_z)

    for part in (0, 1):
        relay(part, 0)
    for part in (0, 1):
        for direction, step in ((0, 1), (1, -1)):
            back = place.beside(f_axis(part), -step)
            link.arrived(number(part, "far", 0, direction), block(part, 2, 0, direction), back)
        pass_on(part, 2)
    use(0, 0)
    for g in (-1, 1):
        for part in (0, 1):
            relay(part, g)
    last(0)
    use(1, 0)
    for part in (0, 1):
        relay(part, 2)
    use(0, -1)
    use(0, 1)
    for g in (-1, 1):
        last(g)
    use(1, -1)
    use(1, 1)
    last(2)
    use(0, 2)
    use(1, 2)


def attention_kernel(
    queries,
    keys,
    values,
    w_out,
    resid,
    hres,
    squares,
    all_keys,
    all_values,
    attn,
    given,
    got_core,
    kept,
    got,
    stats,
    send_sem,
    recv_sem,
):
    place = Place()
    link = Link(send_sem, recv_sem)
    barrier = pltpu.get_barrier_semaphore()
    diagonal = place.ctx == place.tp
    members = [place.member_peer(step) for step in range(1, 16)]
    greeted = place.greet(members)

    @pl.when(diagonal)
    def _():
        pl.semaphore_wait(barrier, greeted)

    @pl.when(jnp.logical_not(diagonal))
    def _():
        pl.semaphore_signal(barrier, inc=1, device_id=place.mirror(), device_id_type=MESH_ID)
        pl.semaphore_wait(barrier, greeted + 1)

    def at(x, z):
        return ((z // 2) * 4 + x) * 2 + lax.rem(z, 2)

    here = place.ctx * 2 + place.zl
    mine = pl.ds(pl.multiple_of(place.zl * 128, 128), 128)
    all_keys[here] = keys[mine, :]
    all_values[here] = values[mine, :]

    def key_block(x, z, part, half):
        ref = (all_keys, all_values)[part]
        if half is None:
            return ref.at[at(x, z)]
        return ref.at[at(x, z), pl.ds(half * 64, 64)]

    plane_gather(place, link, key_block)

    def attend(part):
        @pl.loop(part * 3, part * 3 + 3)
        def _(head):
            columns = pl.ds(pl.multiple_of(head * HD, HD), HD)
            scores = lax.dot_general(
                queries[mine, columns],
                all_keys[...].reshape(2048, HD),
                (((1,), (1,)), ((), ())),
                preferred_element_type=F32,
            ) * HD ** (-0.5)
            query_pos = here * 128 + lax.broadcasted_iota(jnp.int32, (128, 2048), 0)
            key_pos = lax.broadcasted_iota(jnp.int32, (128, 2048), 1)
            scores = jnp.where(key_pos <= query_pos, scores, -1e30)
            probs = jnp.exp(scores - jnp.max(scores, axis=1, keepdims=True))
            denom = jnp.sum(probs, axis=1, keepdims=True)
            update = jnp.dot(
                probs.astype(BF16), all_values[...].reshape(2048, HD), preferred_element_type=F32
            )
            attn[here, :, columns] = (update / denom).astype(BF16)

    def attn_block(x, z, part, half):
        columns = pl.ds(part * 384, 384)
        if half is None:
            return attn.at[at(x, z), :, columns]
        return attn.at[at(x, z), pl.ds(half * 64, 64), columns]

    plane_gather(place, link, attn_block, first=40, ready=attend)

    def project(ctx):
        rows = attn[pl.ds(ctx * 2, 2)].reshape(256, 768)
        return jnp.dot(rows, w_out[...], preferred_element_type=F32)

    partner = {"core": 1 - place.core}
    order = [wrapped(place.y + step) for step in (2, 1, -1, 0)]
    for i, j in enumerate(order):
        given[i] = project(2 * j + 1 - place.core).astype(BF16)
        link.send(80 + i, given.at[i], got_core.at[i], partner)
    for i, j in enumerate(order):
        total = project(2 * j + place.core)
        link.arrived(80 + i, got_core.at[i], partner)
        total = total + got_core[i].astype(F32)
        if i < 3:
            kept[i] = total.astype(BF16)
            link.send(84 + i, kept.at[i], got.at[i], {"y": j})
    for i, step in enumerate((2, 1, -1)):
        link.arrived(84 + i, got.at[i], {"y": wrapped(place.y - step)})
        total = total + got[i].astype(F32)
    kept[3] = total.astype(BF16)
    move = link.copy(87, kept.at[3], got.at[3], place.mirror())

    @pl.when(diagonal)
    def _():
        got[3] = kept[3]

    @pl.when(jnp.logical_not(diagonal))
    def _():
        move.start()
        link.arrived(87, got.at[3], place.mirror())

    total = resid[...].astype(F32) + got[3].astype(F32)
    value = total.astype(BF16)
    hres[...] = value
    value = value.astype(F32)
    sums = lax.dot_general(
        jnp.ones((8, 384), F32),
        value * value,
        (((1,), (1,)), ((), ())),
        precision=lax.Precision.HIGHEST,
        preferred_element_type=F32,
    )
    stats[place.member] = sums
    for step in range(1, 16):
        link.send(92 + step, stats.at[place.member], stats.at[place.member], members[step - 1])
    for step in range(1, 16):
        source = lax.rem(place.member + 16 - step, 16)
        link.arrived(92 + step, stats.at[source], members[15 - step])
    squares[...] = jnp.sum(stats[...], axis=0)
    link.finish()

    @pl.when(jnp.logical_not(diagonal))
    def _():
        move.wait_send()


def attention(queries, keys, values, w_out, resid):
    vmem = pl.BlockSpec(memory_space=pltpu.VMEM)
    return pl.pallas_call(
        attention_kernel,
        out_shape=(jax.ShapeDtypeStruct((256, 384), BF16), jax.ShapeDtypeStruct((8, 256), F32)),
        in_specs=[vmem] * 5,
        out_specs=(vmem, vmem),
        scratch_shapes=[
            pltpu.VMEM((16, 128, HD), BF16),
            pltpu.VMEM((16, 128, HD), BF16),
            pltpu.VMEM((16, 128, 768), BF16),
            pltpu.VMEM((4, 256, 384), BF16),
            pltpu.VMEM((4, 256, 384), BF16),
            pltpu.VMEM((4, 256, 384), BF16),
            pltpu.VMEM((4, 256, 384), BF16),
            pltpu.VMEM((16, 8, 256), F32),
            pltpu.SemaphoreType.DMA((108,)),
            pltpu.SemaphoreType.DMA((108,)),
        ],
        compiler_params=pltpu.CompilerParams(
            collective_id=0, has_side_effects=True, vmem_limit_bytes=48 * 1024 * 1024
        ),
        name="attention",
    )(queries, keys, values, w_out, resid)


def experts_kernel(
    slots,
    w_gate,
    w_up,
    w_down,
    out,
    rows,
    gate_w,
    up_w,
    down_w,
    gate_acc,
    up_acc,
    hidden,
    partial,
    got_half,
    got_part,
    result,
    returned,
    load_sem,
    send_sem,
    recv_sem,
):
    place = Place()
    link = Link(send_sem, recv_sem)
    loads = [
        pltpu.make_async_copy(src, dst, load_sem.at[i])
        for i, (src, dst) in enumerate(((w_gate, gate_w), (w_up, up_w), (w_down, down_w)))
    ]
    loads[0].start()
    loads[1].start()
    greeted = place.greet([place.tp_peer(step) for step in range(1, 8)])
    pl.semaphore_wait(pltpu.get_barrier_semaphore(), greeted)

    base = 80
    for step in range(1, 8):
        target = lax.rem(place.tp + step, 8)
        link.send(base + step, slots.at[target], rows.at[place.x, place.z, place.tp], place.tp_peer(step))
    rows[place.x, place.z, place.tp] = slots[place.tp]
    for step in range(1, 8):
        source = lax.rem(place.tp + 8 - step, 8)
        link.arrived(base + step, rows.at[place.x, place.z, source], place.tp_peer(8 - step))

    def block_of_rows(x, z, part, half):
        if half is None:
            return rows.at[x, z, pl.ds(part * 4, 4)]
        return rows.at[x, z, pl.ds(part * 4 + half * 2, 2)]

    gate_acc[...] = jnp.zeros_like(gate_acc)
    up_acc[...] = jnp.zeros_like(up_acc)

    def use_rows(part, along_z):
        if (part, along_z) == (0, 0):
            loads[0].wait()
            loads[1].wait()
            loads[2].start()
        z = wrapped(place.z + along_z)
        zh, e = z // 2, lax.rem(z, 2)

        @pl.loop(part * 2, part * 2 + 2)
        def _(pair):
            left = jnp.concatenate([rows[:, z, 2 * pair + i].reshape(384, 384) for i in range(2)], axis=1)
            spans = [pl.ds(pl.multiple_of((4 * pair + 2 * i + e) * 384, 384), 384) for i in range(2)]
            for acc, weights in ((gate_acc, gate_w), (up_acc, up_w)):
                right = jnp.concatenate([weights[span, :] for span in spans], axis=0)
                acc[zh] += jnp.dot(left, right, preferred_element_type=F32)

    plane_gather(place, link, block_of_rows, seen=use_rows)
    for zh in range(2):
        gate = gate_acc[zh]
        value = gate / (1.0 + jnp.exp(-gate)) * up_acc[zh]
        hidden[pl.ds(zh * 4, 4)] = value.astype(BF16).reshape(4, 96, 512)
    loads[2].wait()

    def compute(part, g):
        if part == 0:
            x = wrapped(place.x + g)
            left = jnp.concatenate([hidden[x], hidden[4 + x]], axis=0)

            @pl.loop(0, 4)
            def _(t):
                right = down_w[:, pl.ds(pl.multiple_of(t * 768, 768), 768)]
                both = jnp.dot(left, right, preferred_element_type=F32).astype(BF16)
                for zh in range(2):
                    for e in range(2):
                        partial[x, zh * 2 + e, t] = both[zh * 96 : zh * 96 + 96, e * 384 : e * 384 + 384]
        else:
            z = wrapped(place.z + g)
            left = hidden[pl.ds((z // 2) * 4, 4)].reshape(384, 512)

            @pl.loop(4, 8)
            def _(t):
                start = (2 * t + lax.rem(z, 2)) * 384
                right = down_w[:, pl.ds(pl.multiple_of(start, 384), 384)]
                both = jnp.dot(left, right, preferred_element_type=F32).astype(BF16)
                partial[:, z, t] = both.reshape(4, 96, 384)

    def block(part, along_f, along_s):
        x, z = (along_f, along_s) if part == 0 else (along_s, along_f)
        return wrapped(place.x + x), wrapped(place.z + z)

    def half_of(where, part, half):
        return partial.at[where[0], where[1], pl.ds(part * 4 + half * 2, 2)]

    def part_of(where, part):
        return partial.at[where[0], where[1], pl.ds(part * 4, 4)]

    def add(target, *sources):
        total = target[...].astype(F32)
        for source in sources:
            total = total + source[...].astype(F32)
        target[...] = total.astype(BF16)

    class Ring:
        def __init__(self, part, stage, axis, at):
            self.part, self.stage, self.axis, self.at = part, stage, axis, at
            self.number = 100 + (part * 5 + stage) * 4

        def far(self):
            for direction, step in ((0, 1), (1, -1)):
                link.send(
                    self.number + direction,
                    half_of(self.at(2), self.part, direction),
                    got_half.at[self.part, self.stage, direction],
                    place.beside(self.axis, step),
                )

        def near(self):
            for direction, step in ((0, 1), (1, -1)):
                got = got_half.at[self.part, self.stage, direction]
                link.arrived(self.number + direction, got, place.beside(self.axis, -step))
                add(half_of(self.at(step), self.part, direction), got)
                link.send(
                    self.number + 2 + direction,
                    part_of(self.at(step), self.part),
                    got_part.at[self.part, self.stage, direction],
                    place.beside(self.axis, step),
                )

        def receive(self):
            gots = []
            for direction, step in ((0, 1), (1, -1)):
                got = got_part.at[self.part, self.stage, direction]
                link.arrived(self.number + 2 + direction, got, place.beside(self.axis, -step))
                gots.append(got)
            return gots

        def end(self):
            add(part_of(self.at(0), self.part), *self.receive())

    outer = [
        {
            g: Ring(part, FAR_FIRST.index(g), "zx"[part], lambda step, part=part, g=g: block(part, g, step))
            for g in FAR_FIRST
        }
        for part in (0, 1)
    ]
    inner = [Ring(part, 4, "xz"[part], lambda step, part=part: block(part, step, 0)) for part in (0, 1)]
    for g in FAR_FIRST:
        for part in (0, 1):
            compute(part, g)
            outer[part][g].far()
    for g in (2, 1, -1):
        for part in (0, 1):
            outer[part][g].near()
    for part in (0, 1):
        outer[part][2].end()
        inner[part].far()
    for part in (0, 1):
        outer[part][0].near()
    for part in (0, 1):
        outer[part][1].end()
        outer[part][-1].end()
        inner[part].near()
    base = 88
    for part in (0, 1):
        outer[part][0].end()
        gots = inner[part].receive()
        total = part_of(inner[part].at(0), part)[...].astype(F32)
        for got in gots:
            total = total + got[...].astype(F32)
        result[pl.ds(part * 4, 4)] = total.astype(BF16)
    for step in range(1, 8):
        target = lax.rem(place.tp + step, 8)
        link.send(base + step, result.at[target], returned.at[place.tp], place.tp_peer(step))
    returned[place.tp] = result[place.tp]
    for step in range(1, 8):
        source = lax.rem(place.tp + 8 - step, 8)
        link.arrived(base + step, returned.at[source], place.tp_peer(8 - step))
    link.finish()
    out[...] = returned[...]


def experts(slots, w_gate, w_up, w_down):
    copies = 140
    return pl.pallas_call(
        experts_kernel,
        out_shape=jax.ShapeDtypeStruct((8, 96, 384), BF16),
        in_specs=[pl.BlockSpec(memory_space=pltpu.VMEM)] + [pl.BlockSpec(memory_space=pl.ANY)] * 3,
        out_specs=pl.BlockSpec(memory_space=pltpu.VMEM),
        scratch_shapes=[
            pltpu.VMEM((4, 4, 8, 96, 384), BF16),
            pltpu.VMEM((6144, 512), BF16),
            pltpu.VMEM((6144, 512), BF16),
            pltpu.VMEM((512, 6144), BF16),
            pltpu.VMEM((2, 384, 512), F32),
            pltpu.VMEM((2, 384, 512), F32),
            pltpu.VMEM((8, 96, 512), BF16),
            pltpu.VMEM((4, 4, 8, 96, 384), BF16),
            pltpu.VMEM((2, 5, 2, 2, 96, 384), BF16),
            pltpu.VMEM((2, 5, 2, 4, 96, 384), BF16),
            pltpu.VMEM((8, 96, 384), BF16),
            pltpu.VMEM((8, 96, 384), BF16),
            pltpu.SemaphoreType.DMA((3,)),
            pltpu.SemaphoreType.DMA((copies,)),
            pltpu.SemaphoreType.DMA((copies,)),
        ],
        compiler_params=pltpu.CompilerParams(
            collective_id=1, has_side_effects=True, vmem_limit_bytes=64 * 1024 * 1024 - 128 * 1024
        ),
        name="experts",
    )(slots, w_gate, w_up, w_down)


def on_device(
    resid, queries, keys, values, w_out, norm_gain, w_gate, w_up, w_down, expert_ids, route_units
):
    tp_size = lax.axis_size(TP)
    tok_rows = queries.shape[0]
    feat_dev = resid.shape[1]
    capacity = 3 * tok_rows // tp_size
    hres, squares = attention(queries, keys, values, w_out, resid)
    hfloat = hres.astype(jnp.float32)
    square_total = squares[0][:, None]
    normed = (hfloat * lax.rsqrt(square_total / D + 1e-05) * norm_gain.astype(jnp.float32)).astype(
        jnp.bfloat16
    )
    onehot = (expert_ids[..., None] == jnp.arange(tp_size, dtype=jnp.int32)).astype(jnp.int32)
    per_token = jnp.sum(onehot, axis=1)
    earlier = jnp.cumsum(per_token, axis=0) - per_token
    slot = jnp.sum(onehot * earlier[:, None, :], axis=-1)
    codes = expert_ids * capacity + slot
    slot_ids = jnp.arange(tp_size * capacity, dtype=jnp.int32)
    picks = (
        (slot_ids[:, None] == codes[None, :, 0]) | (slot_ids[:, None] == codes[None, :, 1])
    ).astype(jnp.bfloat16)
    dispatched = jnp.dot(picks, normed, preferred_element_type=jnp.float32).astype(jnp.bfloat16)
    returned = experts(dispatched.reshape(tp_size, capacity, feat_dev), w_gate[0], w_up[0], w_down[0])
    units = route_units.astype(jnp.float32)
    weights = (units / jnp.sum(units, axis=-1, keepdims=True)).astype(jnp.bfloat16)
    combine = jnp.where(slot_ids[None, :] == codes[:, 0:1], weights[:, 0:1], 0.0) + jnp.where(
        slot_ids[None, :] == codes[:, 1:2], weights[:, 1:2], 0.0
    )
    moe = jnp.dot(
        combine, returned.reshape(tp_size * capacity, feat_dev), preferred_element_type=jnp.float32
    )
    return (hfloat + moe).astype(jnp.bfloat16)


def solution(mesh):
    torus = Mesh(mesh.devices.reshape(2, 4, 4, 2, 2), ("zh", "x", "y", "core", "zl"))
    in_specs = (
        P(CTX, TP_EP),
        P(CTX, TP),
        P(CTX, TP),
        P(CTX, TP),
        P(TP, ("zh", "x", "zl")),
        P(TP_EP),
        P(TP, None, ("zh", "x", "zl")),
        P(TP, None, ("zh", "x", "zl")),
        P(TP, ("zh", "x", "zl"), None),
        P(CTX, None),
        P(CTX, None),
    )
    return jax.shard_map(
        on_device, mesh=torus, in_specs=in_specs, out_specs=P(CTX, TP_EP), check_vma=False
    )
```

```python
import jax
import jax.numpy as jnp
from jax import lax
from jax.experimental import pallas as pl
from jax.experimental.pallas import tpu as pltpu
from jax.sharding import Mesh
from jax.sharding import PartitionSpec as P

D = 6144
HD = 128
CTX = ("zh", "x")
TP = ("y", "core")
TP_EP = ("y", "core", "zl")
MESH_ID = pl.DeviceIdType.MESH
F32 = jnp.float32
BF16 = jnp.bfloat16
FAR_FIRST = (2, 1, -1, 0)


def wrapped(index, size=4):
    return lax.rem(index + size, size)


class Place:
    def __init__(self):
        self.x = lax.axis_index("x")
        self.z = lax.axis_index("zh") * 2 + lax.axis_index("zl")
        self.y = lax.axis_index("y")
        self.core = lax.axis_index("core")
        self.zl = lax.axis_index("zl")
        self.tp = self.y * 2 + self.core
        self.ctx = lax.axis_index("zh") * 4 + self.x
        self.member = self.tp * 2 + self.zl

    def beside(self, axis, step):
        if axis == "x":
            return {"x": wrapped(self.x + step)}
        z = wrapped(self.z + step)
        return {"zh": z // 2, "zl": lax.rem(z, 2)}

    def tp_peer(self, step):
        other = lax.rem(self.tp + step, 8)
        return {"y": other // 2, "core": lax.rem(other, 2)}

    def member_peer(self, step):
        other = lax.rem(self.member + step, 16)
        return {"y": other // 4, "core": lax.rem(other // 2, 2), "zl": lax.rem(other, 2)}

    def mirror(self):
        return {"zh": self.tp // 4, "x": lax.rem(self.tp, 4), "y": self.ctx // 2, "core": lax.rem(self.ctx, 2)}

    def greet(self, peers):
        barrier = pltpu.get_barrier_semaphore()
        peers = [self.beside(axis, step) for axis in ("x", "z") for step in (1, -1)] + peers
        for peer in peers:
            pl.semaphore_signal(barrier, inc=1, device_id=peer, device_id_type=MESH_ID)
        return len(peers)


class Link:
    def __init__(self, send_sem, recv_sem):
        self.send_sem, self.recv_sem, self.open = send_sem, recv_sem, []

    def copy(self, number, src, dst, device, landing=None):
        return pltpu.make_async_remote_copy(
            src_ref=src,
            dst_ref=dst,
            send_sem=self.send_sem.at[number],
            recv_sem=self.recv_sem.at[number if landing is None else landing],
            device_id=device,
            device_id_type=MESH_ID,
        )

    def send(self, number, src, dst, device, landing=None):
        copy = self.copy(number, src, dst, device, landing)
        copy.start()
        self.open.append(copy)

    def arrived(self, number, dst, device):
        self.copy(number, dst, dst, device).wait_recv()

    def finish(self):
        for copy in self.open:
            copy.wait_send()
        self.open = []


GATHER_COPIES = 40


def plane_gather(place, link, piece, first=0, ready=None, seen=None, busy=None):
    here = (place.x, place.z)

    def block(part, along_f, along_s, half=None):
        f, s = (here[0], here[1]) if part == 0 else (here[1], here[0])
        f, s = wrapped(f + along_f), wrapped(s + along_s)
        return piece(f, s, part, half) if part == 0 else piece(s, f, part, half)

    def f_axis(part):
        return "xz"[part]

    def s_axis(part):
        return "zx"[part]

    def number(part, kind, g, direction):
        base = {"near": 0, "far": 2, "near2": 4, "far2": 12}[kind]
        return first + part * 20 + base + (FAR_FIRST.index(g) * 2 if kind in ("near2", "far2") else 0) + direction

    def pass_on(part, g):
        ref = block(part, g, 0)
        for direction, step in ((0, 1), (1, -1)):
            link.send(number(part, "near2", g, direction), ref, ref, place.beside(s_axis(part), step))

    for part in (0, 1):
        if ready is not None:
            ready(part)
        ref = block(part, 0, 0)
        for direction, step in ((0, 1), (1, -1)):
            link.send(number(part, "near", 0, direction), ref, ref, place.beside(f_axis(part), step))
        if ready is not None:
            pass_on(part, 0)
    if ready is None:
        for part in (0, 1):
            pass_on(part, 0)
    if busy is not None:
        busy()
    for part in (0, 1):
        for direction, step in ((0, 1), (1, -1)):
            back = place.beside(f_axis(part), -step)
            link.arrived(number(part, "near", 0, direction), block(part, -step, 0), back)
            ref = block(part, -step, 0, direction)
            link.send(number(part, "far", 0, direction), ref, ref, place.beside(f_axis(part), step))
    for part in (0, 1):
        pass_on(part, -1)
        pass_on(part, 1)

    def relay(part, g):
        for direction, step in ((0, 1), (1, -1)):
            back = place.beside(s_axis(part), -step)
            link.arrived(number(part, "near2", g, direction), block(part, g, -step), back)
            ref = block(part, g, -step, direction)
            link.send(number(part, "far2", g, direction), ref, ref, place.beside(s_axis(part), step))

    def last(g):
        for part in (0, 1):
            for direction, step in ((0, 1), (1, -1)):
                back = place.beside(s_axis(part), -step)
                link.arrived(number(part, "far2", g, direction), block(part, g, 2, direction), back)

    def use(part, along_z):
        if seen is not None:
            seen(part, along_z)

    for part in (0, 1):
        relay(part, 0)
    for part in (0, 1):
        for direction, step in ((0, 1), (1, -1)):
            back = place.beside(f_axis(part), -step)
            link.arrived(number(part, "far", 0, direction), block(part, 2, 0, direction), back)
        pass_on(part, 2)
    use(0, 0)
    for g in (-1, 1):
        for part in (0, 1):
            relay(part, g)
    last(0)
    use(1, 0)
    for part in (0, 1):
        relay(part, 2)
    use(0, -1)
    use(0, 1)
    for g in (-1, 1):
        last(g)
    use(1, -1)
    use(1, 1)
    last(2)
    use(0, 2)
    use(1, 2)


def layer_kernel(
    resid_hbm,
    queries_hbm,
    keys_hbm,
    values_hbm,
    w_out_hbm,
    gain_hbm,
    w_gate,
    w_up,
    w_down,
    ids_hbm,
    units_hbm,
    out,
    resid,
    queries,
    keys,
    values,
    w_out,
    ids,
    units,
    all_keys,
    all_values,
    gains,
    picks,
    combine,
    hres,
    slots,
    rows,
    gate_w,
    up_w,
    down_w,
    row_squares,
    gate_acc,
    up_acc,
    hidden,
    partial,
    got_half,
    got_part,
    result,
    returned,
    load_sem,
    send_sem,
    recv_sem,
):
    place = Place()
    link = Link(send_sem, recv_sem)
    pieces = Link(send_sem, recv_sem)
    pairs = (
        (keys_hbm, keys),
        (values_hbm, values),
        (queries_hbm, queries),
        (gain_hbm, gains.at[place.member]),
        (ids_hbm, ids),
        (units_hbm, units),
        (w_out_hbm, w_out),
        (resid_hbm, resid),
        (w_down, down_w),
        (w_gate, gate_w),
        (w_up, up_w),
    )
    loads = [pltpu.make_async_copy(src, dst, load_sem.at[i]) for i, (src, dst) in enumerate(pairs)]
    for load in loads[:9]:
        load.start()
    barrier = pltpu.get_barrier_semaphore()
    diagonal = place.ctx == place.tp
    members = [place.member_peer(step) for step in range(1, 16)]
    greeted = place.greet(members)
    for load in loads[:2]:
        load.wait()

    here = place.ctx * 2 + place.zl
    mine = pl.ds(pl.multiple_of(place.zl * 128, 128), 128)
    all_keys[here] = keys[mine, :]
    all_values[here] = values[mine, :]

    @pl.when(diagonal)
    def _():
        pl.semaphore_wait(barrier, greeted)

    @pl.when(jnp.logical_not(diagonal))
    def _():
        pl.semaphore_signal(barrier, inc=1, device_id=place.mirror(), device_id_type=MESH_ID)
        pl.semaphore_wait(barrier, greeted + 1)

    def at(x, z):
        return ((z // 2) * 4 + x) * 2 + lax.rem(z, 2)

    def key_block(x, z, part, half):
        ref = (all_keys, all_values)[part]
        if half is None:
            return ref.at[at(x, z)]
        return ref.at[at(x, z), pl.ds(half * 64, 64)]

    def route():
        loads[3].wait()
        for step in range(1, 16):
            ref = gains.at[place.member]
            link.send(88 + step, ref, ref, members[step - 1])
        loads[4].wait()
        loads[5].wait()
        lanes = lax.broadcasted_iota(jnp.int32, (256, 128), 1)
        named = [ids[:, k : k + 1] == lanes for k in range(2)]
        tokens = jnp.where(named[0] | named[1], 1.0, 0.0).astype(BF16)
        row = lax.broadcasted_iota(jnp.int32, (256, 256), 0)
        column = lax.broadcasted_iota(jnp.int32, (256, 256), 1)
        before = jnp.where(column < row, 1.0, 0.0).astype(BF16)
        earlier = jnp.dot(before, tokens, preferred_element_type=F32)
        amounts = units[...].astype(F32)
        weights = (amounts / jnp.sum(amounts, axis=1, keepdims=True)).astype(BF16).astype(F32)
        slot_ids = lax.broadcasted_iota(jnp.int32, (256, 768), 1).astype(F32)
        hits = []
        for k in range(2):
            slot = jnp.sum(jnp.where(named[k], earlier, 0.0), axis=1, keepdims=True)
            code = ids[:, k : k + 1].astype(F32) * 96.0 + slot
            hits.append(slot_ids == code)
        picks[...] = jnp.where(hits[0] | hits[1], 1.0, 0.0).astype(BF16)
        combine[...] = (
            jnp.where(hits[0], weights[:, 0:1], 0.0) + jnp.where(hits[1], weights[:, 1:2], 0.0)
        ).astype(BF16)

    plane_gather(place, link, key_block, busy=route)
    loads[2].wait()

    def attn_rows(part, block, start, count):
        return pl.ds(pl.multiple_of(part * 2048 + block * 128 + start, 64), count), pl.ds(0, 384)

    def attend(part):
        @pl.loop(0, 3)
        def _(i):
            columns = pl.ds(pl.multiple_of((part * 3 + i) * HD, HD), HD)
            scores = lax.dot_general(
                queries[mine, columns],
                all_keys[...].reshape(2048, HD),
                (((1,), (1,)), ((), ())),
                preferred_element_type=F32,
            ) * HD ** (-0.5)
            query_pos = here * 128 + lax.broadcasted_iota(jnp.int32, (128, 2048), 0)
            key_pos = lax.broadcasted_iota(jnp.int32, (128, 2048), 1)
            scores = jnp.where(key_pos <= query_pos, scores, -1e30)
            probs = jnp.exp(scores - jnp.max(scores, axis=1, keepdims=True))
            denom = jnp.sum(probs, axis=1, keepdims=True)
            update = jnp.dot(
                probs.astype(BF16), all_values[...].reshape(2048, HD), preferred_element_type=F32
            )
            where = attn_rows(part, here, 0, 128)[0]
            gate_w[where, pl.ds(pl.multiple_of(i * HD, HD), HD)] = (update / denom).astype(BF16)

    def attn_block(x, z, part, half):
        if half is None:
            return gate_w.at[attn_rows(part, at(x, z), 0, 128)]
        return gate_w.at[attn_rows(part, at(x, z), half * 64, 64)]

    plane_gather(place, link, attn_block, first=40, ready=attend)

    loads[6].wait()

    def project(ctx):
        total = None
        for part in (0, 1):
            term = jnp.dot(
                gate_w[pl.ds(pl.multiple_of(part * 2048 + ctx * 256, 256), 256), pl.ds(0, 384)],
                w_out[pl.ds(part * 384, 384), :],
                preferred_element_type=F32,
            )
            total = term if total is None else total + term
        return total

    def piece(k):
        return up_w.at[pl.ds(k * 256, 256), pl.ds(0, 384)]

    partner = {"core": 1 - place.core}
    order = [wrapped(place.y + step) for step in (2, 1, -1, 0)]
    for i, j in enumerate(order):
        piece(i)[...] = project(2 * j + 1 - place.core).astype(BF16)
        pieces.send(80 + i, piece(i), piece(4 + i), partner)
    for i, j in enumerate(order):
        total = project(2 * j + place.core)
        pieces.arrived(80 + i, piece(4 + i), partner)
        total = total + piece(4 + i)[...].astype(F32)
        if i < 3:
            piece(8 + i)[...] = total.astype(BF16)
            pieces.send(84 + i, piece(8 + i), piece(12 + i), {"y": j})
    link.finish()
    loads[9].start()
    for i, step in enumerate((2, 1, -1)):
        pieces.arrived(84 + i, piece(12 + i), {"y": wrapped(place.y - step)})
        total = total + piece(12 + i)[...].astype(F32)
    piece(11)[...] = total.astype(BF16)
    move = pieces.copy(87, piece(11), piece(15), place.mirror())

    @pl.when(diagonal)
    def _():
        piece(15)[...] = piece(11)[...]

    @pl.when(jnp.logical_not(diagonal))
    def _():
        move.start()
        pieces.arrived(87, piece(15), place.mirror())

    loads[7].wait()
    hres[...] = (resid[...].astype(F32) + piece(15)[...].astype(F32)).astype(BF16)
    dispatched = lax.dot_general(
        picks[...], hres[...], (((0,), (0,)), ((), ())), preferred_element_type=F32
    ).astype(BF16)
    slots[...] = dispatched.reshape(8, 96, 384)

    base = 104
    for step in range(1, 8):
        target = lax.rem(place.tp + step, 8)
        link.send(base + step, slots.at[target], rows.at[place.x, place.z, place.tp], place.tp_peer(step))
    rows[place.x, place.z, place.tp] = slots[place.tp]

    @pl.when(jnp.logical_not(diagonal))
    def _():
        move.wait_send()

    pieces.finish()
    loads[10].start()
    gate_acc[...] = jnp.zeros_like(gate_acc)
    up_acc[...] = jnp.zeros_like(up_acc)
    row_squares[...] = jnp.zeros_like(row_squares)
    for step in range(1, 16):
        source = lax.rem(place.member + 16 - step, 16)
        link.arrived(88 + step, gains.at[source], members[15 - step])
    for step in range(1, 8):
        source = lax.rem(place.tp + 8 - step, 8)
        link.arrived(base + step, rows.at[place.x, place.z, source], place.tp_peer(8 - step))

    def block_of_rows(x, z, part, half):
        if half is None:
            return rows.at[x, z, pl.ds(part * 4, 4)]
        return rows.at[x, z, pl.ds(part * 4 + half * 2, 2)]

    def use_rows(part, along_z):
        if (part, along_z) == (0, 0):
            loads[9].wait()
            loads[10].wait()
        z = wrapped(place.z + along_z)
        zh, e = z // 2, lax.rem(z, 2)

        @pl.loop(part * 2, part * 2 + 2)
        def _(pair):
            lefts = []
            squares = row_squares[zh]
            for i in range(2):
                t = 2 * pair + i
                value = rows[:, z, t].reshape(384, 384).astype(F32)
                lefts.append((value * gains[2 * t + e, 0:1, :]).astype(BF16))
                square = value * value
                squares = squares + square[:, 0:128] + square[:, 128:256] + square[:, 256:384]
            row_squares[zh] = squares
            left = jnp.concatenate(lefts, axis=1)
            spans = [pl.ds(pl.multiple_of((4 * pair + 2 * i + e) * 384, 384), 384) for i in range(2)]
            for acc, weights in ((gate_acc, gate_w), (up_acc, up_w)):
                right = jnp.concatenate([weights[span, :] for span in spans], axis=0)
                acc[zh] += jnp.dot(left, right, preferred_element_type=F32)

    plane_gather(place, link, block_of_rows, first=112, seen=use_rows)
    for zh in range(2):
        mean = jnp.sum(row_squares[zh], axis=1, keepdims=True) / D
        scale = lax.rsqrt(mean + 1e-05)
        gate = gate_acc[zh] * scale
        value = gate / (1.0 + jnp.exp(-gate)) * (up_acc[zh] * scale)
        hidden[pl.ds(zh * 4, 4)] = value.astype(BF16).reshape(4, 96, 512)
    loads[8].wait()

    def compute(part, g):
        if part == 0:
            x = wrapped(place.x + g)
            left = jnp.concatenate([hidden[x], hidden[4 + x]], axis=0)

            @pl.loop(0, 4)
            def _(t):
                right = down_w[:, pl.ds(pl.multiple_of(t * 768, 768), 768)]
                both = jnp.dot(left, right, preferred_element_type=F32).astype(BF16)
                for zh in range(2):
                    for e in range(2):
                        partial[x, zh * 2 + e, t] = both[zh * 96 : zh * 96 + 96, e * 384 : e * 384 + 384]
        else:
            z = wrapped(place.z + g)
            left = hidden[pl.ds((z // 2) * 4, 4)].reshape(384, 512)

            @pl.loop(4, 8)
            def _(t):
                start = (2 * t + lax.rem(z, 2)) * 384
                right = down_w[:, pl.ds(pl.multiple_of(start, 384), 384)]
                both = jnp.dot(left, right, preferred_element_type=F32).astype(BF16)
                partial[:, z, t] = both.reshape(4, 96, 384)

    def block(part, along_f, along_s):
        x, z = (along_f, along_s) if part == 0 else (along_s, along_f)
        return wrapped(place.x + x), wrapped(place.z + z)

    def half_of(where, part, half):
        return partial.at[where[0], where[1], pl.ds(part * 4 + half * 2, 2)]

    def part_of(where, part):
        return partial.at[where[0], where[1], pl.ds(part * 4, 4)]

    def add(target, *sources):
        total = target[...].astype(F32)
        for source in sources:
            total = total + source[...].astype(F32)
        target[...] = total.astype(BF16)

    class Ring:
        def __init__(self, part, stage, axis, at):
            self.part, self.stage, self.axis, self.at = part, stage, axis, at
            self.number = 152 + (part * 5 + stage) * 4

        def far(self):
            for direction, step in ((0, 1), (1, -1)):
                link.send(
                    self.number + direction,
                    half_of(self.at(2), self.part, direction),
                    got_half.at[self.part, self.stage, direction],
                    place.beside(self.axis, step),
                )

        def near(self):
            for direction, step in ((0, 1), (1, -1)):
                got = got_half.at[self.part, self.stage, direction]
                link.arrived(self.number + direction, got, place.beside(self.axis, -step))
                add(half_of(self.at(step), self.part, direction), got)
                link.send(
                    self.number + 2 + direction,
                    part_of(self.at(step), self.part),
                    got_part.at[self.part, self.stage, direction],
                    place.beside(self.axis, step),
                )

        def receive(self):
            gots = []
            for direction, step in ((0, 1), (1, -1)):
                got = got_part.at[self.part, self.stage, direction]
                link.arrived(self.number + 2 + direction, got, place.beside(self.axis, -step))
                gots.append(got)
            return gots

        def end(self):
            add(part_of(self.at(0), self.part), *self.receive())

    outer = [
        {
            g: Ring(part, FAR_FIRST.index(g), "zx"[part], lambda step, part=part, g=g: block(part, g, step))
            for g in FAR_FIRST
        }
        for part in (0, 1)
    ]
    inner = [Ring(part, 4, "xz"[part], lambda step, part=part: block(part, step, 0)) for part in (0, 1)]
    for g in FAR_FIRST:
        for part in (0, 1):
            compute(part, g)
            outer[part][g].far()
    for g in (2, 1, -1):
        for part in (0, 1):
            outer[part][g].near()
    for part in (0, 1):
        outer[part][2].end()
        inner[part].far()
    for part in (0, 1):
        outer[part][0].near()
    for part in (0, 1):
        outer[part][1].end()
        outer[part][-1].end()
        inner[part].near()
    base = 192
    for part in (0, 1):
        outer[part][0].end()
        gots = inner[part].receive()
        total = part_of(inner[part].at(0), part)[...].astype(F32)
        for got in gots:
            total = total + got[...].astype(F32)
        result[pl.ds(part * 4, 4)] = total.astype(BF16)
    for step in range(1, 8):
        target = lax.rem(place.tp + step, 8)
        link.send(base + step, result.at[target], returned.at[place.tp], place.tp_peer(step))
    returned[place.tp] = result[place.tp]
    for step in range(1, 8):
        source = lax.rem(place.tp + 8 - step, 8)
        link.arrived(base + step, returned.at[source], place.tp_peer(8 - step))
    link.finish()
    moe = jnp.dot(combine[...], returned[...].reshape(768, 384), preferred_element_type=F32)
    out[...] = (hres[...].astype(F32) + moe).astype(BF16)


def on_device(
    resid, queries, keys, values, w_out, norm_gain, w_gate, w_up, w_down, expert_ids, route_units
):
    gain = jnp.broadcast_to(norm_gain.astype(F32)[None], (8, norm_gain.shape[0]))
    copies = 200
    return pl.pallas_call(
        layer_kernel,
        out_shape=jax.ShapeDtypeStruct((256, 384), BF16),
        in_specs=[pl.BlockSpec(memory_space=pl.ANY)] * 11,
        out_specs=pl.BlockSpec(memory_space=pltpu.VMEM),
        scratch_shapes=[
            pltpu.VMEM((256, 384), BF16),
            pltpu.VMEM((256, 768), BF16),
            pltpu.VMEM((256, HD), BF16),
            pltpu.VMEM((256, HD), BF16),
            pltpu.VMEM((768, 384), BF16),
            pltpu.VMEM((256, 2), jnp.int32),
            pltpu.VMEM((256, 2), jnp.int32),
            pltpu.VMEM((16, 128, HD), BF16),
            pltpu.VMEM((16, 128, HD), BF16),
            pltpu.VMEM((16, 8, 384), F32),
            pltpu.VMEM((256, 768), BF16),
            pltpu.VMEM((256, 768), BF16),
            pltpu.VMEM((256, 384), BF16),
            pltpu.VMEM((8, 96, 384), BF16),
            pltpu.VMEM((4, 4, 8, 96, 384), BF16),
            pltpu.VMEM((6144, 512), BF16),
            pltpu.VMEM((6144, 512), BF16),
            pltpu.VMEM((512, 6144), BF16),
            pltpu.VMEM((2, 384, 128), F32),
            pltpu.VMEM((2, 384, 512), F32),
            pltpu.VMEM((2, 384, 512), F32),
            pltpu.VMEM((8, 96, 512), BF16),
            pltpu.VMEM((4, 4, 8, 96, 384), BF16),
            pltpu.VMEM((2, 5, 2, 2, 96, 384), BF16),
            pltpu.VMEM((2, 5, 2, 4, 96, 384), BF16),
            pltpu.VMEM((8, 96, 384), BF16),
            pltpu.VMEM((8, 96, 384), BF16),
            pltpu.SemaphoreType.DMA((11,)),
            pltpu.SemaphoreType.DMA((copies,)),
            pltpu.SemaphoreType.DMA((copies,)),
        ],
        compiler_params=pltpu.CompilerParams(
            collective_id=0, has_side_effects=True, vmem_limit_bytes=64 * 1024 * 1024 - 128 * 1024
        ),
        name="layer",
    )(
        resid, queries, keys, values, w_out, gain, w_gate[0], w_up[0], w_down[0], expert_ids, route_units
    )


def solution(mesh):
    torus = Mesh(mesh.devices.reshape(2, 4, 4, 2, 2), ("zh", "x", "y", "core", "zl"))
    in_specs = (
        P(CTX, TP_EP),
        P(CTX, TP),
        P(CTX, TP),
        P(CTX, TP),
        P(TP, ("zh", "x", "zl")),
        P(TP_EP),
        P(TP, None, ("zh", "x", "zl")),
        P(TP, None, ("zh", "x", "zl")),
        P(TP, ("zh", "x", "zl"), None),
        P(CTX, None),
        P(CTX, None),
    )
    return jax.shard_map(
        on_device, mesh=torus, in_specs=in_specs, out_specs=P(CTX, TP_EP), check_vma=False
    )
```

```python
import jax
import jax.numpy as jnp
from jax import lax
from jax.experimental import pallas as pl
from jax.experimental.pallas import tpu as pltpu
from jax.sharding import Mesh
from jax.sharding import PartitionSpec as P

D = 6144
HD = 128
CTX = ("zh", "x")
TP = ("y", "core")
TP_EP = ("y", "core", "zl")
MESH_ID = pl.DeviceIdType.MESH
F32 = jnp.float32
BF16 = jnp.bfloat16
FAR_FIRST = (2, 1, -1, 0)


def wrapped(index, size=4):
    return lax.rem(index + size, size)


class Place:
    def __init__(self):
        self.x = lax.axis_index("x")
        self.z = lax.axis_index("zh") * 2 + lax.axis_index("zl")
        self.y = lax.axis_index("y")
        self.core = lax.axis_index("core")
        self.zl = lax.axis_index("zl")
        self.tp = self.y * 2 + self.core
        self.ctx = lax.axis_index("zh") * 4 + self.x
        self.member = self.tp * 2 + self.zl

    def beside(self, axis, step):
        if axis == "x":
            return {"x": wrapped(self.x + step)}
        z = wrapped(self.z + step)
        return {"zh": z // 2, "zl": lax.rem(z, 2)}

    def tp_peer(self, step):
        other = lax.rem(self.tp + step, 8)
        return {"y": other // 2, "core": lax.rem(other, 2)}

    def member_peer(self, step):
        other = lax.rem(self.member + step, 16)
        return {"y": other // 4, "core": lax.rem(other // 2, 2), "zl": lax.rem(other, 2)}

    def ctx_peer(self, step):
        other = lax.rem(self.ctx + step, 8)
        return {"zh": other // 4, "x": lax.rem(other, 4)}

    def mirror(self):
        return {"zh": self.tp // 4, "x": lax.rem(self.tp, 4), "y": self.ctx // 2, "core": lax.rem(self.ctx, 2)}

    def greet(self, peers):
        barrier = pltpu.get_barrier_semaphore()
        peers = [self.beside(axis, step) for axis in ("x", "z") for step in (1, -1)] + peers
        for peer in peers:
            pl.semaphore_signal(barrier, inc=1, device_id=peer, device_id_type=MESH_ID)
        return len(peers)


class Link:
    def __init__(self, send_sem, recv_sem):
        self.send_sem, self.recv_sem, self.open = send_sem, recv_sem, []

    def copy(self, number, src, dst, device, landing=None):
        return pltpu.make_async_remote_copy(
            src_ref=src,
            dst_ref=dst,
            send_sem=self.send_sem.at[number],
            recv_sem=self.recv_sem.at[number if landing is None else landing],
            device_id=device,
            device_id_type=MESH_ID,
        )

    def send(self, number, src, dst, device, landing=None):
        copy = self.copy(number, src, dst, device, landing)
        copy.start()
        self.open.append(copy)

    def arrived(self, number, dst, device):
        self.copy(number, dst, dst, device).wait_recv()

    def finish(self):
        for copy in self.open:
            copy.wait_send()
        self.open = []


WAYS = ((0, 1), (1, -1))


class Gather:
    def __init__(self, place, link, piece, first):
        self.place, self.link, self.piece, self.first = place, link, piece, first

    def block(self, part, along_f, along_s, half=None):
        x, z = (along_f, along_s) if part == 0 else (along_s, along_f)
        return self.piece(wrapped(self.place.x + x), wrapped(self.place.z + z), part, half)

    def number(self, part, kind, direction, g=2):
        return self.first + part * 20 + {"near": 0, "far": 2, "near2": 4, "far2": 12}[kind] + (
            FAR_FIRST.index(g) * 2 + direction
        )

    def near(self, part):
        ref = self.block(part, 0, 0)
        for direction, step in WAYS:
            device = self.place.beside("xz"[part], step)
            self.link.send(self.number(part, "near", direction), ref, ref, device)

    def far(self, part):
        for direction, step in WAYS:
            back = self.place.beside("xz"[part], -step)
            self.link.arrived(self.number(part, "near", direction), self.block(part, -step, 0), back)
            ref = self.block(part, -step, 0, direction)
            device = self.place.beside("xz"[part], step)
            self.link.send(self.number(part, "far", direction), ref, ref, device)

    def far_done(self, part):
        for direction, step in WAYS:
            back = self.place.beside("xz"[part], -step)
            self.link.arrived(self.number(part, "far", direction), self.block(part, 2, 0, direction), back)

    def near2(self, part, g):
        ref = self.block(part, g, 0)
        for direction, step in WAYS:
            device = self.place.beside("zx"[part], step)
            self.link.send(self.number(part, "near2", direction, g), ref, ref, device)

    def far2(self, part, g):
        for direction, step in WAYS:
            back = self.place.beside("zx"[part], -step)
            self.link.arrived(self.number(part, "near2", direction, g), self.block(part, g, -step), back)
            ref = self.block(part, g, -step, direction)
            device = self.place.beside("zx"[part], step)
            self.link.send(self.number(part, "far2", direction, g), ref, ref, device)

    def far2_done(self, part, g):
        for direction, step in WAYS:
            back = self.place.beside("zx"[part], -step)
            number = self.number(part, "far2", direction, g)
            self.link.arrived(number, self.block(part, g, 2, direction), back)


def plane_gather(gather, ready=None, busy=None, seen=None):
    both = (0, 1)
    for part in both:
        if ready is not None:
            ready(part)
        gather.near(part)
        if ready is not None:
            gather.near2(part, 0)
    if ready is None:
        for part in both:
            gather.near2(part, 0)
    if busy is not None:
        busy()
    for part in both:
        gather.far(part)
    for part in both:
        gather.near2(part, -1)
        gather.near2(part, 1)
    for part in both:
        gather.far2(part, 0)
    for part in both:
        gather.far_done(part)
        gather.near2(part, 2)
    seen = seen or (lambda *_: None)
    seen(0, 0)
    for g in (-1, 1):
        for part in both:
            gather.far2(part, g)
    for part in both:
        gather.far2_done(part, 0)
    seen(1, 0)
    seen(2, 0)
    for part in both:
        gather.far2(part, 2)
    seen(0, -1)
    seen(0, 1)
    seen(2, 1)
    for g in (-1, 1):
        for part in both:
            gather.far2_done(part, g)
    seen(1, -1)
    seen(1, 1)
    seen(2, -1)
    for part in both:
        gather.far2_done(part, 2)
    seen(0, 2)
    seen(1, 2)
    seen(2, 2)


def picked(tile):
    slot_ids = lax.broadcasted_iota(jnp.int32, (768, 256), 0).astype(F32)
    return slot_ids == tile[0:1, :], slot_ids == tile[1:2, :]


def layer_kernel(
    resid_hbm,
    queries_hbm,
    keys_hbm,
    values_hbm,
    w_out_hbm,
    gain_hbm,
    w_gate,
    w_up,
    w_down,
    ids_hbm,
    units_hbm,
    out,
    resid,
    queries,
    keys,
    values,
    w_out,
    ids,
    units,
    all_keys,
    all_values,
    gain,
    gains,
    codes,
    combine,
    hres,
    slots,
    rows,
    tokens,
    token_rows,
    gate_w,
    up_w,
    down_w,
    row_squares,
    gate_acc,
    up_acc,
    hidden,
    partial,
    got_half,
    got_part,
    result,
    returned,
    load_sem,
    send_sem,
    recv_sem,
):
    place = Place()
    link = Link(send_sem, recv_sem)
    pieces = Link(send_sem, recv_sem)
    pairs = (
        (keys_hbm, keys),
        (values_hbm, values),
        (queries_hbm, queries),
        (gain_hbm, gain),
        (ids_hbm, ids),
        (units_hbm, units),
        (w_out_hbm, w_out),
        (resid_hbm, resid),
        (w_down, down_w),
        (w_gate, gate_w),
        (w_up, up_w),
    )
    loads = [pltpu.make_async_copy(src, dst, load_sem.at[i]) for i, (src, dst) in enumerate(pairs)]
    for load in loads[:9]:
        load.start()
    barrier = pltpu.get_barrier_semaphore()
    diagonal = place.ctx == place.tp
    members = [place.member_peer(step) for step in range(1, 16)]
    ctx_peers = [place.ctx_peer(step) for step in range(1, 8)]
    greeted = place.greet(members + ctx_peers)
    for load in loads[:2]:
        load.wait()

    here = place.ctx * 2 + place.zl
    mine = pl.ds(pl.multiple_of(place.zl * 128, 128), 128)
    all_keys[here] = keys[mine, :]
    all_values[here] = values[mine, :]

    @pl.when(diagonal)
    def _():
        pl.semaphore_wait(barrier, greeted)

    @pl.when(jnp.logical_not(diagonal))
    def _():
        pl.semaphore_signal(barrier, inc=1, device_id=place.mirror(), device_id_type=MESH_ID)
        pl.semaphore_wait(barrier, greeted + 1)

    def at(x, z):
        return ((z // 2) * 4 + x) * 2 + lax.rem(z, 2)

    def key_block(x, z, part, half):
        ref = (all_keys, all_values)[part]
        if half is None:
            return ref.at[at(x, z)]
        return ref.at[at(x, z), pl.ds(half * 64, 64)]

    def route():
        loads[3].wait()
        gains[place.member] = jnp.broadcast_to(gain[...].astype(F32).reshape(1, 384), (8, 384))
        for step in range(1, 16):
            ref = gains.at[place.member]
            link.send(88 + step, ref, ref, members[step - 1])
        loads[4].wait()
        loads[5].wait()
        line = lax.broadcasted_iota(jnp.int32, (8, 256), 0)
        numbers = ids[...]
        named = [line == numbers[k : k + 1, :] for k in range(2)]
        uses = jnp.where(named[0] | named[1], 1.0, 0.0).astype(BF16)
        row = lax.broadcasted_iota(jnp.int32, (256, 256), 0)
        column = lax.broadcasted_iota(jnp.int32, (256, 256), 1)
        before = jnp.where(row < column, 1.0, 0.0).astype(BF16)
        earlier = jnp.dot(uses, before, preferred_element_type=F32)
        amounts = units[...].astype(F32)
        total = amounts[0:1, :] + amounts[1:2, :]
        tile = jnp.zeros((8, 256), F32)
        for k in range(2):
            slot = jnp.sum(jnp.where(named[k], earlier, 0.0), axis=0, keepdims=True)
            code = numbers[k : k + 1, :].astype(F32) * 96.0 + slot
            weight = (amounts[k : k + 1, :] / total).astype(BF16).astype(F32)
            tile = jnp.where(line == k, code, jnp.where(line == 2 + k, weight, tile))
        codes[place.ctx] = tile
        for step in range(1, 8):
            ref = codes.at[place.ctx]
            link.send(200 + step, ref, ref, ctx_peers[step - 1])
        hits = picked(tile)
        combine[...] = (
            jnp.where(hits[0], tile[2:3, :], 0.0) + jnp.where(hits[1], tile[3:4, :], 0.0)
        ).astype(BF16)

    plane_gather(Gather(place, link, key_block, 0), busy=route)
    loads[2].wait()

    def attn_rows(part, block, start, count):
        return pl.ds(pl.multiple_of(part * 2048 + block * 128 + start, 64), count), pl.ds(0, 384)

    def attend(part):
        @pl.loop(0, 3)
        def _(i):
            columns = pl.ds(pl.multiple_of((part * 3 + i) * HD, HD), HD)
            scores = lax.dot_general(
                queries[mine, columns],
                all_keys[...].reshape(2048, HD),
                (((1,), (1,)), ((), ())),
                preferred_element_type=F32,
            ) * HD ** (-0.5)
            query_pos = here * 128 + lax.broadcasted_iota(jnp.int32, (128, 2048), 0)
            key_pos = lax.broadcasted_iota(jnp.int32, (128, 2048), 1)
            scores = jnp.where(key_pos <= query_pos, scores, -1e30)
            probs = jnp.exp(scores - jnp.max(scores, axis=1, keepdims=True))
            denom = jnp.sum(probs, axis=1, keepdims=True)
            update = jnp.dot(
                probs.astype(BF16), all_values[...].reshape(2048, HD), preferred_element_type=F32
            )
            where = attn_rows(part, here, 0, 128)[0]
            gate_w[where, pl.ds(pl.multiple_of(i * HD, HD), HD)] = (update / denom).astype(BF16)

    def attn_block(x, z, part, half):
        if half is None:
            return gate_w.at[attn_rows(part, at(x, z), 0, 128)]
        return gate_w.at[attn_rows(part, at(x, z), half * 64, 64)]

    plane_gather(Gather(place, link, attn_block, 40), ready=attend)

    loads[6].wait()

    def project(ctx):
        total = None
        for part in (0, 1):
            term = jnp.dot(
                gate_w[pl.ds(pl.multiple_of(part * 2048 + ctx * 256, 256), 256), pl.ds(0, 384)],
                w_out[pl.ds(part * 384, 384), :],
                preferred_element_type=F32,
            )
            total = term if total is None else total + term
        return total

    def piece(k):
        return up_w.at[pl.ds(k * 256, 256), pl.ds(0, 384)]

    partner = {"core": 1 - place.core}
    order = [wrapped(place.y + step) for step in (2, 1, -1, 0)]
    for i, j in enumerate(order):
        piece(i)[...] = project(2 * j + 1 - place.core).astype(BF16)
        pieces.send(80 + i, piece(i), piece(4 + i), partner)
    for i, j in enumerate(order):
        total = project(2 * j + place.core)
        pieces.arrived(80 + i, piece(4 + i), partner)
        total = total + piece(4 + i)[...].astype(F32)
        if i < 3:
            piece(8 + i)[...] = total.astype(BF16)
            pieces.send(84 + i, piece(8 + i), piece(12 + i), {"y": j})
    link.finish()
    loads[9].start()
    for i, step in enumerate((2, 1, -1)):
        pieces.arrived(84 + i, piece(12 + i), {"y": wrapped(place.y - step)})
        total = total + piece(12 + i)[...].astype(F32)
    piece(11)[...] = total.astype(BF16)
    move = pieces.copy(87, piece(11), piece(15), place.mirror())

    @pl.when(diagonal)
    def _():
        piece(15)[...] = piece(11)[...]

    @pl.when(jnp.logical_not(diagonal))
    def _():
        move.start()
        pieces.arrived(87, piece(15), place.mirror())

    loads[7].wait()
    hres[...] = (resid[...].astype(F32) + piece(15)[...].astype(F32)).astype(BF16)

    def token_block(x, z, part, half):
        if half is None:
            return tokens.at[at(x, z)]
        return tokens.at[at(x, z), pl.ds(half * 128, 128)]

    flow = Gather(place, link, token_block, 220)
    tokens[here] = hres[:, 256:384]
    flow.near(1)
    flow.near2(1, 0)
    hits = picked(codes[place.ctx])
    picks = jnp.where(hits[0] | hits[1], 1.0, 0.0).astype(BF16)
    slots[...] = jnp.dot(picks, hres[:, 0:256], preferred_element_type=F32).astype(BF16).reshape(8, 96, 256)

    base = 104
    for step in range(1, 8):
        target = lax.rem(place.tp + step, 8)
        link.send(base + step, slots.at[target], rows.at[place.x, place.z, place.tp], place.tp_peer(step))
    rows[place.x, place.z, place.tp] = slots[place.tp]

    @pl.when(jnp.logical_not(diagonal))
    def _():
        move.wait_send()

    pieces.finish()
    loads[10].start()
    flow.far(1)
    for step in range(1, 8):
        source = lax.rem(place.ctx + 8 - step, 8)
        link.arrived(200 + step, codes.at[source], ctx_peers[7 - step])
    flow.near2(1, -1)
    flow.near2(1, 1)
    flow.far_done(1)
    flow.near2(1, 2)

    def chosen(x, target):
        return partial.at[x, pl.ds(0, 2), target, :, pl.ds(0, 256)]

    def send_group(g):
        x = wrapped(place.x + g)
        for zh in range(2):
            ctx = zh * 4 + x
            hits = picked(codes[ctx])
            picks = jnp.where(hits[0] | hits[1], 1.0, 0.0).astype(BF16)
            both = jnp.concatenate([tokens[2 * ctx], tokens[2 * ctx + 1]], axis=1)
            taken = jnp.dot(picks, both, preferred_element_type=F32).astype(BF16)
            partial[x, zh, :, :, 0:256] = taken.reshape(8, 96, 256)
        for step in range(1, 8):
            target = lax.rem(place.tp + step, 8)
            number = 208 + FAR_FIRST.index(g) * 8 + step
            link.send(number, chosen(x, target), token_rows.at[place.tp, x], place.tp_peer(step))
        token_rows[place.tp, x] = chosen(x, place.tp)[...]

    send_group(0)
    gate_acc[...] = jnp.zeros_like(gate_acc)
    up_acc[...] = jnp.zeros_like(up_acc)
    row_squares[...] = jnp.zeros_like(row_squares)
    for step in range(1, 16):
        source = lax.rem(place.member + 16 - step, 16)
        link.arrived(88 + step, gains.at[source], members[15 - step])
    for step in range(1, 8):
        source = lax.rem(place.tp + 8 - step, 8)
        link.arrived(base + step, rows.at[place.x, place.z, source], place.tp_peer(8 - step))

    def block_of_rows(x, z, part, half):
        if half is None:
            return rows.at[x, z, pl.ds(part * 4, 4)]
        return rows.at[x, z, pl.ds(part * 4 + half * 2, 2)]

    def more_groups():
        for g in (0, 1, -1, 2):
            flow.far2(1, g)
        for g in (0, 1, -1, 2):
            flow.far2_done(1, g)
        for g in (1, -1, 2):
            send_group(g)

    def scaled(value, blocks):
        value = value.astype(F32)
        square = value * value
        squares = square[:, 0:128] + square[:, 128:256]
        return (value * blocks).astype(BF16), squares

    def use_rows(part, along):
        if (part, along) == (0, 0):
            loads[9].wait()
            loads[10].wait()
        if part == 2:
            use_tokens(along)
            return
        z = wrapped(place.z + along)
        zh, e = z // 2, lax.rem(z, 2)

        @pl.loop(part * 2, part * 2 + 2)
        def _(pair):
            lefts = []
            squares = row_squares[zh]
            for i in range(2):
                t = 2 * pair + i
                left, more = scaled(rows[:, z, t].reshape(384, 256), gains[2 * t + e, 0:1, 0:256])
                lefts.append(left)
                squares = squares + more.reshape(4, 96, 128)
            row_squares[zh] = squares
            left = jnp.concatenate(lefts, axis=1)
            spans = [pl.ds(pl.multiple_of((4 * pair + 2 * i + e) * 384, 128), 256) for i in range(2)]
            for acc, weights in ((gate_acc, gate_w), (up_acc, up_w)):
                right = jnp.concatenate([weights[span, :] for span in spans], axis=0)
                acc[zh] += jnp.dot(left, right, preferred_element_type=F32).reshape(4, 96, 512)

    def use_tokens(g):
        x = wrapped(place.x + g)
        for step in range(1, 8):
            source = lax.rem(place.tp + 8 - step, 8)
            number = 208 + FAR_FIRST.index(g) * 8 + step
            link.arrived(number, token_rows.at[source, x], place.tp_peer(8 - step))

        @pl.loop(0, 4)
        def _(pair):
            lefts, spans = [], []
            squares = row_squares[:, x]
            for i in range(2):
                t = 2 * pair + i
                blocks = jnp.concatenate([gains[2 * t + e, 0:1, 256:384] for e in range(2)], axis=1)
                left, more = scaled(token_rows[t, x].reshape(192, 256), blocks)
                lefts.append(left)
                squares = squares + more.reshape(2, 96, 128)
                spans += [pl.ds(pl.multiple_of((2 * t + e) * 384 + 256, 128), 128) for e in range(2)]
            row_squares[:, x] = squares
            left = jnp.concatenate(lefts, axis=1)
            for acc, weights in ((gate_acc, gate_w), (up_acc, up_w)):
                right = jnp.concatenate([weights[span, :] for span in spans], axis=0)
                acc[:, x] += jnp.dot(left, right, preferred_element_type=F32).reshape(2, 96, 512)

    plane_gather(Gather(place, link, block_of_rows, 112), busy=more_groups, seen=use_rows)
    link.finish()
    for zh in range(2):
        mean = jnp.sum(row_squares[zh].reshape(384, 128), axis=1, keepdims=True) / D
        scale = lax.rsqrt(mean + 1e-05)
        gate = gate_acc[zh].reshape(384, 512) * scale
        value = gate / (1.0 + jnp.exp(-gate)) * (up_acc[zh].reshape(384, 512) * scale)
        hidden[pl.ds(zh * 4, 4)] = value.astype(BF16).reshape(4, 96, 512)
    loads[8].wait()

    def compute(part, g):
        if part == 0:
            x = wrapped(place.x + g)
            left = jnp.concatenate([hidden[x], hidden[4 + x]], axis=0)

            @pl.loop(0, 4)
            def _(t):
                right = down_w[:, pl.ds(pl.multiple_of(t * 768, 768), 768)]
                both = jnp.dot(left, right, preferred_element_type=F32).astype(BF16)
                for zh in range(2):
                    for e in range(2):
                        partial[x, zh * 2 + e, t] = both[zh * 96 : zh * 96 + 96, e * 384 : e * 384 + 384]
        else:
            z = wrapped(place.z + g)
            left = hidden[pl.ds((z // 2) * 4, 4)].reshape(384, 512)

            @pl.loop(4, 8)
            def _(t):
                start = (2 * t + lax.rem(z, 2)) * 384
                right = down_w[:, pl.ds(pl.multiple_of(start, 384), 384)]
                both = jnp.dot(left, right, preferred_element_type=F32).astype(BF16)
                partial[:, z, t] = both.reshape(4, 96, 384)

    def block(part, along_f, along_s):
        x, z = (along_f, along_s) if part == 0 else (along_s, along_f)
        return wrapped(place.x + x), wrapped(place.z + z)

    def half_of(where, part, half):
        return partial.at[where[0], where[1], pl.ds(part * 4 + half * 2, 2)]

    def part_of(where, part):
        return partial.at[where[0], where[1], pl.ds(part * 4, 4)]

    def add(target, *sources):
        total = target[...].astype(F32)
        for source in sources:
            total = total + source[...].astype(F32)
        target[...] = total.astype(BF16)

    class Ring:
        def __init__(self, part, stage, axis, at):
            self.part, self.stage, self.axis, self.at = part, stage, axis, at
            self.number = 152 + (part * 5 + stage) * 4

        def far(self):
            for direction, step in ((0, 1), (1, -1)):
                link.send(
                    self.number + direction,
                    half_of(self.at(2), self.part, direction),
                    got_half.at[self.part, self.stage, direction],
                    place.beside(self.axis, step),
                )

        def near(self):
            for direction, step in ((0, 1), (1, -1)):
                got = got_half.at[self.part, self.stage, direction]
                link.arrived(self.number + direction, got, place.beside(self.axis, -step))
                add(half_of(self.at(step), self.part, direction), got)
                link.send(
                    self.number + 2 + direction,
                    part_of(self.at(step), self.part),
                    got_part.at[self.part, self.stage, direction],
                    place.beside(self.axis, step),
                )

        def receive(self):
            gots = []
            for direction, step in ((0, 1), (1, -1)):
                got = got_part.at[self.part, self.stage, direction]
                link.arrived(self.number + 2 + direction, got, place.beside(self.axis, -step))
                gots.append(got)
            return gots

        def end(self):
            add(part_of(self.at(0), self.part), *self.receive())

    outer = [
        {
            g: Ring(part, FAR_FIRST.index(g), "zx"[part], lambda step, part=part, g=g: block(part, g, step))
            for g in FAR_FIRST
        }
        for part in (0, 1)
    ]
    inner = [Ring(part, 4, "xz"[part], lambda step, part=part: block(part, step, 0)) for part in (0, 1)]
    for g in FAR_FIRST:
        for part in (0, 1):
            compute(part, g)
            outer[part][g].far()
    for g in (2, 1, -1):
        for part in (0, 1):
            outer[part][g].near()
    for part in (0, 1):
        outer[part][2].end()
        inner[part].far()
    for part in (0, 1):
        outer[part][0].near()
    for part in (0, 1):
        outer[part][1].end()
        outer[part][-1].end()
        inner[part].near()
    base = 192
    for part in (0, 1):
        outer[part][0].end()
        gots = inner[part].receive()
        total = part_of(inner[part].at(0), part)[...].astype(F32)
        for got in gots:
            total = total + got[...].astype(F32)
        result[pl.ds(part * 4, 4)] = total.astype(BF16)
    for step in range(1, 8):
        target = lax.rem(place.tp + step, 8)
        link.send(base + step, result.at[target], returned.at[place.tp], place.tp_peer(step))
    returned[place.tp] = result[place.tp]
    for step in range(1, 8):
        source = lax.rem(place.tp + 8 - step, 8)
        link.arrived(base + step, returned.at[source], place.tp_peer(8 - step))
    link.finish()
    moe = lax.dot_general(
        combine[...],
        returned[...].reshape(768, 384),
        (((0,), (0,)), ((), ())),
        preferred_element_type=F32,
    )
    out[...] = (hres[...].astype(F32) + moe).astype(BF16)


def on_device(
    resid, queries, keys, values, w_out, norm_gain, w_gate, w_up, w_down, expert_ids, route_units
):
    copies = 260
    return pl.pallas_call(
        layer_kernel,
        out_shape=jax.ShapeDtypeStruct((256, 384), BF16),
        in_specs=[pl.BlockSpec(memory_space=pl.ANY)] * 11,
        out_specs=pl.BlockSpec(memory_space=pltpu.VMEM),
        scratch_shapes=[
            pltpu.VMEM((256, 384), BF16),
            pltpu.VMEM((256, 768), BF16),
            pltpu.VMEM((256, HD), BF16),
            pltpu.VMEM((256, HD), BF16),
            pltpu.VMEM((768, 384), BF16),
            pltpu.VMEM((2, 256), jnp.int32),
            pltpu.VMEM((2, 256), jnp.int32),
            pltpu.VMEM((16, 128, HD), BF16),
            pltpu.VMEM((16, 128, HD), BF16),
            pltpu.VMEM((384,), BF16),
            pltpu.VMEM((16, 8, 384), F32),
            pltpu.VMEM((8, 8, 256), F32),
            pltpu.VMEM((768, 256), BF16),
            pltpu.VMEM((256, 384), BF16),
            pltpu.VMEM((8, 96, 256), BF16),
            pltpu.VMEM((4, 4, 8, 96, 256), BF16),
            pltpu.VMEM((16, 256, 128), BF16),
            pltpu.VMEM((8, 4, 2, 96, 256), BF16),
            pltpu.VMEM((6144, 512), BF16),
            pltpu.VMEM((6144, 512), BF16),
            pltpu.VMEM((512, 6144), BF16),
            pltpu.VMEM((2, 4, 96, 128), F32),
            pltpu.VMEM((2, 4, 96, 512), F32),
            pltpu.VMEM((2, 4, 96, 512), F32),
            pltpu.VMEM((8, 96, 512), BF16),
            pltpu.VMEM((4, 4, 8, 96, 384), BF16),
            pltpu.VMEM((2, 5, 2, 2, 96, 384), BF16),
            pltpu.VMEM((2, 5, 2, 4, 96, 384), BF16),
            pltpu.VMEM((8, 96, 384), BF16),
            pltpu.VMEM((8, 96, 384), BF16),
            pltpu.SemaphoreType.DMA((11,)),
            pltpu.SemaphoreType.DMA((copies,)),
            pltpu.SemaphoreType.DMA((copies,)),
        ],
        compiler_params=pltpu.CompilerParams(
            collective_id=0, has_side_effects=True, vmem_limit_bytes=64 * 1024 * 1024 - 128 * 1024
        ),
        name="layer",
    )(
        resid,
        queries,
        keys,
        values,
        w_out,
        norm_gain,
        w_gate[0],
        w_up[0],
        w_down[0],
        expert_ids.T,
        route_units.T,
    )


def solution(mesh):
    torus = Mesh(mesh.devices.reshape(2, 4, 4, 2, 2), ("zh", "x", "y", "core", "zl"))
    in_specs = (
        P(CTX, TP_EP),
        P(CTX, TP),
        P(CTX, TP),
        P(CTX, TP),
        P(TP, ("zh", "x", "zl")),
        P(TP_EP),
        P(TP, None, ("zh", "x", "zl")),
        P(TP, None, ("zh", "x", "zl")),
        P(TP, ("zh", "x", "zl"), None),
        P(CTX, None),
        P(CTX, None),
    )
    return jax.shard_map(
        on_device, mesh=torus, in_specs=in_specs, out_specs=P(CTX, TP_EP), check_vma=False
    )
```

```python
import jax
import jax.numpy as jnp
from jax import lax
from jax.experimental import pallas as pl
from jax.experimental.pallas import tpu as pltpu
from jax.sharding import Mesh
from jax.sharding import PartitionSpec as P

D = 6144
HD = 128
CTX = ("zh", "x")
TP = ("y", "core")
TP_EP = ("y", "core", "zl")
MESH_ID = pl.DeviceIdType.MESH
F32 = jnp.float32
BF16 = jnp.bfloat16
FAR_FIRST = (2, 1, -1, 0)


def wrapped(index, size=4):
    return lax.rem(index + size, size)


class Place:
    def __init__(self):
        self.x = lax.axis_index("x")
        self.z = lax.axis_index("zh") * 2 + lax.axis_index("zl")
        self.y = lax.axis_index("y")
        self.core = lax.axis_index("core")
        self.zl = lax.axis_index("zl")
        self.tp = self.y * 2 + self.core
        self.ctx = lax.axis_index("zh") * 4 + self.x
        self.member = self.tp * 2 + self.zl

    def beside(self, axis, step):
        if axis == "x":
            return {"x": wrapped(self.x + step)}
        z = wrapped(self.z + step)
        return {"zh": z // 2, "zl": lax.rem(z, 2)}

    def tp_peer(self, step):
        other = lax.rem(self.tp + step, 8)
        return {"y": other // 2, "core": lax.rem(other, 2)}

    def member_peer(self, step):
        other = lax.rem(self.member + step, 16)
        return {"y": other // 4, "core": lax.rem(other // 2, 2), "zl": lax.rem(other, 2)}

    def ctx_peer(self, step):
        other = lax.rem(self.ctx + step, 8)
        return {"zh": other // 4, "x": lax.rem(other, 4)}

    def mirror(self):
        return {"zh": self.tp // 4, "x": lax.rem(self.tp, 4), "y": self.ctx // 2, "core": lax.rem(self.ctx, 2)}

    def greet(self, peers):
        barrier = pltpu.get_barrier_semaphore()
        peers = [self.beside(axis, step) for axis in ("x", "z") for step in (1, -1)] + peers
        for peer in peers:
            pl.semaphore_signal(barrier, inc=1, device_id=peer, device_id_type=MESH_ID)
        return len(peers)


class Link:
    def __init__(self, send_sem, recv_sem):
        self.send_sem, self.recv_sem, self.open = send_sem, recv_sem, []

    def copy(self, number, src, dst, device, landing=None):
        return pltpu.make_async_remote_copy(
            src_ref=src,
            dst_ref=dst,
            send_sem=self.send_sem.at[number],
            recv_sem=self.recv_sem.at[number if landing is None else landing],
            device_id=device,
            device_id_type=MESH_ID,
        )

    def send(self, number, src, dst, device, landing=None):
        copy = self.copy(number, src, dst, device, landing)
        copy.start()
        self.open.append(copy)

    def arrived(self, number, dst, device):
        self.copy(number, dst, dst, device).wait_recv()

    def finish(self):
        for copy in self.open:
            copy.wait_send()
        self.open = []


WAYS = ((0, 1), (1, -1))


class Gather:
    def __init__(self, place, link, piece, first):
        self.place, self.link, self.piece, self.first = place, link, piece, first

    def block(self, part, along_f, along_s, half=None):
        x, z = (along_f, along_s) if part == 0 else (along_s, along_f)
        return self.piece(wrapped(self.place.x + x), wrapped(self.place.z + z), part, half)

    def number(self, part, kind, direction, g=2):
        return self.first + part * 20 + {"near": 0, "far": 2, "near2": 4, "far2": 12}[kind] + (
            FAR_FIRST.index(g) * 2 + direction
        )

    def near(self, part):
        ref = self.block(part, 0, 0)
        for direction, step in WAYS:
            device = self.place.beside("xz"[part], step)
            self.link.send(self.number(part, "near", direction), ref, ref, device)

    def far(self, part):
        for direction, step in WAYS:
            back = self.place.beside("xz"[part], -step)
            self.link.arrived(self.number(part, "near", direction), self.block(part, -step, 0), back)
            ref = self.block(part, -step, 0, direction)
            device = self.place.beside("xz"[part], step)
            self.link.send(self.number(part, "far", direction), ref, ref, device)

    def far_done(self, part):
        for direction, step in WAYS:
            back = self.place.beside("xz"[part], -step)
            self.link.arrived(self.number(part, "far", direction), self.block(part, 2, 0, direction), back)

    def near2(self, part, g):
        ref = self.block(part, g, 0)
        for direction, step in WAYS:
            device = self.place.beside("zx"[part], step)
            self.link.send(self.number(part, "near2", direction, g), ref, ref, device)

    def far2(self, part, g):
        for direction, step in WAYS:
            back = self.place.beside("zx"[part], -step)
            self.link.arrived(self.number(part, "near2", direction, g), self.block(part, g, -step), back)
            ref = self.block(part, g, -step, direction)
            device = self.place.beside("zx"[part], step)
            self.link.send(self.number(part, "far2", direction, g), ref, ref, device)

    def far2_done(self, part, g):
        for direction, step in WAYS:
            back = self.place.beside("zx"[part], -step)
            number = self.number(part, "far2", direction, g)
            self.link.arrived(number, self.block(part, g, 2, direction), back)


def plane_gather(gather, ready=None, busy=None, later=None, seen=None):
    both = (0, 1)
    for part in both:
        if ready is not None:
            ready(part)
        gather.near(part)
        if ready is not None:
            gather.near2(part, 0)
    if ready is None:
        for part in both:
            gather.near2(part, 0)
    if busy is not None:
        busy()
    for part in both:
        gather.far(part)
    for part in both:
        gather.near2(part, -1)
        gather.near2(part, 1)
    if later is not None:
        later()
    for part in both:
        gather.far2(part, 0)
    for part in both:
        gather.far_done(part)
        gather.near2(part, 2)
    seen = seen or (lambda *_: None)
    seen(0, 0)
    for g in (-1, 1):
        for part in both:
            gather.far2(part, g)
    for part in both:
        gather.far2_done(part, 0)
    seen(1, 0)
    seen(2, 0)
    for part in both:
        gather.far2(part, 2)
    seen(0, -1)
    seen(0, 1)
    seen(2, 1)
    for g in (-1, 1):
        for part in both:
            gather.far2_done(part, g)
    seen(1, -1)
    seen(1, 1)
    seen(2, -1)
    for part in both:
        gather.far2_done(part, 2)
    seen(0, 2)
    seen(1, 2)
    seen(2, 2)


def picked(tile):
    slot_ids = lax.broadcasted_iota(jnp.int32, (768, 256), 0).astype(F32)
    return slot_ids == tile[0:1, :], slot_ids == tile[1:2, :]


def layer_kernel(
    resid_hbm,
    queries_hbm,
    keys_hbm,
    values_hbm,
    w_out_hbm,
    gain_hbm,
    w_gate,
    w_up,
    w_down,
    ids_hbm,
    units_hbm,
    out,
    resid,
    queries,
    keys,
    values,
    w_out,
    ids,
    units,
    all_keys,
    all_values,
    gain,
    gains,
    codes,
    combine,
    hres,
    slots,
    rows,
    tokens,
    token_rows,
    gate_w,
    up_w,
    down_w,
    row_squares,
    gate_acc,
    up_acc,
    hidden,
    partial,
    got_half,
    got_part,
    back_rows,
    x_half,
    x_part,
    z_half,
    z_part,
    result,
    returned,
    load_sem,
    send_sem,
    recv_sem,
):
    place = Place()
    link = Link(send_sem, recv_sem)
    pieces = Link(send_sem, recv_sem)
    pairs = (
        (keys_hbm, keys),
        (values_hbm, values),
        (queries_hbm, queries),
        (gain_hbm, gain),
        (ids_hbm, ids),
        (units_hbm, units),
        (w_out_hbm, w_out),
        (resid_hbm, resid),
        (w_down, down_w),
        (w_gate, gate_w),
        (w_up, up_w),
    )
    loads = [pltpu.make_async_copy(src, dst, load_sem.at[i]) for i, (src, dst) in enumerate(pairs)]
    for load in loads[:9]:
        load.start()
    barrier = pltpu.get_barrier_semaphore()
    diagonal = place.ctx == place.tp
    members = [place.member_peer(step) for step in range(1, 16)]
    ctx_peers = [place.ctx_peer(step) for step in range(1, 8)]
    greeted = place.greet(members + ctx_peers)
    for load in loads[:2]:
        load.wait()

    here = place.ctx * 2 + place.zl
    mine = pl.ds(pl.multiple_of(place.zl * 128, 128), 128)
    all_keys[here] = keys[mine, :]
    all_values[here] = values[mine, :]

    @pl.when(diagonal)
    def _():
        pl.semaphore_wait(barrier, greeted)

    @pl.when(jnp.logical_not(diagonal))
    def _():
        pl.semaphore_signal(barrier, inc=1, device_id=place.mirror(), device_id_type=MESH_ID)
        pl.semaphore_wait(barrier, greeted + 1)

    def at(x, z):
        return ((z // 2) * 4 + x) * 2 + lax.rem(z, 2)

    def key_block(x, z, part, half):
        ref = (all_keys, all_values)[part]
        if half is None:
            return ref.at[at(x, z)]
        return ref.at[at(x, z), pl.ds(half * 64, 64)]

    def route():
        loads[3].wait()
        gains[place.member] = jnp.broadcast_to(gain[...].astype(F32).reshape(1, 384), (8, 384))
        for step in range(1, 16):
            ref = gains.at[place.member]
            link.send(88 + step, ref, ref, members[step - 1])
        loads[4].wait()
        loads[5].wait()
        line = lax.broadcasted_iota(jnp.int32, (8, 256), 0)
        numbers = ids[...]
        named = [line == numbers[k : k + 1, :] for k in range(2)]
        uses = jnp.where(named[0] | named[1], 1.0, 0.0).astype(BF16)
        row = lax.broadcasted_iota(jnp.int32, (256, 256), 0)
        column = lax.broadcasted_iota(jnp.int32, (256, 256), 1)
        before = jnp.where(row < column, 1.0, 0.0).astype(BF16)
        earlier = jnp.dot(uses, before, preferred_element_type=F32)
        amounts = units[...].astype(F32)
        total = amounts[0:1, :] + amounts[1:2, :]
        tile = jnp.zeros((8, 256), F32)
        for k in range(2):
            slot = jnp.sum(jnp.where(named[k], earlier, 0.0), axis=0, keepdims=True)
            code = numbers[k : k + 1, :].astype(F32) * 96.0 + slot
            weight = (amounts[k : k + 1, :] / total).astype(BF16).astype(F32)
            tile = jnp.where(line == k, code, jnp.where(line == 2 + k, weight, tile))
        codes[place.ctx] = tile
        for step in range(1, 8):
            ref = codes.at[place.ctx]
            link.send(200 + step, ref, ref, ctx_peers[step - 1])
        hits = picked(tile)
        combine[...] = (
            jnp.where(hits[0], tile[2:3, :], 0.0) + jnp.where(hits[1], tile[3:4, :], 0.0)
        ).astype(BF16)

    plane_gather(Gather(place, link, key_block, 0), busy=route)
    loads[2].wait()

    def attn_rows(part, block, start, count):
        return pl.ds(pl.multiple_of(part * 2048 + block * 128 + start, 64), count), pl.ds(0, 384)

    def attend(part):
        @pl.loop(0, 3)
        def _(i):
            columns = pl.ds(pl.multiple_of((part * 3 + i) * HD, HD), HD)
            scores = lax.dot_general(
                queries[mine, columns],
                all_keys[...].reshape(2048, HD),
                (((1,), (1,)), ((), ())),
                preferred_element_type=F32,
            ) * HD ** (-0.5)
            query_pos = here * 128 + lax.broadcasted_iota(jnp.int32, (128, 2048), 0)
            key_pos = lax.broadcasted_iota(jnp.int32, (128, 2048), 1)
            scores = jnp.where(key_pos <= query_pos, scores, -1e30)
            probs = jnp.exp(scores - jnp.max(scores, axis=1, keepdims=True))
            denom = jnp.sum(probs, axis=1, keepdims=True)
            update = jnp.dot(
                probs.astype(BF16), all_values[...].reshape(2048, HD), preferred_element_type=F32
            )
            where = attn_rows(part, here, 0, 128)[0]
            gate_w[where, pl.ds(pl.multiple_of(i * HD, HD), HD)] = (update / denom).astype(BF16)

    def attn_block(x, z, part, half):
        if half is None:
            return gate_w.at[attn_rows(part, at(x, z), 0, 128)]
        return gate_w.at[attn_rows(part, at(x, z), half * 64, 64)]

    plane_gather(Gather(place, link, attn_block, 40), ready=attend)

    loads[6].wait()

    def project(ctx):
        total = None
        for part in (0, 1):
            term = jnp.dot(
                gate_w[pl.ds(pl.multiple_of(part * 2048 + ctx * 256, 256), 256), pl.ds(0, 384)],
                w_out[pl.ds(part * 384, 384), :],
                preferred_element_type=F32,
            )
            total = term if total is None else total + term
        return total

    def piece(k):
        return up_w.at[pl.ds(k * 256, 256), pl.ds(0, 384)]

    partner = {"core": 1 - place.core}
    order = [wrapped(place.y + step) for step in (2, 1, -1, 0)]
    for i, j in enumerate(order):
        piece(i)[...] = project(2 * j + 1 - place.core).astype(BF16)
        pieces.send(80 + i, piece(i), piece(4 + i), partner)
    for i, j in enumerate(order):
        total = project(2 * j + place.core)
        pieces.arrived(80 + i, piece(4 + i), partner)
        total = total + piece(4 + i)[...].astype(F32)
        if i < 3:
            piece(8 + i)[...] = total.astype(BF16)
            pieces.send(84 + i, piece(8 + i), piece(12 + i), {"y": j})
    link.finish()
    loads[9].start()
    for i, step in enumerate((2, 1, -1)):
        pieces.arrived(84 + i, piece(12 + i), {"y": wrapped(place.y - step)})
        total = total + piece(12 + i)[...].astype(F32)
    piece(11)[...] = total.astype(BF16)
    move = pieces.copy(87, piece(11), piece(15), place.mirror())

    @pl.when(diagonal)
    def _():
        piece(15)[...] = piece(11)[...]

    @pl.when(jnp.logical_not(diagonal))
    def _():
        move.start()
        pieces.arrived(87, piece(15), place.mirror())

    loads[7].wait()
    hres[...] = (resid[...].astype(F32) + piece(15)[...].astype(F32)).astype(BF16)

    def token_block(x, z, part, half):
        where = z // 2, 2 * x + lax.rem(z, 2)
        if half is None:
            return tokens.at[where]
        return tokens.at[(*where, pl.ds(half * 128, 128))]

    flow = Gather(place, link, token_block, 220)
    own = place.z // 2, 2 * place.x + place.zl
    tokens[own] = hres[:, 256:384]
    flow.near(1)
    flow.near2(1, 0)
    hits = picked(codes[place.ctx])
    picks = jnp.where(hits[0] | hits[1], 1.0, 0.0).astype(BF16)
    slots[...] = jnp.dot(picks, hres[:, 0:256], preferred_element_type=F32).astype(BF16).reshape(8, 96, 256)

    base = 104
    for step in range(1, 8):
        target = lax.rem(place.tp + step, 8)
        link.send(base + step, slots.at[target], rows.at[place.x, place.z, place.tp], place.tp_peer(step))
    rows[place.x, place.z, place.tp] = slots[place.tp]

    @pl.when(jnp.logical_not(diagonal))
    def _():
        move.wait_send()

    pieces.finish()
    loads[10].start()
    flow.far(1)
    for step in range(1, 8):
        source = lax.rem(place.ctx + 8 - step, 8)
        link.arrived(200 + step, codes.at[source], ctx_peers[7 - step])
    flow.near2(1, -1)
    flow.near2(1, 1)

    def chosen(x, target):
        return partial.at[x, pl.ds(0, 2), target]

    def send_group(g):
        x = wrapped(place.x + g)
        for zh in range(2):
            ctx = zh * 4 + x
            hits = picked(codes[ctx])
            picks = jnp.where(hits[0] | hits[1], 1.0, 0.0).astype(BF16)
            both = jnp.concatenate([tokens[zh, 2 * x + e] for e in range(2)], axis=1)
            taken = jnp.dot(picks, both, preferred_element_type=F32).astype(BF16)
            partial[x, zh] = taken.reshape(8, 96, 256)
        for step in range(1, 8):
            target = lax.rem(place.tp + step, 8)
            number = 208 + FAR_FIRST.index(g) * 8 + step
            link.send(number, chosen(x, target), token_rows.at[place.tp, x], place.tp_peer(step))
        token_rows[place.tp, x] = chosen(x, place.tp)[...]

    for step in range(1, 16):
        source = lax.rem(place.member + 16 - step, 16)
        link.arrived(88 + step, gains.at[source], members[15 - step])
    for step in range(1, 8):
        source = lax.rem(place.tp + 8 - step, 8)
        link.arrived(base + step, rows.at[place.x, place.z, source], place.tp_peer(8 - step))

    def block_of_rows(x, z, part, half):
        if half is None:
            return rows.at[x, z, pl.ds(part * 4, 4)]
        return rows.at[x, z, pl.ds(part * 4 + half * 2, 2)]

    def first_group():
        flow.far_done(1)
        flow.near2(1, 2)
        send_group(0)
        for g in (0, 1, -1, 2):
            flow.far2(1, g)

    def more_groups():
        for g in (0, 1, -1, 2):
            flow.far2_done(1, g)
        for g in (1, -1, 2):
            send_group(g)
        gate_acc[...] = jnp.zeros_like(gate_acc)
        up_acc[...] = jnp.zeros_like(up_acc)
        row_squares[...] = jnp.zeros_like(row_squares)

    def scaled(value, blocks):
        value = value.astype(F32)
        square = value * value
        squares = square[:, 0:128] + square[:, 128:256]
        return (value * blocks).astype(BF16), squares

    def use_rows(part, along):
        if (part, along) == (0, 0):
            loads[9].wait()
            loads[10].wait()
        if part == 2:
            use_tokens(along)
            return
        z = wrapped(place.z + along)
        zh, e = z // 2, lax.rem(z, 2)

        @pl.loop(part * 2, part * 2 + 2)
        def _(pair):
            lefts = []
            squares = row_squares[zh]
            for i in range(2):
                t = 2 * pair + i
                left, more = scaled(rows[:, z, t].reshape(384, 256), gains[2 * t + e, 0:1, 0:256])
                lefts.append(left)
                squares = squares + more.reshape(4, 96, 128)
            row_squares[zh] = squares
            left = jnp.concatenate(lefts, axis=1)
            spans = [pl.ds(pl.multiple_of((4 * pair + 2 * i + e) * 384, 128), 256) for i in range(2)]
            for acc, weights in ((gate_acc, gate_w), (up_acc, up_w)):
                right = jnp.concatenate([weights[span, :] for span in spans], axis=0)
                acc[zh] += jnp.dot(left, right, preferred_element_type=F32).reshape(4, 96, 512)

    def use_tokens(g):
        x = wrapped(place.x + g)
        for step in range(1, 8):
            source = lax.rem(place.tp + 8 - step, 8)
            number = 208 + FAR_FIRST.index(g) * 8 + step
            link.arrived(number, token_rows.at[source, x], place.tp_peer(8 - step))

        @pl.loop(0, 4)
        def _(pair):
            lefts, spans = [], []
            squares = row_squares[:, x]
            for i in range(2):
                t = 2 * pair + i
                blocks = jnp.concatenate([gains[2 * t + e, 0:1, 256:384] for e in range(2)], axis=1)
                left, more = scaled(token_rows[t, x].reshape(192, 256), blocks)
                lefts.append(left)
                squares = squares + more.reshape(2, 96, 128)
                spans += [pl.ds(pl.multiple_of((2 * t + e) * 384 + 256, 128), 128) for e in range(2)]
            row_squares[:, x] = squares
            left = jnp.concatenate(lefts, axis=1)
            for acc, weights in ((gate_acc, gate_w), (up_acc, up_w)):
                right = jnp.concatenate([weights[span, :] for span in spans], axis=0)
                acc[:, x] += jnp.dot(left, right, preferred_element_type=F32).reshape(2, 96, 512)

    plane_gather(Gather(place, link, block_of_rows, 112), busy=first_group, later=more_groups, seen=use_rows)
    link.finish()
    for zh in range(2):
        mean = jnp.sum(row_squares[zh].reshape(384, 128), axis=1, keepdims=True) / D
        scale = lax.rsqrt(mean + 1e-05)
        gate = gate_acc[zh].reshape(384, 512) * scale
        value = gate / (1.0 + jnp.exp(-gate)) * (up_acc[zh].reshape(384, 512) * scale)
        hidden[pl.ds(zh * 4, 4)] = value.astype(BF16).reshape(4, 96, 512)
    loads[8].wait()

    def compute(part, g):
        if part == 0:
            x = wrapped(place.x + g)
            left = jnp.concatenate([hidden[x], hidden[4 + x]], axis=0)

            @pl.loop(0, 4)
            def _(t):
                right = jnp.concatenate(
                    [down_w[:, pl.ds(pl.multiple_of((2 * t + e) * 384, 128), 256)] for e in range(2)], axis=1
                )
                both = jnp.dot(left, right, preferred_element_type=F32).astype(BF16)
                for zh in range(2):
                    for e in range(2):
                        partial[x, zh * 2 + e, t] = both[zh * 96 : zh * 96 + 96, e * 256 : e * 256 + 256]
        else:
            z = wrapped(place.z + g)
            left = hidden[pl.ds((z // 2) * 4, 4)].reshape(384, 512)

            @pl.loop(4, 8)
            def _(t):
                start = (2 * t + lax.rem(z, 2)) * 384
                right = down_w[:, pl.ds(pl.multiple_of(start, 128), 256)]
                both = jnp.dot(left, right, preferred_element_type=F32).astype(BF16)
                partial[:, z, t] = both.reshape(4, 96, 256)

    def send_back(g):
        x = wrapped(place.x + g)
        left = jnp.concatenate([hidden[x], hidden[4 + x]], axis=0)

        @pl.loop(0, 8)
        def _(t):
            right = jnp.concatenate(
                [down_w[:, pl.ds(pl.multiple_of((2 * t + e) * 384 + 256, 128), 128)] for e in range(2)],
                axis=1,
            )
            both = jnp.dot(left, right, preferred_element_type=F32).astype(BF16)
            token_rows[t, x] = both.reshape(2, 96, 256)

        for step in range(1, 8):
            target = lax.rem(place.tp + step, 8)
            number = 260 + FAR_FIRST.index(g) * 8 + step
            link.send(number, token_rows.at[target, x], back_rows.at[place.tp, x], place.tp_peer(step))
        back_rows[place.tp, x] = token_rows[place.tp, x]

    def weigh(g):
        x = wrapped(place.x + g)
        for step in range(1, 8):
            source = lax.rem(place.tp + 8 - step, 8)
            number = 260 + FAR_FIRST.index(g) * 8 + step
            link.arrived(number, back_rows.at[source, x], place.tp_peer(8 - step))
        for zh in range(2):
            tile = codes[zh * 4 + x]
            hits = picked(tile)
            shares = (
                jnp.where(hits[0], tile[2:3, :], 0.0) + jnp.where(hits[1], tile[3:4, :], 0.0)
            ).astype(BF16)
            total = lax.dot_general(
                shares,
                back_rows[:, x, zh].reshape(768, 256),
                (((0,), (0,)), ((), ())),
                preferred_element_type=F32,
            ).astype(BF16)
            for e in range(2):
                tokens[zh, 2 * x + e] = total[:, e * 128 : e * 128 + 128]

    def add(target, *sources):
        total = target[...].astype(F32)
        for source in sources:
            total = total + source[...].astype(F32)
        target[...] = total.astype(BF16)

    class Ring:
        def __init__(self, number, axis, whole, half, got_half, got_part):
            self.number, self.axis, self.whole, self.half = number, axis, whole, half
            self.got_half, self.got_part = got_half, got_part

        def far(self):
            for direction, step in WAYS:
                link.send(
                    self.number + direction,
                    self.half(2, direction),
                    self.got_half.at[direction],
                    place.beside(self.axis, step),
                )

        def near(self):
            for direction, step in WAYS:
                got = self.got_half.at[direction]
                link.arrived(self.number + direction, got, place.beside(self.axis, -step))
                add(self.half(step, direction), got)
                link.send(
                    self.number + 2 + direction,
                    self.whole(step),
                    self.got_part.at[direction],
                    place.beside(self.axis, step),
                )

        def receive(self):
            for direction, step in WAYS:
                got = self.got_part.at[direction]
                link.arrived(self.number + 2 + direction, got, place.beside(self.axis, -step))
            return [self.got_part.at[direction] for direction in range(2)]

        def end(self):
            add(self.whole(0), *self.receive())

    def slot_ring(part, stage, axis, at):
        def whole(step):
            x, z = at(step)
            return partial.at[x, z, pl.ds(part * 4, 4)]

        def half(step, direction):
            x, z = at(step)
            return partial.at[x, z, pl.ds(part * 4 + direction * 2, 2)]

        number = 152 + (part * 5 + stage) * 4
        return Ring(number, axis, whole, half, got_half.at[part, stage], got_part.at[part, stage])

    def spot(part, along_f, along_s):
        x, z = (along_f, along_s) if part == 0 else (along_s, along_f)
        return wrapped(place.x + x), wrapped(place.z + z)

    outer = [
        {
            g: slot_ring(
                part, FAR_FIRST.index(g), "zx"[part], lambda step, part=part, g=g: spot(part, g, step)
            )
            for g in FAR_FIRST
        }
        for part in (0, 1)
    ]
    inner = [slot_ring(part, 4, "xz"[part], lambda step, part=part: spot(part, step, 0)) for part in (0, 1)]

    def column(step, rows=slice(None)):
        return tokens.at[:, pl.ds(2 * wrapped(place.x + step), 2), rows]

    def cell(step, rows=slice(None)):
        z = wrapped(place.z + step)
        return tokens.at[z // 2, 2 * place.x + lax.rem(z, 2), rows]

    over_x = Ring(292, "x", column, lambda step, d: column(step, pl.ds(d * 128, 128)), x_half, x_part)
    over_z = Ring(296, "z", cell, lambda step, d: cell(step, pl.ds(d * 128, 128)), z_half, z_part)

    for g in FAR_FIRST:
        send_back(g)
        for part in (0, 1):
            compute(part, g)
            outer[part][g].far()
    for g in (2, 1, -1):
        for part in (0, 1):
            outer[part][g].near()
    weigh(2)
    over_x.far()
    for part in (0, 1):
        outer[part][2].end()
        inner[part].far()
    for part in (0, 1):
        outer[part][0].near()
    weigh(1)
    for part in (0, 1):
        outer[part][1].end()
        outer[part][-1].end()
        inner[part].near()
    weigh(-1)
    over_x.near()
    base = 192
    for part in (0, 1):
        outer[part][0].end()
        gots = inner[part].receive()
        total = inner[part].whole(0)[...].astype(F32)
        for got in gots:
            total = total + got[...].astype(F32)
        result[pl.ds(part * 4, 4)] = total.astype(BF16)
    for step in range(1, 8):
        target = lax.rem(place.tp + step, 8)
        link.send(base + step, result.at[target], returned.at[place.tp], place.tp_peer(step))
    returned[place.tp] = result[place.tp]
    weigh(0)
    over_x.end()
    over_z.far()
    over_z.near()
    for step in range(1, 8):
        source = lax.rem(place.tp + 8 - step, 8)
        link.arrived(base + step, returned.at[source], place.tp_peer(8 - step))
    moe = lax.dot_general(
        combine[...],
        returned[...].reshape(768, 256),
        (((0,), (0,)), ((), ())),
        preferred_element_type=F32,
    )
    out[:, 0:256] = (hres[:, 0:256].astype(F32) + moe).astype(BF16)
    total = over_z.whole(0)[...].astype(F32)
    for got in over_z.receive():
        total = total + got[...].astype(F32)
    out[:, 256:384] = (hres[:, 256:384].astype(F32) + total).astype(BF16)
    link.finish()


def on_device(
    resid, queries, keys, values, w_out, norm_gain, w_gate, w_up, w_down, expert_ids, route_units
):
    copies = 300
    return pl.pallas_call(
        layer_kernel,
        out_shape=jax.ShapeDtypeStruct((256, 384), BF16),
        in_specs=[pl.BlockSpec(memory_space=pl.ANY)] * 11,
        out_specs=pl.BlockSpec(memory_space=pltpu.VMEM),
        scratch_shapes=[
            pltpu.VMEM((256, 384), BF16),
            pltpu.VMEM((256, 768), BF16),
            pltpu.VMEM((256, HD), BF16),
            pltpu.VMEM((256, HD), BF16),
            pltpu.VMEM((768, 384), BF16),
            pltpu.VMEM((2, 256), jnp.int32),
            pltpu.VMEM((2, 256), jnp.int32),
            pltpu.VMEM((16, 128, HD), BF16),
            pltpu.VMEM((16, 128, HD), BF16),
            pltpu.VMEM((384,), BF16),
            pltpu.VMEM((16, 8, 384), F32),
            pltpu.VMEM((8, 8, 256), F32),
            pltpu.VMEM((768, 256), BF16),
            pltpu.VMEM((256, 384), BF16),
            pltpu.VMEM((8, 96, 256), BF16),
            pltpu.VMEM((4, 4, 8, 96, 256), BF16),
            pltpu.VMEM((2, 8, 256, 128), BF16),
            pltpu.VMEM((8, 4, 2, 96, 256), BF16),
            pltpu.VMEM((6144, 512), BF16),
            pltpu.VMEM((6144, 512), BF16),
            pltpu.VMEM((512, 6144), BF16),
            pltpu.VMEM((2, 4, 96, 128), F32),
            pltpu.VMEM((2, 4, 96, 512), F32),
            pltpu.VMEM((2, 4, 96, 512), F32),
            pltpu.VMEM((8, 96, 512), BF16),
            pltpu.VMEM((4, 4, 8, 96, 256), BF16),
            pltpu.VMEM((2, 5, 2, 2, 96, 256), BF16),
            pltpu.VMEM((2, 5, 2, 4, 96, 256), BF16),
            pltpu.VMEM((8, 4, 2, 96, 256), BF16),
            pltpu.VMEM((2, 2, 2, 128, 128), BF16),
            pltpu.VMEM((2, 2, 2, 256, 128), BF16),
            pltpu.VMEM((2, 128, 128), BF16),
            pltpu.VMEM((2, 256, 128), BF16),
            pltpu.VMEM((8, 96, 256), BF16),
            pltpu.VMEM((8, 96, 256), BF16),
            pltpu.SemaphoreType.DMA((11,)),
            pltpu.SemaphoreType.DMA((copies,)),
            pltpu.SemaphoreType.DMA((copies,)),
        ],
        compiler_params=pltpu.CompilerParams(
            collective_id=0, has_side_effects=True, vmem_limit_bytes=64 * 1024 * 1024 - 128 * 1024
        ),
        name="layer",
    )(
        resid,
        queries,
        keys,
        values,
        w_out,
        norm_gain,
        w_gate[0],
        w_up[0],
        w_down[0],
        expert_ids.T,
        route_units.T,
    )


def solution(mesh):
    torus = Mesh(mesh.devices.reshape(2, 4, 4, 2, 2), ("zh", "x", "y", "core", "zl"))
    in_specs = (
        P(CTX, TP_EP),
        P(CTX, TP),
        P(CTX, TP),
        P(CTX, TP),
        P(TP, ("zh", "x", "zl")),
        P(TP_EP),
        P(TP, None, ("zh", "x", "zl")),
        P(TP, None, ("zh", "x", "zl")),
        P(TP, ("zh", "x", "zl"), None),
        P(CTX, None),
        P(CTX, None),
    )
    return jax.shard_map(
        on_device, mesh=torus, in_specs=in_specs, out_specs=P(CTX, TP_EP), check_vma=False
    )
```

```python
import jax
import jax.numpy as jnp
from jax import lax
from jax.experimental import pallas as pl
from jax.experimental.pallas import tpu as pltpu
from jax.sharding import Mesh
from jax.sharding import PartitionSpec as P

D = 6144
HD = 128
CTX = ("zh", "x")
TP = ("y", "core")
TP_EP = ("y", "core", "zl")
MESH_ID = pl.DeviceIdType.MESH
F32 = jnp.float32
BF16 = jnp.bfloat16
FAR_FIRST = (2, 1, -1, 0)


def wrapped(index, size=4):
    return lax.rem(index + size, size)


class Place:
    def __init__(self):
        self.x = lax.axis_index("x")
        self.z = lax.axis_index("zh") * 2 + lax.axis_index("zl")
        self.y = lax.axis_index("y")
        self.core = lax.axis_index("core")
        self.zl = lax.axis_index("zl")
        self.tp = self.y * 2 + self.core
        self.ctx = lax.axis_index("zh") * 4 + self.x
        self.member = self.tp * 2 + self.zl

    def beside(self, axis, step):
        if axis == "x":
            return {"x": wrapped(self.x + step)}
        z = wrapped(self.z + step)
        return {"zh": z // 2, "zl": lax.rem(z, 2)}

    def tp_peer(self, step):
        other = lax.rem(self.tp + step, 8)
        return {"y": other // 2, "core": lax.rem(other, 2)}

    def member_peer(self, step):
        other = lax.rem(self.member + step, 16)
        return {"y": other // 4, "core": lax.rem(other // 2, 2), "zl": lax.rem(other, 2)}

    def ctx_peer(self, step):
        other = lax.rem(self.ctx + step, 8)
        return {"zh": other // 4, "x": lax.rem(other, 4)}

    def mirror(self):
        return {"zh": self.tp // 4, "x": lax.rem(self.tp, 4), "y": self.ctx // 2, "core": lax.rem(self.ctx, 2)}

    def greet(self, peers):
        barrier = pltpu.get_barrier_semaphore()
        peers = [self.beside(axis, step) for axis in ("x", "z") for step in (1, -1)] + peers
        for peer in peers:
            pl.semaphore_signal(barrier, inc=1, device_id=peer, device_id_type=MESH_ID)
        return len(peers)


class Link:
    def __init__(self, send_sem, recv_sem):
        self.send_sem, self.recv_sem, self.open = send_sem, recv_sem, []

    def copy(self, number, src, dst, device, landing=None):
        return pltpu.make_async_remote_copy(
            src_ref=src,
            dst_ref=dst,
            send_sem=self.send_sem.at[number],
            recv_sem=self.recv_sem.at[number if landing is None else landing],
            device_id=device,
            device_id_type=MESH_ID,
        )

    def send(self, number, src, dst, device, landing=None):
        copy = self.copy(number, src, dst, device, landing)
        copy.start()
        self.open.append(copy)

    def arrived(self, number, dst, device):
        self.copy(number, dst, dst, device).wait_recv()

    def sent(self, copies):
        for copy in copies:
            copy.wait_send()
        self.open = [copy for copy in self.open if all(copy is not other for other in copies)]

    def finish(self):
        for copy in self.open:
            copy.wait_send()
        self.open = []


WAYS = ((0, 1), (1, -1))


class Gather:
    def __init__(self, place, link, piece, first):
        self.place, self.link, self.piece, self.first = place, link, piece, first

    def block(self, part, along_f, along_s, half=None):
        x, z = (along_f, along_s) if part == 0 else (along_s, along_f)
        return self.piece(wrapped(self.place.x + x), wrapped(self.place.z + z), part, half)

    def number(self, part, kind, direction, g=2):
        return self.first + part * 20 + {"near": 0, "far": 2, "near2": 4, "far2": 12}[kind] + (
            FAR_FIRST.index(g) * 2 + direction
        )

    def near(self, part):
        ref = self.block(part, 0, 0)
        for direction, step in WAYS:
            device = self.place.beside("xz"[part], step)
            self.link.send(self.number(part, "near", direction), ref, ref, device)

    def far(self, part):
        for direction, step in WAYS:
            back = self.place.beside("xz"[part], -step)
            self.link.arrived(self.number(part, "near", direction), self.block(part, -step, 0), back)
            ref = self.block(part, -step, 0, direction)
            device = self.place.beside("xz"[part], step)
            self.link.send(self.number(part, "far", direction), ref, ref, device)

    def far_done(self, part):
        for direction, step in WAYS:
            back = self.place.beside("xz"[part], -step)
            self.link.arrived(self.number(part, "far", direction), self.block(part, 2, 0, direction), back)

    def near2(self, part, g):
        ref = self.block(part, g, 0)
        for direction, step in WAYS:
            device = self.place.beside("zx"[part], step)
            self.link.send(self.number(part, "near2", direction, g), ref, ref, device)

    def far2(self, part, g):
        for direction, step in WAYS:
            back = self.place.beside("zx"[part], -step)
            self.link.arrived(self.number(part, "near2", direction, g), self.block(part, g, -step), back)
            ref = self.block(part, g, -step, direction)
            device = self.place.beside("zx"[part], step)
            self.link.send(self.number(part, "far2", direction, g), ref, ref, device)

    def far2_done(self, part, g):
        for direction, step in WAYS:
            back = self.place.beside("zx"[part], -step)
            number = self.number(part, "far2", direction, g)
            self.link.arrived(number, self.block(part, g, 2, direction), back)


def plane_gather(gather, ready=None, busy=None, later=None, seen=None):
    both = (0, 1)
    for part in both:
        if ready is not None:
            ready(part)
        gather.near(part)
        if ready is not None:
            gather.near2(part, 0)
    if ready is None:
        for part in both:
            gather.near2(part, 0)
    if busy is not None:
        busy()
    for part in both:
        gather.far(part)
    for part in both:
        gather.near2(part, -1)
        gather.near2(part, 1)
    if later is not None:
        later()
    for part in both:
        gather.far2(part, 0)
    for part in both:
        gather.far_done(part)
        gather.near2(part, 2)
    seen = seen or (lambda *_: None)
    seen(0, 0)
    for g in (-1, 1):
        for part in both:
            gather.far2(part, g)
    for part in both:
        gather.far2_done(part, 0)
    seen(1, 0)
    seen(2, 0)
    for part in both:
        gather.far2(part, 2)
    seen(0, -1)
    seen(0, 1)
    seen(2, 1)
    for g in (-1, 1):
        for part in both:
            gather.far2_done(part, g)
    seen(1, -1)
    seen(1, 1)
    seen(2, -1)
    for part in both:
        gather.far2_done(part, 2)
    seen(0, 2)
    seen(1, 2)
    seen(2, 2)


def picked(tile):
    slot_ids = lax.broadcasted_iota(jnp.int32, (768, 256), 0).astype(F32)
    return slot_ids == tile[0:1, :], slot_ids == tile[1:2, :]


def layer_kernel(
    resid_hbm,
    queries_hbm,
    keys_hbm,
    values_hbm,
    w_out_hbm,
    gain_hbm,
    w_gate,
    w_up,
    w_down,
    ids_hbm,
    units_hbm,
    out,
    resid,
    queries,
    keys,
    values,
    w_out,
    ids,
    units,
    all_keys,
    all_values,
    gain,
    gains,
    codes,
    combine,
    hres,
    slots,
    rows,
    tokens,
    token_rows,
    gate_w,
    up_w,
    down_w,
    row_squares,
    gate_acc,
    up_acc,
    hidden,
    partial,
    got_half,
    got_part,
    back_rows,
    x_half,
    x_part,
    z_half,
    z_part,
    result,
    returned,
    load_sem,
    send_sem,
    recv_sem,
):
    place = Place()
    link = Link(send_sem, recv_sem)
    pieces = Link(send_sem, recv_sem)
    pairs = (
        (keys_hbm, keys),
        (values_hbm, values),
        (queries_hbm, queries),
        (gain_hbm, gain),
        (ids_hbm, ids),
        (units_hbm, units),
        (w_out_hbm, w_out),
        (resid_hbm, resid),
        (w_down, down_w),
        (w_gate, gate_w),
        (w_up, up_w),
    )
    loads = [pltpu.make_async_copy(src, dst, load_sem.at[i]) for i, (src, dst) in enumerate(pairs)]
    for load in loads[:9]:
        load.start()
    barrier = pltpu.get_barrier_semaphore()
    diagonal = place.ctx == place.tp
    members = [place.member_peer(step) for step in range(1, 16)]
    ctx_peers = [place.ctx_peer(step) for step in range(1, 8)]
    greeted = place.greet(members + ctx_peers)
    for load in loads[:2]:
        load.wait()

    here = place.ctx * 2 + place.zl
    mine = pl.ds(pl.multiple_of(place.zl * 128, 128), 128)
    all_keys[here] = keys[mine, :]
    all_values[here] = values[mine, :]

    @pl.when(diagonal)
    def _():
        pl.semaphore_wait(barrier, greeted)

    @pl.when(jnp.logical_not(diagonal))
    def _():
        pl.semaphore_signal(barrier, inc=1, device_id=place.mirror(), device_id_type=MESH_ID)
        pl.semaphore_wait(barrier, greeted + 1)

    def at(x, z):
        return ((z // 2) * 4 + x) * 2 + lax.rem(z, 2)

    def key_block(x, z, part, half):
        ref = (all_keys, all_values)[part]
        if half is None:
            return ref.at[at(x, z)]
        return ref.at[at(x, z), pl.ds(half * 64, 64)]

    def route():
        loads[3].wait()
        gains[place.member] = jnp.broadcast_to(gain[...].astype(F32).reshape(1, 384), (8, 384))
        for step in range(1, 16):
            ref = gains.at[place.member]
            link.send(88 + step, ref, ref, members[step - 1])
        loads[4].wait()
        loads[5].wait()
        line = lax.broadcasted_iota(jnp.int32, (8, 256), 0)
        numbers = ids[...]
        named = [line == numbers[k : k + 1, :] for k in range(2)]
        uses = jnp.where(named[0] | named[1], 1.0, 0.0).astype(BF16)
        row = lax.broadcasted_iota(jnp.int32, (256, 256), 0)
        column = lax.broadcasted_iota(jnp.int32, (256, 256), 1)
        before = jnp.where(row < column, 1.0, 0.0).astype(BF16)
        earlier = jnp.dot(uses, before, preferred_element_type=F32)
        amounts = units[...].astype(F32)
        total = amounts[0:1, :] + amounts[1:2, :]
        tile = jnp.zeros((8, 256), F32)
        for k in range(2):
            slot = jnp.sum(jnp.where(named[k], earlier, 0.0), axis=0, keepdims=True)
            code = numbers[k : k + 1, :].astype(F32) * 96.0 + slot
            weight = (amounts[k : k + 1, :] / total).astype(BF16).astype(F32)
            tile = jnp.where(line == k, code, jnp.where(line == 2 + k, weight, tile))
        codes[place.ctx] = tile
        for step in range(1, 8):
            ref = codes.at[place.ctx]
            link.send(200 + step, ref, ref, ctx_peers[step - 1])
        hits = picked(tile)
        combine[...] = (
            jnp.where(hits[0], tile[2:3, :], 0.0) + jnp.where(hits[1], tile[3:4, :], 0.0)
        ).astype(BF16)

    plane_gather(Gather(place, link, key_block, 0), busy=route)
    loads[2].wait()

    def attn_rows(part, block, start, count):
        return pl.ds(pl.multiple_of(part * 2048 + block * 128 + start, 64), count), pl.ds(0, 384)

    def attend(part):
        @pl.loop(0, 3)
        def _(i):
            columns = pl.ds(pl.multiple_of((part * 3 + i) * HD, HD), HD)
            scores = lax.dot_general(
                queries[mine, columns],
                all_keys[...].reshape(2048, HD),
                (((1,), (1,)), ((), ())),
                preferred_element_type=F32,
            ) * HD ** (-0.5)
            query_pos = here * 128 + lax.broadcasted_iota(jnp.int32, (128, 2048), 0)
            key_pos = lax.broadcasted_iota(jnp.int32, (128, 2048), 1)
            scores = jnp.where(key_pos <= query_pos, scores, -1e30)
            probs = jnp.exp(scores - jnp.max(scores, axis=1, keepdims=True))
            denom = jnp.sum(probs, axis=1, keepdims=True)
            update = jnp.dot(
                probs.astype(BF16), all_values[...].reshape(2048, HD), preferred_element_type=F32
            )
            where = attn_rows(part, here, 0, 128)[0]
            gate_w[where, pl.ds(pl.multiple_of(i * HD, HD), HD)] = (update / denom).astype(BF16)

    def attn_block(x, z, part, half):
        if half is None:
            return gate_w.at[attn_rows(part, at(x, z), 0, 128)]
        return gate_w.at[attn_rows(part, at(x, z), half * 64, 64)]

    plane_gather(Gather(place, link, attn_block, 40), ready=attend)

    loads[6].wait()

    def project(ctx):
        total = None
        for part in (0, 1):
            term = jnp.dot(
                gate_w[pl.ds(pl.multiple_of(part * 2048 + ctx * 256, 256), 256), pl.ds(0, 384)],
                w_out[pl.ds(part * 384, 384), :],
                preferred_element_type=F32,
            )
            total = term if total is None else total + term
        return total

    def piece(k):
        return up_w.at[pl.ds(k * 256, 256), pl.ds(0, 384)]

    partner = {"core": 1 - place.core}
    order = [wrapped(place.y + step) for step in (2, 1, -1, 0)]
    for i, j in enumerate(order):
        piece(i)[...] = project(2 * j + 1 - place.core).astype(BF16)
        pieces.send(80 + i, piece(i), piece(4 + i), partner)
    for i, j in enumerate(order):
        total = project(2 * j + place.core)
        pieces.arrived(80 + i, piece(4 + i), partner)
        total = total + piece(4 + i)[...].astype(F32)
        if i < 3:
            piece(8 + i)[...] = total.astype(BF16)
            pieces.send(84 + i, piece(8 + i), piece(12 + i), {"y": j})
    link.finish()
    loads[9].start()
    for i, step in enumerate((2, 1, -1)):
        pieces.arrived(84 + i, piece(12 + i), {"y": wrapped(place.y - step)})
        total = total + piece(12 + i)[...].astype(F32)
    piece(11)[...] = total.astype(BF16)
    move = pieces.copy(87, piece(11), piece(15), place.mirror())

    @pl.when(diagonal)
    def _():
        piece(15)[...] = piece(11)[...]

    @pl.when(jnp.logical_not(diagonal))
    def _():
        move.start()
        pieces.arrived(87, piece(15), place.mirror())

    loads[7].wait()
    hres[...] = (resid[...].astype(F32) + piece(15)[...].astype(F32)).astype(BF16)

    def token_block(x, z, part, half):
        where = z // 2, 2 * x + lax.rem(z, 2)
        if half is None:
            return tokens.at[where]
        return tokens.at[(*where, pl.ds(half * 128, 128))]

    flow = Gather(place, link, token_block, 220)
    own = place.z // 2, 2 * place.x + place.zl
    tokens[own] = hres[:, 256:384]
    flow.near(1)
    flow.near2(1, 0)
    hits = picked(codes[place.ctx])
    picks = jnp.where(hits[0] | hits[1], 1.0, 0.0).astype(BF16)
    slots[...] = jnp.dot(picks, hres[:, 0:256], preferred_element_type=F32).astype(BF16).reshape(8, 96, 256)

    base = 104
    for step in range(1, 8):
        target = lax.rem(place.tp + step, 8)
        link.send(base + step, slots.at[target], rows.at[place.x, place.z, place.tp], place.tp_peer(step))
    rows[place.x, place.z, place.tp] = slots[place.tp]

    @pl.when(jnp.logical_not(diagonal))
    def _():
        move.wait_send()

    pieces.finish()
    loads[10].start()
    flow.far(1)
    for step in range(1, 8):
        source = lax.rem(place.ctx + 8 - step, 8)
        link.arrived(200 + step, codes.at[source], ctx_peers[7 - step])
    flow.near2(1, -1)
    flow.near2(1, 1)

    def chosen(x, target):
        return partial.at[x, pl.ds(0, 2), target]

    groups = {}

    def send_group(g):
        x = wrapped(place.x + g)
        for zh in range(2):
            ctx = zh * 4 + x
            hits = picked(codes[ctx])
            picks = jnp.where(hits[0] | hits[1], 1.0, 0.0).astype(BF16)
            both = jnp.concatenate([tokens[zh, 2 * x + e] for e in range(2)], axis=1)
            taken = jnp.dot(picks, both, preferred_element_type=F32).astype(BF16)
            partial[x, zh] = taken.reshape(8, 96, 256)
        for step in range(1, 8):
            target = lax.rem(place.tp + step, 8)
            number = 208 + FAR_FIRST.index(g) * 8 + step
            link.send(number, chosen(x, target), token_rows.at[place.tp, x], place.tp_peer(step))
        token_rows[place.tp, x] = chosen(x, place.tp)[...]
        groups[g] = link.open[-7:]

    flow.far_done(1)
    flow.near2(1, 2)
    send_group(0)
    for g in (0, 1, -1):
        flow.far2(1, g)
    for step in range(1, 16):
        source = lax.rem(place.member + 16 - step, 16)
        link.arrived(88 + step, gains.at[source], members[15 - step])
    for step in range(1, 8):
        source = lax.rem(place.tp + 8 - step, 8)
        link.arrived(base + step, rows.at[place.x, place.z, source], place.tp_peer(8 - step))

    def block_of_rows(x, z, part, half):
        if half is None:
            return rows.at[x, z, pl.ds(part * 4, 4)]
        return rows.at[x, z, pl.ds(part * 4 + half * 2, 2)]

    def middle_groups():
        flow.far2(1, 2)
        send_group(1)

    def next_group():
        for g in (0, 1, -1, 2):
            flow.far2_done(1, g)
        link.sent(groups[0])
        send_group(-1)
        gate_acc[...] = jnp.zeros_like(gate_acc)
        up_acc[...] = jnp.zeros_like(up_acc)
        row_squares[...] = jnp.zeros_like(row_squares)

    def scaled(value, blocks):
        value = value.astype(F32)
        square = value * value
        squares = square[:, 0:128] + square[:, 128:256]
        return (value * blocks).astype(BF16), squares

    def use_rows(part, along):
        if (part, along) == (0, 0):
            loads[9].wait()
            loads[10].wait()
        if part == 2:
            if along == 0:
                link.sent(groups[1])
                send_group(2)
            use_tokens(along)
            return
        z = wrapped(place.z + along)
        zh, e = z // 2, lax.rem(z, 2)

        @pl.loop(part * 2, part * 2 + 2)
        def _(pair):
            lefts = []
            squares = row_squares[zh]
            for i in range(2):
                t = 2 * pair + i
                left, more = scaled(rows[:, z, t].reshape(384, 256), gains[2 * t + e, 0:1, 0:256])
                lefts.append(left)
                squares = squares + more.reshape(4, 96, 128)
            row_squares[zh] = squares
            left = jnp.concatenate(lefts, axis=1)
            spans = [pl.ds(pl.multiple_of((4 * pair + 2 * i + e) * 384, 128), 256) for i in range(2)]
            for acc, weights in ((gate_acc, gate_w), (up_acc, up_w)):
                right = jnp.concatenate([weights[span, :] for span in spans], axis=0)
                acc[zh] += jnp.dot(left, right, preferred_element_type=F32).reshape(4, 96, 512)

    def use_tokens(g):
        x = wrapped(place.x + g)
        for step in range(1, 8):
            source = lax.rem(place.tp + 8 - step, 8)
            number = 208 + FAR_FIRST.index(g) * 8 + step
            link.arrived(number, token_rows.at[source, x], place.tp_peer(8 - step))

        @pl.loop(0, 4)
        def _(pair):
            lefts, spans = [], []
            squares = row_squares[:, x]
            for i in range(2):
                t = 2 * pair + i
                blocks = jnp.concatenate([gains[2 * t + e, 0:1, 256:384] for e in range(2)], axis=1)
                left, more = scaled(token_rows[t, x].reshape(192, 256), blocks)
                lefts.append(left)
                squares = squares + more.reshape(2, 96, 128)
                spans += [pl.ds(pl.multiple_of((2 * t + e) * 384 + 256, 128), 128) for e in range(2)]
            row_squares[:, x] = squares
            left = jnp.concatenate(lefts, axis=1)
            for acc, weights in ((gate_acc, gate_w), (up_acc, up_w)):
                right = jnp.concatenate([weights[span, :] for span in spans], axis=0)
                acc[:, x] += jnp.dot(left, right, preferred_element_type=F32).reshape(2, 96, 512)

    plane_gather(Gather(place, link, block_of_rows, 112), busy=middle_groups, later=next_group, seen=use_rows)
    link.finish()
    for zh in range(2):
        mean = jnp.sum(row_squares[zh].reshape(384, 128), axis=1, keepdims=True) / D
        scale = lax.rsqrt(mean + 1e-05)
        gate = gate_acc[zh].reshape(384, 512) * scale
        value = gate / (1.0 + jnp.exp(-gate)) * (up_acc[zh].reshape(384, 512) * scale)
        hidden[pl.ds(zh * 4, 4)] = value.astype(BF16).reshape(4, 96, 512)
    loads[8].wait()

    def compute(part, g):
        if part == 0:
            x = wrapped(place.x + g)
            left = jnp.concatenate([hidden[x], hidden[4 + x]], axis=0)

            @pl.loop(0, 4)
            def _(t):
                right = jnp.concatenate(
                    [down_w[:, pl.ds(pl.multiple_of((2 * t + e) * 384, 128), 256)] for e in range(2)], axis=1
                )
                both = jnp.dot(left, right, preferred_element_type=F32).astype(BF16)
                for zh in range(2):
                    for e in range(2):
                        partial[x, zh * 2 + e, t] = both[zh * 96 : zh * 96 + 96, e * 256 : e * 256 + 256]
        else:
            z = wrapped(place.z + g)
            left = hidden[pl.ds((z // 2) * 4, 4)].reshape(384, 512)

            @pl.loop(4, 8)
            def _(t):
                start = (2 * t + lax.rem(z, 2)) * 384
                right = down_w[:, pl.ds(pl.multiple_of(start, 128), 256)]
                both = jnp.dot(left, right, preferred_element_type=F32).astype(BF16)
                partial[:, z, t] = both.reshape(4, 96, 256)

    def send_back(g):
        x = wrapped(place.x + g)
        left = jnp.concatenate([hidden[x], hidden[4 + x]], axis=0)

        @pl.loop(0, 8)
        def _(t):
            right = jnp.concatenate(
                [down_w[:, pl.ds(pl.multiple_of((2 * t + e) * 384 + 256, 128), 128)] for e in range(2)],
                axis=1,
            )
            both = jnp.dot(left, right, preferred_element_type=F32).astype(BF16)
            token_rows[t, x] = both.reshape(2, 96, 256)

        for step in range(1, 8):
            target = lax.rem(place.tp + step, 8)
            number = 260 + FAR_FIRST.index(g) * 8 + step
            link.send(number, token_rows.at[target, x], back_rows.at[place.tp, x], place.tp_peer(step))
        back_rows[place.tp, x] = token_rows[place.tp, x]
        groups[g] = link.open[-7:]

    def weigh(g):
        x = wrapped(place.x + g)
        for step in range(1, 8):
            source = lax.rem(place.tp + 8 - step, 8)
            number = 260 + FAR_FIRST.index(g) * 8 + step
            link.arrived(number, back_rows.at[source, x], place.tp_peer(8 - step))
        for zh in range(2):
            tile = codes[zh * 4 + x]
            hits = picked(tile)
            shares = (
                jnp.where(hits[0], tile[2:3, :], 0.0) + jnp.where(hits[1], tile[3:4, :], 0.0)
            ).astype(BF16)
            total = lax.dot_general(
                shares,
                back_rows[:, x, zh].reshape(768, 256),
                (((0,), (0,)), ((), ())),
                preferred_element_type=F32,
            ).astype(BF16)
            for e in range(2):
                tokens[zh, 2 * x + e] = total[:, e * 128 : e * 128 + 128]

    def add(target, *sources):
        total = target[...].astype(F32)
        for source in sources:
            total = total + source[...].astype(F32)
        target[...] = total.astype(BF16)

    class Ring:
        def __init__(self, number, axis, whole, half, got_half, got_part):
            self.number, self.axis, self.whole, self.half = number, axis, whole, half
            self.got_half, self.got_part = got_half, got_part

        def far(self):
            for direction, step in WAYS:
                link.send(
                    self.number + direction,
                    self.half(2, direction),
                    self.got_half.at[direction],
                    place.beside(self.axis, step),
                )

        def near(self):
            for direction, step in WAYS:
                got = self.got_half.at[direction]
                link.arrived(self.number + direction, got, place.beside(self.axis, -step))
                add(self.half(step, direction), got)
                link.send(
                    self.number + 2 + direction,
                    self.whole(step),
                    self.got_part.at[direction],
                    place.beside(self.axis, step),
                )

        def receive(self):
            for direction, step in WAYS:
                got = self.got_part.at[direction]
                link.arrived(self.number + 2 + direction, got, place.beside(self.axis, -step))
            return [self.got_part.at[direction] for direction in range(2)]

        def end(self):
            add(self.whole(0), *self.receive())

    def slot_ring(part, stage, axis, at):
        def whole(step):
            x, z = at(step)
            return partial.at[x, z, pl.ds(part * 4, 4)]

        def half(step, direction):
            x, z = at(step)
            return partial.at[x, z, pl.ds(part * 4 + direction * 2, 2)]

        number = 152 + (part * 5 + stage) * 4
        return Ring(number, axis, whole, half, got_half.at[part, stage], got_part.at[part, stage])

    def spot(part, along_f, along_s):
        x, z = (along_f, along_s) if part == 0 else (along_s, along_f)
        return wrapped(place.x + x), wrapped(place.z + z)

    outer = [
        {
            g: slot_ring(
                part, FAR_FIRST.index(g), "zx"[part], lambda step, part=part, g=g: spot(part, g, step)
            )
            for g in FAR_FIRST
        }
        for part in (0, 1)
    ]
    inner = [slot_ring(part, 4, "xz"[part], lambda step, part=part: spot(part, step, 0)) for part in (0, 1)]

    def column(step, rows=slice(None)):
        return tokens.at[:, pl.ds(2 * wrapped(place.x + step), 2), rows]

    def cell(step, rows=slice(None)):
        z = wrapped(place.z + step)
        return tokens.at[z // 2, 2 * place.x + lax.rem(z, 2), rows]

    over_x = Ring(292, "x", column, lambda step, d: column(step, pl.ds(d * 128, 128)), x_half, x_part)
    over_z = Ring(296, "z", cell, lambda step, d: cell(step, pl.ds(d * 128, 128)), z_half, z_part)

    for g in FAR_FIRST:
        if g in (2, 1):
            send_back(g)
        for part in (0, 1):
            compute(part, g)
            outer[part][g].far()
    for g in (2, 1, -1):
        for part in (0, 1):
            outer[part][g].near()
    link.sent(groups[2])
    send_back(-1)
    for part in (0, 1):
        outer[part][2].end()
        inner[part].far()
    for part in (0, 1):
        outer[part][0].near()
    weigh(2)
    over_x.far()
    for part in (0, 1):
        outer[part][1].end()
        outer[part][-1].end()
        inner[part].near()
    link.sent(groups[1])
    send_back(0)
    weigh(1)
    weigh(-1)
    over_x.near()
    base = 192
    for part in (0, 1):
        outer[part][0].end()
        gots = inner[part].receive()
        total = inner[part].whole(0)[...].astype(F32)
        for got in gots:
            total = total + got[...].astype(F32)
        result[pl.ds(part * 4, 4)] = total.astype(BF16)
    for step in range(1, 8):
        target = lax.rem(place.tp + step, 8)
        link.send(base + step, result.at[target], returned.at[place.tp], place.tp_peer(step))
    returned[place.tp] = result[place.tp]
    weigh(0)
    over_x.end()
    over_z.far()
    over_z.near()
    for step in range(1, 8):
        source = lax.rem(place.tp + 8 - step, 8)
        link.arrived(base + step, returned.at[source], place.tp_peer(8 - step))
    moe = lax.dot_general(
        combine[...],
        returned[...].reshape(768, 256),
        (((0,), (0,)), ((), ())),
        preferred_element_type=F32,
    )
    out[:, 0:256] = (hres[:, 0:256].astype(F32) + moe).astype(BF16)
    total = over_z.whole(0)[...].astype(F32)
    for got in over_z.receive():
        total = total + got[...].astype(F32)
    out[:, 256:384] = (hres[:, 256:384].astype(F32) + total).astype(BF16)
    link.finish()


def on_device(
    resid, queries, keys, values, w_out, norm_gain, w_gate, w_up, w_down, expert_ids, route_units
):
    copies = 300
    return pl.pallas_call(
        layer_kernel,
        out_shape=jax.ShapeDtypeStruct((256, 384), BF16),
        in_specs=[pl.BlockSpec(memory_space=pl.ANY)] * 11,
        out_specs=pl.BlockSpec(memory_space=pltpu.VMEM),
        scratch_shapes=[
            pltpu.VMEM((256, 384), BF16),
            pltpu.VMEM((256, 768), BF16),
            pltpu.VMEM((256, HD), BF16),
            pltpu.VMEM((256, HD), BF16),
            pltpu.VMEM((768, 384), BF16),
            pltpu.VMEM((2, 256), jnp.int32),
            pltpu.VMEM((2, 256), jnp.int32),
            pltpu.VMEM((16, 128, HD), BF16),
            pltpu.VMEM((16, 128, HD), BF16),
            pltpu.VMEM((384,), BF16),
            pltpu.VMEM((16, 8, 384), F32),
            pltpu.VMEM((8, 8, 256), F32),
            pltpu.VMEM((768, 256), BF16),
            pltpu.VMEM((256, 384), BF16),
            pltpu.VMEM((8, 96, 256), BF16),
            pltpu.VMEM((4, 4, 8, 96, 256), BF16),
            pltpu.VMEM((2, 8, 256, 128), BF16),
            pltpu.VMEM((8, 4, 2, 96, 256), BF16),
            pltpu.VMEM((6144, 512), BF16),
            pltpu.VMEM((6144, 512), BF16),
            pltpu.VMEM((512, 6144), BF16),
            pltpu.VMEM((2, 4, 96, 128), F32),
            pltpu.VMEM((2, 4, 96, 512), F32),
            pltpu.VMEM((2, 4, 96, 512), F32),
            pltpu.VMEM((8, 96, 512), BF16),
            pltpu.VMEM((4, 4, 8, 96, 256), BF16),
            pltpu.VMEM((2, 5, 2, 2, 96, 256), BF16),
            pltpu.VMEM((2, 5, 2, 4, 96, 256), BF16),
            pltpu.VMEM((8, 4, 2, 96, 256), BF16),
            pltpu.VMEM((2, 2, 2, 128, 128), BF16),
            pltpu.VMEM((2, 2, 2, 256, 128), BF16),
            pltpu.VMEM((2, 128, 128), BF16),
            pltpu.VMEM((2, 256, 128), BF16),
            pltpu.VMEM((8, 96, 256), BF16),
            pltpu.VMEM((8, 96, 256), BF16),
            pltpu.SemaphoreType.DMA((11,)),
            pltpu.SemaphoreType.DMA((copies,)),
            pltpu.SemaphoreType.DMA((copies,)),
        ],
        compiler_params=pltpu.CompilerParams(
            collective_id=0, has_side_effects=True, vmem_limit_bytes=64 * 1024 * 1024 - 128 * 1024
        ),
        name="layer",
    )(
        resid,
        queries,
        keys,
        values,
        w_out,
        norm_gain,
        w_gate[0],
        w_up[0],
        w_down[0],
        expert_ids.T,
        route_units.T,
    )


def solution(mesh):
    torus = Mesh(mesh.devices.reshape(2, 4, 4, 2, 2), ("zh", "x", "y", "core", "zl"))
    in_specs = (
        P(CTX, TP_EP),
        P(CTX, TP),
        P(CTX, TP),
        P(CTX, TP),
        P(TP, ("zh", "x", "zl")),
        P(TP_EP),
        P(TP, None, ("zh", "x", "zl")),
        P(TP, None, ("zh", "x", "zl")),
        P(TP, ("zh", "x", "zl"), None),
        P(CTX, None),
        P(CTX, None),
    )
    return jax.shard_map(
        on_device, mesh=torus, in_specs=in_specs, out_specs=P(CTX, TP_EP), check_vma=False
    )
```

```python
import jax
import jax.numpy as jnp
from jax import lax
from jax.experimental import pallas as pl
from jax.experimental.pallas import tpu as pltpu
from jax.sharding import Mesh
from jax.sharding import PartitionSpec as P

D = 6144
HD = 128
CTX = ("zh", "x")
TP = ("y", "core")
TP_EP = ("y", "core", "zl")
MESH_ID = pl.DeviceIdType.MESH
F32 = jnp.float32
BF16 = jnp.bfloat16
FAR_FIRST = (2, 1, -1, 0)


def wrapped(index, size=4):
    return lax.rem(index + size, size)


class Place:
    def __init__(self):
        self.x = lax.axis_index("x")
        self.z = lax.axis_index("zh") * 2 + lax.axis_index("zl")
        self.y = lax.axis_index("y")
        self.core = lax.axis_index("core")
        self.zl = lax.axis_index("zl")
        self.tp = self.y * 2 + self.core
        self.ctx = lax.axis_index("zh") * 4 + self.x
        self.member = self.tp * 2 + self.zl

    def beside(self, axis, step):
        if axis == "x":
            return {"x": wrapped(self.x + step)}
        z = wrapped(self.z + step)
        return {"zh": z // 2, "zl": lax.rem(z, 2)}

    def tp_peer(self, step):
        other = lax.rem(self.tp + step, 8)
        return {"y": other // 2, "core": lax.rem(other, 2)}

    def member_peer(self, step):
        other = lax.rem(self.member + step, 16)
        return {"y": other // 4, "core": lax.rem(other // 2, 2), "zl": lax.rem(other, 2)}

    def ctx_peer(self, step):
        other = lax.rem(self.ctx + step, 8)
        return {"zh": other // 4, "x": lax.rem(other, 4)}

    def mirror(self):
        return {"zh": self.tp // 4, "x": lax.rem(self.tp, 4), "y": self.ctx // 2, "core": lax.rem(self.ctx, 2)}

    def greet(self, peers):
        barrier = pltpu.get_barrier_semaphore()
        peers = [self.beside(axis, step) for axis in ("x", "z") for step in (1, -1)] + peers
        for peer in peers:
            pl.semaphore_signal(barrier, inc=1, device_id=peer, device_id_type=MESH_ID)
        return len(peers)


class Link:
    def __init__(self, send_sem, recv_sem):
        self.send_sem, self.recv_sem, self.open = send_sem, recv_sem, []

    def copy(self, number, src, dst, device, landing=None):
        return pltpu.make_async_remote_copy(
            src_ref=src,
            dst_ref=dst,
            send_sem=self.send_sem.at[number],
            recv_sem=self.recv_sem.at[number if landing is None else landing],
            device_id=device,
            device_id_type=MESH_ID,
        )

    def send(self, number, src, dst, device, landing=None):
        copy = self.copy(number, src, dst, device, landing)
        copy.start()
        self.open.append(copy)

    def arrived(self, number, dst, device):
        self.copy(number, dst, dst, device).wait_recv()

    def sent(self, copies):
        for copy in copies:
            copy.wait_send()
        self.open = [copy for copy in self.open if all(copy is not other for other in copies)]

    def finish(self):
        for copy in self.open:
            copy.wait_send()
        self.open = []


WAYS = ((0, 1), (1, -1))


class Gather:
    def __init__(self, place, link, piece, first):
        self.place, self.link, self.piece, self.first = place, link, piece, first

    def block(self, part, along_f, along_s, half=None):
        x, z = (along_f, along_s) if part == 0 else (along_s, along_f)
        return self.piece(wrapped(self.place.x + x), wrapped(self.place.z + z), part, half)

    def number(self, part, kind, direction, g=2):
        return self.first + part * 20 + {"near": 0, "far": 2, "near2": 4, "far2": 12}[kind] + (
            FAR_FIRST.index(g) * 2 + direction
        )

    def near(self, part):
        ref = self.block(part, 0, 0)
        for direction, step in WAYS:
            device = self.place.beside("xz"[part], step)
            self.link.send(self.number(part, "near", direction), ref, ref, device)

    def far(self, part):
        for direction, step in WAYS:
            back = self.place.beside("xz"[part], -step)
            self.link.arrived(self.number(part, "near", direction), self.block(part, -step, 0), back)
            ref = self.block(part, -step, 0, direction)
            device = self.place.beside("xz"[part], step)
            self.link.send(self.number(part, "far", direction), ref, ref, device)

    def far_done(self, part):
        for direction, step in WAYS:
            back = self.place.beside("xz"[part], -step)
            self.link.arrived(self.number(part, "far", direction), self.block(part, 2, 0, direction), back)

    def near2(self, part, g):
        ref = self.block(part, g, 0)
        for direction, step in WAYS:
            device = self.place.beside("zx"[part], step)
            self.link.send(self.number(part, "near2", direction, g), ref, ref, device)

    def far2(self, part, g):
        for direction, step in WAYS:
            back = self.place.beside("zx"[part], -step)
            self.link.arrived(self.number(part, "near2", direction, g), self.block(part, g, -step), back)
            ref = self.block(part, g, -step, direction)
            device = self.place.beside("zx"[part], step)
            self.link.send(self.number(part, "far2", direction, g), ref, ref, device)

    def far2_done(self, part, g):
        for direction, step in WAYS:
            back = self.place.beside("zx"[part], -step)
            number = self.number(part, "far2", direction, g)
            self.link.arrived(number, self.block(part, g, 2, direction), back)


def plane_gather(gather, ready=None, busy=None, later=None, seen=None):
    both = (0, 1)
    for part in both:
        if ready is not None:
            ready(part)
        gather.near(part)
        if ready is not None:
            gather.near2(part, 0)
    if ready is None:
        for part in both:
            gather.near2(part, 0)
    if busy is not None:
        busy()
    for part in both:
        gather.far(part)
    for part in both:
        gather.near2(part, -1)
        gather.near2(part, 1)
    if later is not None:
        later()
    for part in both:
        gather.far2(part, 0)
    for part in both:
        gather.far_done(part)
        gather.near2(part, 2)
    seen = seen or (lambda *_: None)
    seen(0, 0)
    for g in (-1, 1):
        for part in both:
            gather.far2(part, g)
    for part in both:
        gather.far2_done(part, 0)
    seen(1, 0)
    seen(2, 0)
    for part in both:
        gather.far2(part, 2)
    seen(0, -1)
    seen(0, 1)
    seen(2, 1)
    for g in (-1, 1):
        for part in both:
            gather.far2_done(part, g)
    seen(1, -1)
    seen(1, 1)
    seen(2, -1)
    for part in both:
        gather.far2_done(part, 2)
    seen(0, 2)
    seen(1, 2)
    seen(2, 2)


def picked(tile):
    slot_ids = lax.broadcasted_iota(jnp.int32, (768, 256), 0).astype(F32)
    return slot_ids == tile[0:1, :], slot_ids == tile[1:2, :]


def layer_kernel(
    resid_hbm,
    queries_hbm,
    keys_hbm,
    values_hbm,
    w_out_hbm,
    gain_hbm,
    w_gate,
    w_up,
    w_down,
    ids_hbm,
    units_hbm,
    out,
    resid,
    queries,
    keys,
    values,
    w_out,
    ids,
    units,
    all_keys,
    all_values,
    gain,
    gains,
    codes,
    combine,
    hres,
    slots,
    rows,
    tokens,
    token_rows,
    gate_w,
    up_w,
    down_w,
    row_squares,
    gate_acc,
    up_acc,
    hidden,
    partial,
    got_half,
    got_part,
    back_rows,
    x_half,
    x_part,
    z_half,
    z_part,
    result,
    returned,
    load_sem,
    send_sem,
    recv_sem,
):
    place = Place()
    link = Link(send_sem, recv_sem)
    pieces = Link(send_sem, recv_sem)
    pairs = (
        (keys_hbm, keys),
        (values_hbm, values),
        (queries_hbm, queries),
        (gain_hbm, gain),
        (ids_hbm, ids),
        (units_hbm, units),
        (w_out_hbm, w_out),
        (resid_hbm, resid),
        (w_down, down_w),
        (w_gate, gate_w),
        (w_up, up_w),
    )
    loads = [pltpu.make_async_copy(src, dst, load_sem.at[i]) for i, (src, dst) in enumerate(pairs)]
    for load in loads[:9]:
        load.start()
    barrier = pltpu.get_barrier_semaphore()
    diagonal = place.ctx == place.tp
    members = [place.member_peer(step) for step in range(1, 16)]
    ctx_peers = [place.ctx_peer(step) for step in range(1, 8)]
    greeted = place.greet(members + ctx_peers)
    for load in loads[:2]:
        load.wait()

    here = place.ctx * 2 + place.zl
    mine = pl.ds(pl.multiple_of(place.zl * 128, 128), 128)
    all_keys[here] = keys[mine, :]
    all_values[here] = values[mine, :]

    @pl.when(diagonal)
    def _():
        pl.semaphore_wait(barrier, greeted)

    @pl.when(jnp.logical_not(diagonal))
    def _():
        pl.semaphore_signal(barrier, inc=1, device_id=place.mirror(), device_id_type=MESH_ID)
        pl.semaphore_wait(barrier, greeted + 1)

    def at(x, z):
        return ((z // 2) * 4 + x) * 2 + lax.rem(z, 2)

    def key_block(x, z, part, half):
        ref = (all_keys, all_values)[part]
        if half is None:
            return ref.at[at(x, z)]
        return ref.at[at(x, z), pl.ds(half * 64, 64)]

    def route():
        loads[3].wait()
        gains[place.member] = jnp.broadcast_to(gain[...].astype(F32).reshape(1, 384), (8, 384))
        for step in range(1, 16):
            ref = gains.at[place.member]
            link.send(88 + step, ref, ref, members[step - 1])
        loads[4].wait()
        loads[5].wait()
        line = lax.broadcasted_iota(jnp.int32, (8, 256), 0)
        numbers = ids[...]
        named = [line == numbers[k : k + 1, :] for k in range(2)]
        uses = jnp.where(named[0] | named[1], 1.0, 0.0).astype(BF16)
        row = lax.broadcasted_iota(jnp.int32, (256, 256), 0)
        column = lax.broadcasted_iota(jnp.int32, (256, 256), 1)
        before = jnp.where(row < column, 1.0, 0.0).astype(BF16)
        earlier = jnp.dot(uses, before, preferred_element_type=F32)
        amounts = units[...].astype(F32)
        total = amounts[0:1, :] + amounts[1:2, :]
        tile = jnp.zeros((8, 256), F32)
        for k in range(2):
            slot = jnp.sum(jnp.where(named[k], earlier, 0.0), axis=0, keepdims=True)
            code = numbers[k : k + 1, :].astype(F32) * 96.0 + slot
            weight = (amounts[k : k + 1, :] / total).astype(BF16).astype(F32)
            tile = jnp.where(line == k, code, jnp.where(line == 2 + k, weight, tile))
        codes[place.ctx] = tile
        for step in range(1, 8):
            ref = codes.at[place.ctx]
            link.send(200 + step, ref, ref, ctx_peers[step - 1])
        hits = picked(tile)
        combine[...] = (
            jnp.where(hits[0], tile[2:3, :], 0.0) + jnp.where(hits[1], tile[3:4, :], 0.0)
        ).astype(BF16)

    plane_gather(Gather(place, link, key_block, 0), busy=route)
    loads[2].wait()

    def attn_rows(part, block, start, count):
        return pl.ds(pl.multiple_of(part * 2048 + block * 128 + start, 64), count), pl.ds(0, 384)

    def attend(part):
        @pl.loop(0, 3)
        def _(i):
            columns = pl.ds(pl.multiple_of((part * 3 + i) * HD, HD), HD)
            scores = lax.dot_general(
                queries[mine, columns],
                all_keys[...].reshape(2048, HD),
                (((1,), (1,)), ((), ())),
                preferred_element_type=F32,
            ) * HD ** (-0.5)
            query_pos = here * 128 + lax.broadcasted_iota(jnp.int32, (128, 2048), 0)
            key_pos = lax.broadcasted_iota(jnp.int32, (128, 2048), 1)
            scores = jnp.where(key_pos <= query_pos, scores, -1e30)
            probs = jnp.exp(scores - jnp.max(scores, axis=1, keepdims=True))
            denom = jnp.sum(probs, axis=1, keepdims=True)
            update = jnp.dot(
                probs.astype(BF16), all_values[...].reshape(2048, HD), preferred_element_type=F32
            )
            where = attn_rows(part, here, 0, 128)[0]
            gate_w[where, pl.ds(pl.multiple_of(i * HD, HD), HD)] = (update / denom).astype(BF16)

    def attn_block(x, z, part, half):
        if half is None:
            return gate_w.at[attn_rows(part, at(x, z), 0, 128)]
        return gate_w.at[attn_rows(part, at(x, z), half * 64, 64)]

    plane_gather(Gather(place, link, attn_block, 40), ready=attend)

    loads[6].wait()

    def project(ctx):
        total = None
        for part in (0, 1):
            term = jnp.dot(
                gate_w[pl.ds(pl.multiple_of(part * 2048 + ctx * 256, 256), 256), pl.ds(0, 384)],
                w_out[pl.ds(part * 384, 384), :],
                preferred_element_type=F32,
            )
            total = term if total is None else total + term
        return total

    def piece(k):
        return up_w.at[pl.ds(k * 256, 256), pl.ds(0, 384)]

    partner = {"core": 1 - place.core}
    order = [wrapped(place.y + step) for step in (2, 1, -1, 0)]
    for i, j in enumerate(order):
        piece(i)[...] = project(2 * j + 1 - place.core).astype(BF16)
        pieces.send(80 + i, piece(i), piece(4 + i), partner)
    for i, j in enumerate(order):
        total = project(2 * j + place.core)
        pieces.arrived(80 + i, piece(4 + i), partner)
        total = total + piece(4 + i)[...].astype(F32)
        if i < 3:
            piece(8 + i)[...] = total.astype(BF16)
            pieces.send(84 + i, piece(8 + i), piece(12 + i), {"y": j})
    link.finish()
    loads[9].start()
    for i, step in enumerate((2, 1, -1)):
        pieces.arrived(84 + i, piece(12 + i), {"y": wrapped(place.y - step)})
        total = total + piece(12 + i)[...].astype(F32)
    piece(11)[...] = total.astype(BF16)
    move = pieces.copy(87, piece(11), piece(15), place.mirror())

    @pl.when(diagonal)
    def _():
        piece(15)[...] = piece(11)[...]

    @pl.when(jnp.logical_not(diagonal))
    def _():
        move.start()
        pieces.arrived(87, piece(15), place.mirror())

    loads[7].wait()
    hres[...] = (resid[...].astype(F32) + piece(15)[...].astype(F32)).astype(BF16)

    def token_block(x, z, part, half):
        where = z // 2, 2 * x + lax.rem(z, 2)
        if half is None:
            return tokens.at[where]
        return tokens.at[(*where, pl.ds(half * 128, 128))]

    flow = Gather(place, link, token_block, 220)
    own = place.z // 2, 2 * place.x + place.zl
    tokens[own] = hres[:, 256:384]
    flow.near(1)
    flow.near2(1, 0)
    hits = picked(codes[place.ctx])
    picks = jnp.where(hits[0] | hits[1], 1.0, 0.0).astype(BF16)
    slots[...] = jnp.dot(picks, hres[:, 0:256], preferred_element_type=F32).astype(BF16).reshape(8, 96, 256)

    base = 104
    for step in range(1, 8):
        target = lax.rem(place.tp + step, 8)
        link.send(base + step, slots.at[target], rows.at[place.x, place.z, place.tp], place.tp_peer(step))
    rows[place.x, place.z, place.tp] = slots[place.tp]

    @pl.when(jnp.logical_not(diagonal))
    def _():
        move.wait_send()

    pieces.finish()
    loads[10].start()
    flow.far(1)
    for step in range(1, 8):
        source = lax.rem(place.ctx + 8 - step, 8)
        link.arrived(200 + step, codes.at[source], ctx_peers[7 - step])
    flow.near2(1, -1)
    flow.near2(1, 1)

    def chosen(x, target):
        return partial.at[x, pl.ds(0, 2), target]

    groups = {}

    def send_group(g):
        x = wrapped(place.x + g)
        for zh in range(2):
            ctx = zh * 4 + x
            hits = picked(codes[ctx])
            picks = jnp.where(hits[0] | hits[1], 1.0, 0.0).astype(BF16)
            both = jnp.concatenate([tokens[zh, 2 * x + e] for e in range(2)], axis=1)
            taken = jnp.dot(picks, both, preferred_element_type=F32).astype(BF16)
            partial[x, zh] = taken.reshape(8, 96, 256)
        for step in range(1, 8):
            target = lax.rem(place.tp + step, 8)
            number = 208 + FAR_FIRST.index(g) * 8 + step
            link.send(number, chosen(x, target), token_rows.at[place.tp, x], place.tp_peer(step))
        token_rows[place.tp, x] = chosen(x, place.tp)[...]
        groups[g] = link.open[-7:]

    flow.far_done(1)
    flow.near2(1, 2)
    send_group(0)
    for g in (0, 1, -1):
        flow.far2(1, g)
    for step in range(1, 16):
        source = lax.rem(place.member + 16 - step, 16)
        link.arrived(88 + step, gains.at[source], members[15 - step])
    for step in range(1, 8):
        source = lax.rem(place.tp + 8 - step, 8)
        link.arrived(base + step, rows.at[place.x, place.z, source], place.tp_peer(8 - step))

    def block_of_rows(x, z, part, half):
        if half is None:
            return rows.at[x, z, pl.ds(part * 4, 4)]
        return rows.at[x, z, pl.ds(part * 4 + half * 2, 2)]

    def middle_groups():
        flow.far2(1, 2)
        send_group(1)

    def next_group():
        for g in (0, 1, -1, 2):
            flow.far2_done(1, g)
        link.sent(groups[0])
        send_group(-1)
        gate_acc[...] = jnp.zeros_like(gate_acc)
        up_acc[...] = jnp.zeros_like(up_acc)
        row_squares[...] = jnp.zeros_like(row_squares)

    def scaled(value, blocks):
        value = value.astype(F32)
        square = value * value
        squares = square[:, 0:128] + square[:, 128:256]
        return (value * blocks).astype(BF16), squares

    def use_rows(part, along):
        if (part, along) == (0, 0):
            loads[9].wait()
            loads[10].wait()
        if part == 2:
            if along == 0:
                link.sent(groups[1])
                send_group(2)
            use_tokens(along)
            return
        z = wrapped(place.z + along)
        zh, e = z // 2, lax.rem(z, 2)

        @pl.loop(part * 2, part * 2 + 2)
        def _(pair):
            lefts = []
            squares = row_squares[zh]
            for i in range(2):
                t = 2 * pair + i
                left, more = scaled(rows[:, z, t].reshape(384, 256), gains[2 * t + e, 0:1, 0:256])
                lefts.append(left)
                squares = squares + more.reshape(4, 96, 128)
            row_squares[zh] = squares
            left = jnp.concatenate(lefts, axis=1)
            spans = [pl.ds(pl.multiple_of((4 * pair + 2 * i + e) * 384, 128), 256) for i in range(2)]
            for acc, weights in ((gate_acc, gate_w), (up_acc, up_w)):
                right = jnp.concatenate([weights[span, :] for span in spans], axis=0)
                acc[zh] += jnp.dot(left, right, preferred_element_type=F32).reshape(4, 96, 512)

    def use_tokens(g):
        x = wrapped(place.x + g)
        for step in range(1, 8):
            source = lax.rem(place.tp + 8 - step, 8)
            number = 208 + FAR_FIRST.index(g) * 8 + step
            link.arrived(number, token_rows.at[source, x], place.tp_peer(8 - step))

        @pl.loop(0, 4)
        def _(pair):
            lefts, spans = [], []
            squares = row_squares[:, x]
            for i in range(2):
                t = 2 * pair + i
                blocks = jnp.concatenate([gains[2 * t + e, 0:1, 256:384] for e in range(2)], axis=1)
                left, more = scaled(token_rows[t, x].reshape(192, 256), blocks)
                lefts.append(left)
                squares = squares + more.reshape(2, 96, 128)
                spans += [pl.ds(pl.multiple_of((2 * t + e) * 384 + 256, 128), 128) for e in range(2)]
            row_squares[:, x] = squares
            left = jnp.concatenate(lefts, axis=1)
            for acc, weights in ((gate_acc, gate_w), (up_acc, up_w)):
                right = jnp.concatenate([weights[span, :] for span in spans], axis=0)
                acc[:, x] += jnp.dot(left, right, preferred_element_type=F32).reshape(2, 96, 512)

    plane_gather(Gather(place, link, block_of_rows, 112), busy=middle_groups, later=next_group, seen=use_rows)
    link.finish()
    for zh in range(2):
        mean = jnp.sum(row_squares[zh].reshape(384, 128), axis=1, keepdims=True) / D
        scale = lax.rsqrt(mean + 1e-05)
        gate = gate_acc[zh].reshape(384, 512) * scale
        value = gate / (1.0 + jnp.exp(-gate)) * (up_acc[zh].reshape(384, 512) * scale)
        hidden[pl.ds(zh * 4, 4)] = value.astype(BF16).reshape(4, 96, 512)
    loads[8].wait()

    def compute(part, g):
        if part == 0:
            x = wrapped(place.x + g)
            left = jnp.concatenate([hidden[x], hidden[4 + x]], axis=0)

            @pl.loop(0, 4)
            def _(t):
                right = jnp.concatenate(
                    [down_w[:, pl.ds(pl.multiple_of((2 * t + e) * 384, 128), 256)] for e in range(2)], axis=1
                )
                both = jnp.dot(left, right, preferred_element_type=F32).astype(BF16)
                for zh in range(2):
                    for e in range(2):
                        partial[x, zh * 2 + e, t] = both[zh * 96 : zh * 96 + 96, e * 256 : e * 256 + 256]
        else:
            z = wrapped(place.z + g)
            left = hidden[pl.ds((z // 2) * 4, 4)].reshape(384, 512)

            @pl.loop(4, 8)
            def _(t):
                start = (2 * t + lax.rem(z, 2)) * 384
                right = down_w[:, pl.ds(pl.multiple_of(start, 128), 256)]
                both = jnp.dot(left, right, preferred_element_type=F32).astype(BF16)
                partial[:, z, t] = both.reshape(4, 96, 256)

    def send_back(g):
        x = wrapped(place.x + g)
        left = jnp.concatenate([hidden[x], hidden[4 + x]], axis=0)

        @pl.loop(0, 8)
        def _(t):
            right = jnp.concatenate(
                [down_w[:, pl.ds(pl.multiple_of((2 * t + e) * 384 + 256, 128), 128)] for e in range(2)],
                axis=1,
            )
            both = jnp.dot(left, right, preferred_element_type=F32).astype(BF16)
            token_rows[t, x] = both.reshape(2, 96, 256)

        for step in range(1, 8):
            target = lax.rem(place.tp + step, 8)
            number = 260 + FAR_FIRST.index(g) * 8 + step
            link.send(number, token_rows.at[target, x], back_rows.at[place.tp, x], place.tp_peer(step))
        back_rows[place.tp, x] = token_rows[place.tp, x]
        groups[g] = link.open[-7:]

    def weigh(g):
        x = wrapped(place.x + g)
        for step in range(1, 8):
            source = lax.rem(place.tp + 8 - step, 8)
            number = 260 + FAR_FIRST.index(g) * 8 + step
            link.arrived(number, back_rows.at[source, x], place.tp_peer(8 - step))
        for zh in range(2):
            tile = codes[zh * 4 + x]
            hits = picked(tile)
            shares = (
                jnp.where(hits[0], tile[2:3, :], 0.0) + jnp.where(hits[1], tile[3:4, :], 0.0)
            ).astype(BF16)
            total = lax.dot_general(
                shares,
                back_rows[:, x, zh].reshape(768, 256),
                (((0,), (0,)), ((), ())),
                preferred_element_type=F32,
            ).astype(BF16)
            for e in range(2):
                tokens[zh, 2 * x + e] = total[:, e * 128 : e * 128 + 128]

    def add(target, *sources):
        total = target[...].astype(F32)
        for source in sources:
            total = total + source[...].astype(F32)
        target[...] = total.astype(BF16)

    class Ring:
        def __init__(self, number, axis, whole, half, got_half, got_part):
            self.number, self.axis, self.whole, self.half = number, axis, whole, half
            self.got_half, self.got_part = got_half, got_part

        def far(self):
            for direction, step in WAYS:
                link.send(
                    self.number + direction,
                    self.half(2, direction),
                    self.got_half.at[direction],
                    place.beside(self.axis, step),
                )

        def near(self):
            for direction, step in WAYS:
                got = self.got_half.at[direction]
                link.arrived(self.number + direction, got, place.beside(self.axis, -step))
                add(self.half(step, direction), got)
                link.send(
                    self.number + 2 + direction,
                    self.whole(step),
                    self.got_part.at[direction],
                    place.beside(self.axis, step),
                )

        def receive(self):
            for direction, step in WAYS:
                got = self.got_part.at[direction]
                link.arrived(self.number + 2 + direction, got, place.beside(self.axis, -step))
            return [self.got_part.at[direction] for direction in range(2)]

        def end(self):
            add(self.whole(0), *self.receive())

    def slot_ring(part, stage, axis, at):
        def whole(step):
            x, z = at(step)
            return partial.at[x, z, pl.ds(part * 4, 4)]

        def half(step, direction):
            x, z = at(step)
            return partial.at[x, z, pl.ds(part * 4 + direction * 2, 2)]

        number = 152 + (part * 5 + stage) * 4
        return Ring(number, axis, whole, half, got_half.at[part, stage], got_part.at[part, stage])

    def spot(part, along_f, along_s):
        x, z = (along_f, along_s) if part == 0 else (along_s, along_f)
        return wrapped(place.x + x), wrapped(place.z + z)

    outer = [
        {
            g: slot_ring(
                part, FAR_FIRST.index(g), "zx"[part], lambda step, part=part, g=g: spot(part, g, step)
            )
            for g in FAR_FIRST
        }
        for part in (0, 1)
    ]
    inner = [slot_ring(part, 4, "xz"[part], lambda step, part=part: spot(part, step, 0)) for part in (0, 1)]

    def column(step, rows=slice(None)):
        return tokens.at[:, pl.ds(2 * wrapped(place.x + step), 2), rows]

    def cell(step, rows=slice(None)):
        z = wrapped(place.z + step)
        return tokens.at[z // 2, 2 * place.x + lax.rem(z, 2), rows]

    over_x = Ring(292, "x", column, lambda step, d: column(step, pl.ds(d * 128, 128)), x_half, x_part)
    over_z = Ring(296, "z", cell, lambda step, d: cell(step, pl.ds(d * 128, 128)), z_half, z_part)

    for g in FAR_FIRST:
        if g == 2:
            send_back(g)
        for part in (0, 1):
            compute(part, g)
            outer[part][g].far()
    for part in (0, 1):
        outer[part][2].near()
    link.sent(groups[2])
    send_back(1)
    for g in (1, -1):
        for part in (0, 1):
            outer[part][g].near()
    for part in (0, 1):
        outer[part][2].end()
        inner[part].far()
    for part in (0, 1):
        outer[part][0].near()
    weigh(2)
    over_x.far()
    link.sent(groups[1])
    send_back(-1)
    for part in (0, 1):
        outer[part][1].end()
        outer[part][-1].end()
        inner[part].near()
    weigh(1)
    link.sent(groups[-1])
    send_back(0)
    weigh(-1)
    over_x.near()
    base = 192
    for part in (0, 1):
        outer[part][0].end()
        gots = inner[part].receive()
        total = inner[part].whole(0)[...].astype(F32)
        for got in gots:
            total = total + got[...].astype(F32)
        result[pl.ds(part * 4, 4)] = total.astype(BF16)
    for step in range(1, 8):
        target = lax.rem(place.tp + step, 8)
        link.send(base + step, result.at[target], returned.at[place.tp], place.tp_peer(step))
    returned[place.tp] = result[place.tp]
    weigh(0)
    over_x.end()
    over_z.far()
    over_z.near()
    for step in range(1, 8):
        source = lax.rem(place.tp + 8 - step, 8)
        link.arrived(base + step, returned.at[source], place.tp_peer(8 - step))
    moe = lax.dot_general(
        combine[...],
        returned[...].reshape(768, 256),
        (((0,), (0,)), ((), ())),
        preferred_element_type=F32,
    )
    out[:, 0:256] = (hres[:, 0:256].astype(F32) + moe).astype(BF16)
    total = over_z.whole(0)[...].astype(F32)
    for got in over_z.receive():
        total = total + got[...].astype(F32)
    out[:, 256:384] = (hres[:, 256:384].astype(F32) + total).astype(BF16)
    link.finish()


def on_device(
    resid, queries, keys, values, w_out, norm_gain, w_gate, w_up, w_down, expert_ids, route_units
):
    copies = 300
    return pl.pallas_call(
        layer_kernel,
        out_shape=jax.ShapeDtypeStruct((256, 384), BF16),
        in_specs=[pl.BlockSpec(memory_space=pl.ANY)] * 11,
        out_specs=pl.BlockSpec(memory_space=pltpu.VMEM),
        scratch_shapes=[
            pltpu.VMEM((256, 384), BF16),
            pltpu.VMEM((256, 768), BF16),
            pltpu.VMEM((256, HD), BF16),
            pltpu.VMEM((256, HD), BF16),
            pltpu.VMEM((768, 384), BF16),
            pltpu.VMEM((2, 256), jnp.int32),
            pltpu.VMEM((2, 256), jnp.int32),
            pltpu.VMEM((16, 128, HD), BF16),
            pltpu.VMEM((16, 128, HD), BF16),
            pltpu.VMEM((384,), BF16),
            pltpu.VMEM((16, 8, 384), F32),
            pltpu.VMEM((8, 8, 256), F32),
            pltpu.VMEM((768, 256), BF16),
            pltpu.VMEM((256, 384), BF16),
            pltpu.VMEM((8, 96, 256), BF16),
            pltpu.VMEM((4, 4, 8, 96, 256), BF16),
            pltpu.VMEM((2, 8, 256, 128), BF16),
            pltpu.VMEM((8, 4, 2, 96, 256), BF16),
            pltpu.VMEM((6144, 512), BF16),
            pltpu.VMEM((6144, 512), BF16),
            pltpu.VMEM((512, 6144), BF16),
            pltpu.VMEM((2, 4, 96, 128), F32),
            pltpu.VMEM((2, 4, 96, 512), F32),
            pltpu.VMEM((2, 4, 96, 512), F32),
            pltpu.VMEM((8, 96, 512), BF16),
            pltpu.VMEM((4, 4, 8, 96, 256), BF16),
            pltpu.VMEM((2, 5, 2, 2, 96, 256), BF16),
            pltpu.VMEM((2, 5, 2, 4, 96, 256), BF16),
            pltpu.VMEM((8, 4, 2, 96, 256), BF16),
            pltpu.VMEM((2, 2, 2, 128, 128), BF16),
            pltpu.VMEM((2, 2, 2, 256, 128), BF16),
            pltpu.VMEM((2, 128, 128), BF16),
            pltpu.VMEM((2, 256, 128), BF16),
            pltpu.VMEM((8, 96, 256), BF16),
            pltpu.VMEM((8, 96, 256), BF16),
            pltpu.SemaphoreType.DMA((11,)),
            pltpu.SemaphoreType.DMA((copies,)),
            pltpu.SemaphoreType.DMA((copies,)),
        ],
        compiler_params=pltpu.CompilerParams(
            collective_id=0, has_side_effects=True, vmem_limit_bytes=64 * 1024 * 1024 - 128 * 1024
        ),
        name="layer",
    )(
        resid,
        queries,
        keys,
        values,
        w_out,
        norm_gain,
        w_gate[0],
        w_up[0],
        w_down[0],
        expert_ids.T,
        route_units.T,
    )


def solution(mesh):
    torus = Mesh(mesh.devices.reshape(2, 4, 4, 2, 2), ("zh", "x", "y", "core", "zl"))
    in_specs = (
        P(CTX, TP_EP),
        P(CTX, TP),
        P(CTX, TP),
        P(CTX, TP),
        P(TP, ("zh", "x", "zl")),
        P(TP_EP),
        P(TP, None, ("zh", "x", "zl")),
        P(TP, None, ("zh", "x", "zl")),
        P(TP, ("zh", "x", "zl"), None),
        P(CTX, None),
        P(CTX, None),
    )
    return jax.shard_map(
        on_device, mesh=torus, in_specs=in_specs, out_specs=P(CTX, TP_EP), check_vma=False
    )
```
